256 devices in a mesh: leaf: 16 (over z, core), grp: 16 (over y, x).
Axes of the slice: x: 4, y: 4, z: 8, core: 2. Of those that a mesh axis runs over, the one named last changes fastest.
Arguments:
- front_rows: bfloat16 [16384, 24576], P('leaf', 'grp'), may hold values from -0.0390625 to 0.0390625
- sample_matrix: bfloat16 [24576, 1024], P('grp'), may hold values from -6 to 6
- pivots: int32 [31, 512], replicated, may hold values from 0 to 1023, as said below
Outputs:
- bases: float32 [5, 16, 1024, 512], P(None, 'leaf', 'grp')
- top_sample: float32 [1024, 512], P('grp')
The draws below stay inside these ranges and needn't reach their ends.
Inputs may be any that keep to these rules, and one draw needn't show every extreme that they name: `pivots`: row o_l + j (o_l = 2 * 16 - 2 * 16 / 2^l) holds node j of level l: 512 distinct column numbers of its 1024 columns; entries k * 32 to (k + 1) * 32 - 1 lie in k * 64 to (k + 1) * 64 - 1.
All inputs are finite; a program needn't handle non-finite values.
Results may differ from the reference program's by a relative error of at most 0.0003.
Values sent between devices are 32-bit elements; how exact they have to be, the bound alone decides.
A program may use at most 128 MiB of HBM per device.

```python
import jax
import jax.numpy as jnp
from jax import lax

R = 512
K = 1024
LEAVES = 16
MERGES = 4
NODES = 31
COLS = 24576
ROWS_DEV = 64
PIV_DEV = 32


def draw_pivots(key, part):
    blocks = 2 * R // ROWS_DEV
    keys = jax.random.split(jax.random.fold_in(key, 17), NODES * blocks)
    orders = jax.vmap(lambda single: jax.random.permutation(single, ROWS_DEV))(keys)
    picked = orders[:, :PIV_DEV].astype(jnp.int32).reshape(NODES, blocks, PIV_DEV)
    starts = (jnp.arange(blocks, dtype=jnp.int32) * ROWS_DEV)[None, :, None]
    return (picked + starts).reshape(NODES, R).astype(jnp.int32)


def shard_levels(key, shape, cuts, least, high):
    gain = 1.0
    for dim, parts in cuts:
        draws = jax.random.uniform(jax.random.fold_in(jax.random.fold_in(key, 6), dim), (parts,), jnp.float32, least / len(cuts), high / len(cuts))
        gain = gain * jnp.repeat(jnp.exp(draws), shape[dim] // parts).reshape((-1,) + (1,) * (len(shape) - 1 - dim))
    return gain


def noise(own_key, shape, scale, reach, cuts=(), kind=jnp.bfloat16):
    result = scale * jax.random.normal(own_key, shape, jnp.float32)
    if cuts:
        result = result * shard_levels(own_key, shape, cuts, -0.22, 0.18)
    return jnp.clip(result, -reach, reach).astype(kind)


def setup_inputs(seed: int = 0) -> dict:
    splits = jax.random.split(jax.random.key(seed), 4)
    front_rows = noise(splits[0], (LEAVES * 2 * R, COLS), COLS ** -0.5, 0.0390625, ((0, 16), (1, 16)))
    sample_matrix = noise(splits[1], (COLS, K), 1.0, 6.0, ((0, 16),))
    pivots = draw_pivots(jax.random.fold_in(splits[3], 71), 0)
    return {"front_rows": front_rows, "sample_matrix": sample_matrix, "pivots": pivots}


def solve_basis(gram, cross):
    factor = jnp.linalg.cholesky(gram)
    identity = jnp.eye(gram.shape[0], dtype=gram.dtype)
    inverse_factor = jax.scipy.linalg.solve_triangular(factor, identity, lower=True)
    gram_inverse = jnp.dot(inverse_factor.T.astype(jnp.float32), inverse_factor.astype(jnp.float32), precision=lax.Precision.HIGHEST, preferred_element_type=jnp.float32)
    return jnp.dot(cross.astype(jnp.float32), gram_inverse.astype(jnp.float32), precision=lax.Precision.HIGHEST, preferred_element_type=jnp.float32)

def reference(front_rows, sample_matrix, pivots):

    def first_sample(block):
        return lax.dot_general(sample_matrix.astype(jnp.float32), block.astype(jnp.float32), (((0,), (1,)), ((), ())), preferred_element_type=jnp.float32)
    samples = lax.map(first_sample, front_rows.reshape(LEAVES, 2 * R, COLS))

    def one_node(packed):
        sample, chosen = packed
        skeleton = jnp.take(sample, chosen, axis=1)
        gram = lax.dot_general(skeleton.astype(jnp.float32), skeleton.astype(jnp.float32), (((0,), (0,)), ((), ())), precision=lax.Precision.HIGHEST, preferred_element_type=jnp.float32)
        cross = lax.dot_general(sample.astype(jnp.float32), skeleton.astype(jnp.float32), (((0,), (0,)), ((), ())), precision=lax.Precision.HIGHEST, preferred_element_type=jnp.float32)
        return (solve_basis(gram, cross), skeleton)
    collected = []
    offset = 0
    skeletons = samples
    for depth_level in range(MERGES + 1):
        nodes_now = LEAVES >> depth_level
        chosen = pivots[offset:offset + nodes_now]
        node_bases, skeletons = lax.map(one_node, (samples, chosen))
        collected.append(jnp.repeat(node_bases, 2 ** depth_level, axis=0))
        offset = offset + nodes_now
        if depth_level < MERGES:
            paired = skeletons.reshape(nodes_now // 2, 2, K, R)
            samples = jnp.concatenate([paired[:, 0], paired[:, 1]], axis=2)
    return (jnp.stack(collected), skeletons[0])
```

```python
import jax
import jax.numpy as jnp
from jax import lax
from jax.experimental import pallas as pl
from jax.experimental.pallas import tpu as pltpu
from jax.sharding import PartitionSpec as P

HI = lax.Precision.HIGHEST
MESH = pl.DeviceIdType.MESH
SOLVERS = ((0, 0, 0), (0, 1, 10), (1, 0, 2), (2, 1, 8), (3, 0, 5), (4, 1, 15))


def bit(value, place):
    return lax.rem(value // (1 << place), 2)


def flip(value, mask):
    for place in range(4):
        if mask >> place & 1:
            value = value + (1 << place) * (1 - 2 * bit(value, place))
    return value


def send(src, dst, send_sem, recv_sem, device):
    return pltpu.make_async_remote_copy(
        src_ref=src, dst_ref=dst, send_sem=send_sem, recv_sem=recv_sem, device_id=device, device_id_type=MESH
    )


def permuted(src, index):
    rows = src.shape[0]
    wanted = jnp.where(lax.broadcasted_iota(jnp.int32, (256, 256), 0) == index, 1.0, 0.0).astype(jnp.bfloat16)
    high = src.astype(jnp.bfloat16)
    rest = src - high.astype(jnp.float32)
    middle = rest.astype(jnp.bfloat16)
    low = (rest - middle.astype(jnp.float32)).astype(jnp.bfloat16)
    stacked = jnp.concatenate([high, middle, low], axis=0)
    out = jnp.dot(stacked, wanted, preferred_element_type=jnp.float32)
    return (out[:rows] + out[rows : 2 * rows]) + out[2 * rows :]


def gather_kernel(
    p_ref, index_ref, z_ref, top_ref,
    hop1, comb1, near1, sum1, hop2, comb2, near2, y_ref, a3_ref, r1_ref, r2_ref, r3_ref, r4_ref,
    rs_send, rs_recv, leaf_send, leaf_recv, z_send, z_recv, z_local,
):
    leaf, grp = lax.axis_index("leaf"), lax.axis_index("grp")
    y, x = grp // 4, lax.rem(grp, 4)
    core = lax.rem(leaf, 2)

    barrier = pltpu.get_barrier_semaphore()
    for other in range(1, 16):
        pl.semaphore_signal(barrier, inc=1, device_id=(leaf, lax.rem(grp + other, 16)), device_id_type=MESH)
        pl.semaphore_signal(barrier, inc=1, device_id=(lax.rem(leaf + other, 16), grp), device_id_type=MESH)
    pl.semaphore_wait(barrier, 30)

    started = []

    def begin(copy):
        copy.start()
        started.append(copy)
        return copy

    def neighbour(along_x, offset):
        if along_x:
            return (leaf, y * 4 + lax.rem(x + offset, 4))
        return (leaf, lax.rem(y + offset, 4) * 4 + x)

    def source(phase, half, chunk, sub):
        if phase == 0:
            lanes = pl.ds(512 * half, 512)
            if half == 0:
                return p_ref.at[pl.ds(2 * sub, 2), chunk, :, lanes]
            return p_ref.at[chunk, pl.ds(2 * sub, 2), :, lanes]
        return sum1.at[half, chunk, pl.ds(32 * sub, 32), :]

    def landing(phase, half, way, sub):
        if phase == 0:
            return near1.at[half, way, pl.ds(2 * sub, 2), :, :]
        return near2.at[half, way, pl.ds(32 * sub, 32), :]

    hops, combs = (hop1, hop2), (comb1, comb2)
    rings = {}

    def ring_first(phase, half):
        along_x = (phase == 0) == (half == 0)
        at = x if along_x else y
        for way in range(2):
            to = neighbour(along_x, 1 if way == 0 else 3)
            sems = lambda kind: (rs_send.at[phase, half, way, kind], rs_recv.at[phase, half, way, kind])
            rings[phase, half, way, 0] = begin(
                send(source(phase, half, lax.rem(at + 2, 4), way), hops[phase].at[half, way], *sems(0), to)
            )
        for way in range(2):
            to = neighbour(along_x, 1 if way == 0 else 3)
            sems = lambda kind: (rs_send.at[phase, half, way, kind], rs_recv.at[phase, half, way, kind])
            chunk = lax.rem(at + (1 if way == 0 else 3), 4)
            rings[phase, half, way, 1] = begin(
                send(source(phase, half, chunk, 1 - way), landing(phase, half, way, 1 - way), *sems(1), to)
            )

    def ring_second(phase, half):
        along_x = (phase == 0) == (half == 0)
        at = x if along_x else y
        for way in range(2):
            to = neighbour(along_x, 1 if way == 0 else 3)
            chunk = lax.rem(at + (1 if way == 0 else 3), 4)
            rings[phase, half, way, 0].wait_recv()
            combs[phase][half, way] = hops[phase][half, way] + source(phase, half, chunk, way)[...]
            rings[phase, half, way, 2] = begin(
                send(
                    combs[phase].at[half, way], landing(phase, half, way, way),
                    rs_send.at[phase, half, way, 2], rs_recv.at[phase, half, way, 2], to,
                )
            )

    def ring_last(phase, half):
        for way in range(2):
            for kind in (1, 2):
                rings[phase, half, way, kind].wait_recv()

    for half in range(2):
        ring_first(0, half)
    for half in range(2):
        ring_second(0, half)
    for half in range(2):
        ring_last(0, half)
        if half == 0:
            own = p_ref[:, x, :, 0:512]
        else:
            own = p_ref[y, :, :, 512:1024]
        sum1[half] = (near1[half, 0] + own) + near1[half, 1]
        ring_first(1, half)
    for half in range(2):
        ring_second(1, half)
    mine = []
    for half in range(2):
        ring_last(1, half)
        own = sum1[half, y if half == 0 else x]
        mine.append((near2[half, 0] + own) + near2[half, 1])

    def select(level, block, value):
        chosen = permuted(value, index_ref[level * 4 + block])
        y_ref[level, block] = chosen[:, :128]
        y_ref[level, block + 4] = chosen[:, 128:]

    def pair(ref, *place):
        return jnp.concatenate([ref[place[:-1] + (place[-1],)], ref[place[:-1] + (place[-1] + 1,)]], axis=1)

    def to_solver(level):
        for of_level, of_core, place in SOLVERS:
            if of_level != level:
                continue
            is_core = core == of_core

            @pl.when(jnp.logical_and(is_core, grp != place))
            def _():
                send(y_ref.at[level], z_ref.at[grp], z_send.at[level], z_recv.at[grp], (leaf, place)).start()

            @pl.when(jnp.logical_and(is_core, grp == place))
            def _():
                pltpu.make_async_copy(y_ref.at[level], z_ref.at[grp], z_local).start()

    def solver_end(level):
        for of_level, of_core, place in SOLVERS:
            if of_level != level:
                continue
            is_core = core == of_core

            @pl.when(jnp.logical_and(is_core, grp != place))
            def _():
                send(y_ref.at[level], z_ref.at[grp], z_send.at[level], z_recv.at[grp], (leaf, place)).wait_send()

            @pl.when(jnp.logical_and(is_core, grp == place))
            def _():
                pltpu.make_async_copy(y_ref.at[level], z_ref.at[grp], z_local).wait()
                for source_grp in range(16):
                    if source_grp != place:
                        send(
                            y_ref.at[level], z_ref.at[source_grp], z_send.at[level], z_recv.at[source_grp], (leaf, source_grp)
                        ).wait_recv()

    side = [bit(leaf, b) for b in range(4)]
    for block in range(4):
        select(0, block, mine[block // 2][:, 256 * (block % 2) : 256 * (block % 2) + 256])
    out1 = begin(send(y_ref.at[0, pl.ds(0, 4)], r1_ref, leaf_send.at[0], leaf_recv.at[0], (flip(leaf, 1), grp)))
    for i in range(2):
        select(1, 2 * side[0] + i, pair(y_ref, 0, 2 * i))
    out2 = []
    for m in (2, 3):
        out2.append(
            begin(
                send(
                    y_ref.at[1, pl.ds(2 * side[0], 2)], r2_ref.at[lax.rem(leaf, 2)],
                    leaf_send.at[m - 1], leaf_recv.at[1 + lax.rem(leaf, 2)], (flip(leaf, m), grp),
                )
            )
        )
    own2 = 2 * side[1] + side[0]
    select(2, own2, pair(y_ref, 1, 2 * side[0]))
    for m in range(4, 8):
        begin(
            send(
                y_ref.at[2, own2], r3_ref.at[lax.rem(leaf, 4)],
                leaf_send.at[m - 1], leaf_recv.at[3 + lax.rem(leaf, 4)], (flip(leaf, m), grp),
            )
        )
    own3 = 2 * side[2] + side[1]
    value = y_ref[2, own2]
    zero = jnp.zeros_like(value)
    wide = jnp.concatenate([jnp.where(side[0] == 0, value, zero), jnp.where(side[0] == 0, zero, value)], axis=1)
    placed = permuted(wide, index_ref[12 + own3])[:, :128]
    a3_ref[...] = placed[:32] + pltpu.roll(placed[32:], 64, 1)
    for m in range(8, 16):
        begin(
            send(
                a3_ref, r4_ref.at[lax.rem(leaf, 8)],
                leaf_send.at[m - 1], leaf_recv.at[7 + lax.rem(leaf, 8)], (flip(leaf, m), grp),
            )
        )
    to_solver(0)

    def arrived(ref, slot):
        send(ref, ref, leaf_send.at[0], leaf_recv.at[slot], (flip(leaf, 1), grp)).wait_recv()

    arrived(r1_ref, 0)
    for i in range(2):
        select(1, 2 * (1 - side[0]) + i, pair(r1_ref, 2 * i))
    to_solver(1)
    select(2, 2 * side[1] + 1 - side[0], pair(y_ref, 1, 2 * (1 - side[0])))
    for s in range(2):
        arrived(r2_ref.at[s], 1 + s)
    for s in range(2):
        select(2, 2 * (1 - side[1]) + s, jnp.concatenate([r2_ref[s, 0], r2_ref[s, 1]], axis=1))
    to_solver(2)
    for i in range(2):
        select(3, 2 * side[2] + i, pair(y_ref, 2, 2 * i))
    for s in range(4):
        arrived(r3_ref.at[s], 3 + s)
    for i in range(2):
        select(3, 2 * (1 - side[2]) + i, pair(r3_ref, 2 * i))
    to_solver(3)
    for i in range(2):
        select(4, 2 * side[3] + i, pair(y_ref, 3, 2 * i))
    for s in range(8):
        arrived(r4_ref.at[s], 7 + s)
    low_lanes = lax.broadcasted_iota(jnp.int32, (32, 128), 1) < 64
    joined = []
    for i in range(4):
        even, odd = r4_ref[2 * i], r4_ref[2 * i + 1]
        upper = jnp.where(low_lanes, even, odd)
        lower = pltpu.roll(jnp.where(low_lanes, odd, even), 64, 1)
        joined.append(jnp.concatenate([upper, lower], axis=0))
    for i in range(2):
        select(4, 2 * (1 - side[3]) + i, jnp.concatenate([joined[2 * i], joined[2 * i + 1]], axis=1))
    to_solver(4)
    for b in range(4):
        top_ref[:, 128 * b : 128 * b + 128] = y_ref[4, b]
    for copy in started:
        copy.wait_send()
    for level in range(5):
        solver_end(level)


def gathered(partial, index):
    dma = pltpu.SemaphoreType.DMA
    f32 = lambda *shape: pltpu.VMEM(shape, jnp.float32)
    return pl.pallas_call(
        gather_kernel,
        out_shape=(jax.ShapeDtypeStruct((16, 8, 64, 128), jnp.float32), jax.ShapeDtypeStruct((64, 512), jnp.float32)),
        in_specs=[pl.BlockSpec(memory_space=pltpu.VMEM)] * 2,
        out_specs=(pl.BlockSpec(memory_space=pl.ANY), pl.BlockSpec(memory_space=pltpu.VMEM)),
        scratch_shapes=[
            f32(2, 2, 2, 64, 512), f32(2, 2, 2, 64, 512), f32(2, 2, 4, 64, 512), f32(2, 4, 64, 512),
            f32(2, 2, 32, 512), f32(2, 2, 32, 512), f32(2, 2, 64, 512),
            f32(5, 8, 64, 128), f32(32, 128), f32(4, 64, 128), f32(2, 2, 64, 128), f32(4, 64, 128), f32(8, 32, 128),
            dma((2, 2, 2, 3)), dma((2, 2, 2, 3)), dma((15,)), dma((15,)), dma((5,)), dma((16,)), dma,
        ],
        compiler_params=pltpu.CompilerParams(collective_id=1, has_side_effects=True, vmem_limit_bytes=56 * 1024 * 1024),
    )(partial, index)


def spread_kernel(u_ref, pivot_ref, other_ref, out_ref, rows_ref, u_send, u_recv, u_local):
    leaf, grp = lax.axis_index("leaf"), lax.axis_index("grp")
    core = lax.rem(leaf, 2)
    base = leaf - core
    barrier = pltpu.get_barrier_semaphore()
    for other in range(1, 16):
        pl.semaphore_signal(barrier, inc=1, device_id=(leaf, lax.rem(grp + other, 16)), device_id_type=MESH)
    for other in range(16):
        pl.semaphore_signal(barrier, inc=1, device_id=(base + 1 - core, other), device_id_type=MESH)
    pl.semaphore_wait(barrier, 31)

    def each(level, of_core, place, act):
        def to(target_core, target, slot):
            return send(
                u_ref.at[pl.ds(32 * target, 32)], rows_ref.at[level], u_send.at[slot], u_recv.at[level],
                (base + target_core, target),
            )

        @pl.when(jnp.logical_and(core == of_core, grp == place))
        def _():
            for target in range(16):
                if target != place:
                    act(to(of_core, target, target))
                if level > 0:
                    act(to(1 - of_core, target, 16 + target))

    for level, of_core, place in SOLVERS:
        each(level, of_core, place, lambda copy: copy.start())

    for level, of_core, place in SOLVERS:
        own = jnp.logical_and(core == of_core, grp == place)

        @pl.when(own)
        def _():
            copy = pltpu.make_async_copy(u_ref.at[pl.ds(32 * place, 32)], rows_ref.at[level], u_local)
            copy.start()
            copy.wait()

        gets = jnp.logical_not(own)
        if level == 0:
            gets = jnp.logical_and(core == of_core, gets)

        @pl.when(gets)
        def _():
            send(
                u_ref.at[pl.ds(0, 32)], rows_ref.at[level], u_send.at[0], u_recv.at[level], (base + of_core, place)
            ).wait_recv()

    for level in range(5):
        at = grp * 64 + lax.broadcasted_iota(jnp.int32, (64, 512), 0)
        is_pivot = jnp.where(at == pivot_ref[level], 1.0, 0.0)
        spot = jnp.where(lax.broadcasted_iota(jnp.int32, (64, 32), 0) == other_ref[level], 1.0, 0.0)
        rest = lax.dot_general(
            spot, rows_ref[level], (((1,), (0,)), ((), ())), precision=HI, preferred_element_type=jnp.float32
        )
        out_ref[level] = is_pivot + rest
    for level, of_core, place in SOLVERS:
        each(level, of_core, place, lambda copy: copy.wait_send())


def spread(u, pivot, other):
    dma = pltpu.SemaphoreType.DMA
    return pl.pallas_call(
        spread_kernel,
        out_shape=jax.ShapeDtypeStruct((5, 64, 512), jnp.float32),
        in_specs=[pl.BlockSpec(memory_space=pltpu.VMEM)] * 3,
        out_specs=pl.BlockSpec(memory_space=pltpu.VMEM),
        scratch_shapes=[pltpu.VMEM((5, 32, 512), jnp.float32), dma((32,)), dma((5,)), dma],
        compiler_params=pltpu.CompilerParams(collective_id=2, has_side_effects=True, vmem_limit_bytes=16 * 1024 * 1024),
    )(u, pivot, other)


def is_solver():
    leaf, grp = lax.axis_index("leaf"), lax.axis_index("grp")
    core = lax.rem(leaf, 2)
    found = False
    for _, of_core, place in SOLVERS:
        found = jnp.logical_or(found, jnp.logical_and(core == of_core, grp == place))
    return found


def invert(read):
    lane = lax.broadcasted_iota(jnp.int32, (8, 128), 1)
    sub = lax.broadcasted_iota(jnp.int32, (8, 128), 0)

    def eight(_, blocks):
        blocks = list(blocks)
        for s in range(8):
            row = blocks[0][s : s + 1, :]
            scale = 1.0 / row[:, s : s + 1]
            scaled = jnp.where(lane[:1] == s, scale, row * scale)
            for i in range(16):
                rest = jnp.where(lane == s, 0.0, blocks[i])
                new = rest - blocks[i][:, s : s + 1] * scaled
                if i == 0:
                    new = jnp.where(sub == s, scaled, new)
                blocks[i] = new
        blocks = [pltpu.roll(b, 120, 1) for b in blocks]
        return tuple(blocks[1:] + blocks[:1])

    blocks = tuple(read(i) for i in range(16))
    return jnp.concatenate(lax.fori_loop(0, 16, eight, blocks), axis=0)

def dot(a, b):
    return lax.dot_general(a, b, (((1,), (0,)), ((), ())), precision=HI, preferred_element_type=jnp.float32)

def solve_kernel(z_ref, u_ref, m_ref):
    step = pl.program_id(0)

    active = is_solver()

    @pl.when(step == 0)
    def _():
        m_ref[...] = jnp.zeros_like(m_ref)
    @pl.when(active)
    def _():
        rows = []
        for g in range(4):
            rows.append(jnp.concatenate([z_ref[g, b] for b in range(8)], axis=1))
        z = jnp.concatenate(rows, axis=0)
        m_ref[...] += lax.dot_general(z, z[:, :512], (((0,), (0,)), ((), ())), precision=HI, preferred_element_type=jnp.float32)

    @pl.when(jnp.logical_and(active, step == 3))
    def _():
        for p in range(4):
            at = 128 * p
            dinv = invert(lambda i: m_ref[at + 8 * i : at + 8 * i + 8, at : at + 128])
            lead = m_ref[at : at + 128, :]
            for low in range(at + 128, 1024, 128):
                w = dot(m_ref[low : low + 128, at : at + 128], dinv)
                for q in range(4):
                    if q != p:
                        m_ref[low : low + 128, 128 * q : 128 * q + 128] -= dot(w, lead[:, 128 * q : 128 * q + 128])
                m_ref[low : low + 128, at : at + 128] = w
        u_ref[...] = m_ref[512:, :]

def solve(z):
    return pl.pallas_call(
        solve_kernel,
        grid=(4,),
        in_specs=[pl.BlockSpec((4, 8, 64, 128), lambda i: (i, 0, 0, 0))],
        out_specs=pl.BlockSpec((512, 512), lambda i: (0, 0)),
        out_shape=jax.ShapeDtypeStruct((512, 512), jnp.float32),
        scratch_shapes=[pltpu.VMEM((1024, 512), jnp.float32)],
        compiler_params=pltpu.CompilerParams(dimension_semantics=("arbitrary",), vmem_limit_bytes=60 * 1024 * 1024),
    )(z)


def orders(pivots, leaf):
    nodes = jnp.stack([32 - (32 >> level) + leaf // (1 << level) for level in range(5)])
    chosen = jnp.take(pivots, nodes, axis=0)
    local = chosen.reshape(5, 16, 32) - 64 * jnp.arange(16, dtype=jnp.int32)[:, None]
    places = jnp.arange(64, dtype=jnp.int32)
    free = jnp.logical_not((local[:, :, :, None] == places).any(2))
    before = (free[:, :, None, :] & (places[None, :] < places[:, None])).sum(-1, dtype=jnp.int32)
    slots = jnp.arange(32, dtype=jnp.int32)[:, None]
    other = jnp.where(free[:, :, None, :] & (before[:, :, None, :] == slots), places, 0).sum(-1, dtype=jnp.int32)
    shift = 64 * (jnp.arange(16, dtype=jnp.int32) % 4)[:, None]
    index = jnp.concatenate([(local + shift).reshape(20, 1, 128), (other + shift).reshape(20, 1, 128)], axis=2)
    return chosen, other, index


def on_device(front_rows, sample_matrix, pivots):
    leaf, grp = lax.axis_index("leaf"), lax.axis_index("grp")
    chosen, other, index = orders(pivots, leaf)
    partial = lax.dot_general(
        sample_matrix, front_rows, (((0,), (1,)), ((), ())), preferred_element_type=jnp.float32
    ).reshape(4, 4, 64, 1024)
    z, top = gathered(partial, index)
    u = solve(z)
    mine = lax.dynamic_index_in_dim(other, grp, 1, keepdims=True)
    bases = spread(u, chosen[:, None, :], mine)
    return (bases[:, None], top)


def solution(mesh):
    return jax.shard_map(
        on_device,
        mesh=mesh,
        in_specs=(P("leaf", "grp"), P("grp", None), P()),
        out_specs=(P(None, "leaf", "grp", None), P("grp", None)),
        check_vma=False,
    )
```

```python
import jax
import jax.numpy as jnp
from jax import lax
from jax.experimental import pallas as pl
from jax.experimental.pallas import tpu as pltpu
from jax.sharding import PartitionSpec as P

HI = lax.Precision.HIGHEST
MESH = pl.DeviceIdType.MESH
SOLVERS = ((0, 0, 0), (0, 1, 10), (1, 0, 2), (2, 1, 8), (3, 0, 5), (4, 1, 15))


def bit(value, place):
    return lax.rem(value // (1 << place), 2)


def flip(value, mask):
    for place in range(4):
        if mask >> place & 1:
            value = value + (1 << place) * (1 - 2 * bit(value, place))
    return value


def send(src, dst, send_sem, recv_sem, device):
    return pltpu.make_async_remote_copy(
        src_ref=src, dst_ref=dst, send_sem=send_sem, recv_sem=recv_sem, device_id=device, device_id_type=MESH
    )


def permuted(src, index):
    rows = src.shape[0]
    wanted = jnp.where(lax.broadcasted_iota(jnp.int32, (256, 256), 0) == index, 1.0, 0.0).astype(jnp.bfloat16)
    high = src.astype(jnp.bfloat16)
    rest = src - high.astype(jnp.float32)
    middle = rest.astype(jnp.bfloat16)
    low = (rest - middle.astype(jnp.float32)).astype(jnp.bfloat16)
    stacked = jnp.concatenate([high, middle, low], axis=0)
    out = jnp.dot(stacked, wanted, preferred_element_type=jnp.float32)
    return (out[:rows] + out[rows : 2 * rows]) + out[2 * rows :]


def gather_kernel(
    p_ref, index_ref, z_ref, top_ref,
    hop1, comb1, near1, sum1, hop2, comb2, near2, y_ref, a3_ref, r1_ref, r2_ref, r3_ref, r4_ref,
    rs_send, rs_recv, leaf_send, leaf_recv, z_send, z_recv, z_local,
):
    leaf, grp = lax.axis_index("leaf"), lax.axis_index("grp")
    y, x = grp // 4, lax.rem(grp, 4)
    core = lax.rem(leaf, 2)

    barrier = pltpu.get_barrier_semaphore()
    for other in range(1, 16):
        pl.semaphore_signal(barrier, inc=1, device_id=(leaf, lax.rem(grp + other, 16)), device_id_type=MESH)
        pl.semaphore_signal(barrier, inc=1, device_id=(lax.rem(leaf + other, 16), grp), device_id_type=MESH)
    pl.semaphore_wait(barrier, 30)

    started = []

    def begin(copy):
        copy.start()
        started.append(copy)
        return copy

    def neighbour(along_x, offset):
        if along_x:
            return (leaf, y * 4 + lax.rem(x + offset, 4))
        return (leaf, lax.rem(y + offset, 4) * 4 + x)

    def source(phase, half, chunk, sub):
        if phase == 0:
            lanes = pl.ds(512 * half, 512)
            if half == 0:
                return p_ref.at[pl.ds(2 * sub, 2), chunk, :, lanes]
            return p_ref.at[chunk, pl.ds(2 * sub, 2), :, lanes]
        return sum1.at[half, chunk, pl.ds(32 * sub, 32), :]

    def landing(phase, half, way, sub):
        if phase == 0:
            return near1.at[half, way, pl.ds(2 * sub, 2), :, :]
        return near2.at[half, way, pl.ds(32 * sub, 32), :]

    hops, combs = (hop1, hop2), (comb1, comb2)
    rings = {}

    def ring_first(phase, half):
        along_x = (phase == 0) == (half == 0)
        at = x if along_x else y
        for way in range(2):
            to = neighbour(along_x, 1 if way == 0 else 3)
            sems = lambda kind: (rs_send.at[phase, half, way, kind], rs_recv.at[phase, half, way, kind])
            rings[phase, half, way, 0] = begin(
                send(source(phase, half, lax.rem(at + 2, 4), way), hops[phase].at[half, way], *sems(0), to)
            )
        for way in range(2):
            to = neighbour(along_x, 1 if way == 0 else 3)
            sems = lambda kind: (rs_send.at[phase, half, way, kind], rs_recv.at[phase, half, way, kind])
            chunk = lax.rem(at + (1 if way == 0 else 3), 4)
            rings[phase, half, way, 1] = begin(
                send(source(phase, half, chunk, 1 - way), landing(phase, half, way, 1 - way), *sems(1), to)
            )

    def ring_second(phase, half):
        along_x = (phase == 0) == (half == 0)
        at = x if along_x else y
        for way in range(2):
            to = neighbour(along_x, 1 if way == 0 else 3)
            chunk = lax.rem(at + (1 if way == 0 else 3), 4)
            rings[phase, half, way, 0].wait_recv()
            combs[phase][half, way] = hops[phase][half, way] + source(phase, half, chunk, way)[...]
            rings[phase, half, way, 2] = begin(
                send(
                    combs[phase].at[half, way], landing(phase, half, way, way),
                    rs_send.at[phase, half, way, 2], rs_recv.at[phase, half, way, 2], to,
                )
            )

    def ring_last(phase, half):
        for way in range(2):
            for kind in (1, 2):
                rings[phase, half, way, kind].wait_recv()

    for half in range(2):
        ring_first(0, half)
    for half in range(2):
        ring_second(0, half)
    for half in range(2):
        ring_last(0, half)
        if half == 0:
            own = p_ref[:, x, :, 0:512]
        else:
            own = p_ref[y, :, :, 512:1024]
        sum1[half] = (near1[half, 0] + own) + near1[half, 1]
        ring_first(1, half)
    for half in range(2):
        ring_second(1, half)
    mine = []
    for half in range(2):
        ring_last(1, half)
        own = sum1[half, y if half == 0 else x]
        mine.append((near2[half, 0] + own) + near2[half, 1])

    def select(level, block, value):
        chosen = permuted(value, index_ref[level * 4 + block])
        y_ref[level, block] = chosen[:, :128]
        y_ref[level, block + 4] = chosen[:, 128:]

    def pair(ref, *place):
        return jnp.concatenate([ref[place[:-1] + (place[-1],)], ref[place[:-1] + (place[-1] + 1,)]], axis=1)

    def to_solver(level):
        for of_level, of_core, place in SOLVERS:
            if of_level != level:
                continue
            is_core = core == of_core

            @pl.when(jnp.logical_and(is_core, grp != place))
            def _():
                send(y_ref.at[level], z_ref.at[grp], z_send.at[level], z_recv.at[grp], (leaf, place)).start()

            @pl.when(jnp.logical_and(is_core, grp == place))
            def _():
                pltpu.make_async_copy(y_ref.at[level], z_ref.at[grp], z_local).start()

    def solver_end(level):
        for of_level, of_core, place in SOLVERS:
            if of_level != level:
                continue
            is_core = core == of_core

            @pl.when(jnp.logical_and(is_core, grp != place))
            def _():
                send(y_ref.at[level], z_ref.at[grp], z_send.at[level], z_recv.at[grp], (leaf, place)).wait_send()

            @pl.when(jnp.logical_and(is_core, grp == place))
            def _():
                pltpu.make_async_copy(y_ref.at[level], z_ref.at[grp], z_local).wait()
                for source_grp in range(16):
                    if source_grp != place:
                        send(
                            y_ref.at[level], z_ref.at[source_grp], z_send.at[level], z_recv.at[source_grp], (leaf, source_grp)
                        ).wait_recv()

    side = [bit(leaf, b) for b in range(4)]
    for block in range(4):
        select(0, block, mine[block // 2][:, 256 * (block % 2) : 256 * (block % 2) + 256])
    out1 = begin(send(y_ref.at[0, pl.ds(0, 4)], r1_ref, leaf_send.at[0], leaf_recv.at[0], (flip(leaf, 1), grp)))
    for i in range(2):
        select(1, 2 * side[0] + i, pair(y_ref, 0, 2 * i))
    out2 = []
    for m in (2, 3):
        out2.append(
            begin(
                send(
                    y_ref.at[1, pl.ds(2 * side[0], 2)], r2_ref.at[lax.rem(leaf, 2)],
                    leaf_send.at[m - 1], leaf_recv.at[1 + lax.rem(leaf, 2)], (flip(leaf, m), grp),
                )
            )
        )
    own2 = 2 * side[1] + side[0]
    select(2, own2, pair(y_ref, 1, 2 * side[0]))
    for m in range(4, 8):
        begin(
            send(
                y_ref.at[2, own2], r3_ref.at[lax.rem(leaf, 4)],
                leaf_send.at[m - 1], leaf_recv.at[3 + lax.rem(leaf, 4)], (flip(leaf, m), grp),
            )
        )
    own3 = 2 * side[2] + side[1]
    value = y_ref[2, own2]
    zero = jnp.zeros_like(value)
    wide = jnp.concatenate([jnp.where(side[0] == 0, value, zero), jnp.where(side[0] == 0, zero, value)], axis=1)
    placed = permuted(wide, index_ref[12 + own3])[:, :128]
    a3_ref[...] = placed[:32] + pltpu.roll(placed[32:], 64, 1)
    for m in range(8, 16):
        begin(
            send(
                a3_ref, r4_ref.at[lax.rem(leaf, 8)],
                leaf_send.at[m - 1], leaf_recv.at[7 + lax.rem(leaf, 8)], (flip(leaf, m), grp),
            )
        )
    to_solver(0)

    def arrived(ref, slot):
        send(ref, ref, leaf_send.at[0], leaf_recv.at[slot], (flip(leaf, 1), grp)).wait_recv()

    arrived(r1_ref, 0)
    for i in range(2):
        select(1, 2 * (1 - side[0]) + i, pair(r1_ref, 2 * i))
    to_solver(1)
    select(2, 2 * side[1] + 1 - side[0], pair(y_ref, 1, 2 * (1 - side[0])))
    for s in range(2):
        arrived(r2_ref.at[s], 1 + s)
    for s in range(2):
        select(2, 2 * (1 - side[1]) + s, jnp.concatenate([r2_ref[s, 0], r2_ref[s, 1]], axis=1))
    to_solver(2)
    for i in range(2):
        select(3, 2 * side[2] + i, pair(y_ref, 2, 2 * i))
    for s in range(4):
        arrived(r3_ref.at[s], 3 + s)
    for i in range(2):
        select(3, 2 * (1 - side[2]) + i, pair(r3_ref, 2 * i))
    to_solver(3)
    for i in range(2):
        select(4, 2 * side[3] + i, pair(y_ref, 3, 2 * i))
    for s in range(8):
        arrived(r4_ref.at[s], 7 + s)
    low_lanes = lax.broadcasted_iota(jnp.int32, (32, 128), 1) < 64
    joined = []
    for i in range(4):
        even, odd = r4_ref[2 * i], r4_ref[2 * i + 1]
        upper = jnp.where(low_lanes, even, odd)
        lower = pltpu.roll(jnp.where(low_lanes, odd, even), 64, 1)
        joined.append(jnp.concatenate([upper, lower], axis=0))
    for i in range(2):
        select(4, 2 * (1 - side[3]) + i, jnp.concatenate([joined[2 * i], joined[2 * i + 1]], axis=1))
    to_solver(4)
    for b in range(4):
        top_ref[:, 128 * b : 128 * b + 128] = y_ref[4, b]
    for copy in started:
        copy.wait_send()
    for level in range(5):
        solver_end(level)


def gathered(partial, index):
    dma = pltpu.SemaphoreType.DMA
    f32 = lambda *shape: pltpu.VMEM(shape, jnp.float32)
    return pl.pallas_call(
        gather_kernel,
        out_shape=(jax.ShapeDtypeStruct((16, 8, 64, 128), jnp.float32), jax.ShapeDtypeStruct((64, 512), jnp.float32)),
        in_specs=[pl.BlockSpec(memory_space=pltpu.VMEM)] * 2,
        out_specs=(pl.BlockSpec(memory_space=pl.ANY), pl.BlockSpec(memory_space=pltpu.VMEM)),
        scratch_shapes=[
            f32(2, 2, 2, 64, 512), f32(2, 2, 2, 64, 512), f32(2, 2, 4, 64, 512), f32(2, 4, 64, 512),
            f32(2, 2, 32, 512), f32(2, 2, 32, 512), f32(2, 2, 64, 512),
            f32(5, 8, 64, 128), f32(32, 128), f32(4, 64, 128), f32(2, 2, 64, 128), f32(4, 64, 128), f32(8, 32, 128),
            dma((2, 2, 2, 3)), dma((2, 2, 2, 3)), dma((15,)), dma((15,)), dma((5,)), dma((16,)), dma,
        ],
        compiler_params=pltpu.CompilerParams(collective_id=1, has_side_effects=True, vmem_limit_bytes=56 * 1024 * 1024),
    )(partial, index)


def spread_kernel(u_ref, pivot_ref, other_ref, out_ref, rows_ref, u_send, u_recv, u_local):
    leaf, grp = lax.axis_index("leaf"), lax.axis_index("grp")
    core = lax.rem(leaf, 2)
    base = leaf - core
    barrier = pltpu.get_barrier_semaphore()
    for other in range(1, 16):
        pl.semaphore_signal(barrier, inc=1, device_id=(leaf, lax.rem(grp + other, 16)), device_id_type=MESH)
    for other in range(16):
        pl.semaphore_signal(barrier, inc=1, device_id=(base + 1 - core, other), device_id_type=MESH)
    pl.semaphore_wait(barrier, 31)

    def each(level, of_core, place, act):
        def to(target_core, target, slot):
            return send(
                u_ref.at[pl.ds(32 * target, 32)], rows_ref.at[level], u_send.at[slot], u_recv.at[level],
                (base + target_core, target),
            )

        @pl.when(jnp.logical_and(core == of_core, grp == place))
        def _():
            for target in range(16):
                if target != place:
                    act(to(of_core, target, target))
                if level > 0:
                    act(to(1 - of_core, target, 16 + target))

    for level, of_core, place in SOLVERS:
        each(level, of_core, place, lambda copy: copy.start())

    for level, of_core, place in SOLVERS:
        own = jnp.logical_and(core == of_core, grp == place)

        @pl.when(own)
        def _():
            copy = pltpu.make_async_copy(u_ref.at[pl.ds(32 * place, 32)], rows_ref.at[level], u_local)
            copy.start()
            copy.wait()

        gets = jnp.logical_not(own)
        if level == 0:
            gets = jnp.logical_and(core == of_core, gets)

        @pl.when(gets)
        def _():
            send(
                u_ref.at[pl.ds(0, 32)], rows_ref.at[level], u_send.at[0], u_recv.at[level], (base + of_core, place)
            ).wait_recv()

    for level in range(5):
        at = grp * 64 + lax.broadcasted_iota(jnp.int32, (64, 512), 0)
        is_pivot = jnp.where(at == pivot_ref[level], 1.0, 0.0)
        spot = jnp.where(lax.broadcasted_iota(jnp.int32, (64, 32), 0) == other_ref[level], 1.0, 0.0)
        rest = lax.dot_general(
            spot, rows_ref[level], (((1,), (0,)), ((), ())), precision=HI, preferred_element_type=jnp.float32
        )
        out_ref[level] = is_pivot + rest
    for level, of_core, place in SOLVERS:
        each(level, of_core, place, lambda copy: copy.wait_send())


def spread(u, pivot, other):
    dma = pltpu.SemaphoreType.DMA
    return pl.pallas_call(
        spread_kernel,
        out_shape=jax.ShapeDtypeStruct((5, 64, 512), jnp.float32),
        in_specs=[pl.BlockSpec(memory_space=pltpu.VMEM)] * 3,
        out_specs=pl.BlockSpec(memory_space=pltpu.VMEM),
        scratch_shapes=[pltpu.VMEM((5, 32, 512), jnp.float32), dma((32,)), dma((5,)), dma],
        compiler_params=pltpu.CompilerParams(collective_id=2, has_side_effects=True, vmem_limit_bytes=16 * 1024 * 1024),
    )(u, pivot, other)


def is_solver():
    leaf, grp = lax.axis_index("leaf"), lax.axis_index("grp")
    core = lax.rem(leaf, 2)
    found = False
    for _, of_core, place in SOLVERS:
        found = jnp.logical_or(found, jnp.logical_and(core == of_core, grp == place))
    return found


def wide(value):
    return jnp.broadcast_to(value, (8, 128))


def small_inverse(columns, sub):
    columns = list(columns)
    for k in range(8):
        rows = [wide(column[k : k + 1, :]) for column in columns]
        scale = 1.0 / rows[k]
        here = sub == k
        lead = columns[k]
        for j in range(8):
            if j != k:
                row = rows[j] * scale
                columns[j] = jnp.where(here, row, columns[j] - lead * row)
        columns[k] = jnp.where(here, scale, -(lead * scale))
    return columns


def weighted(columns, rows):
    even, odd = columns[0] * rows[0], columns[1] * rows[1]
    for j in range(2, 8, 2):
        even = even + columns[j] * rows[j]
        odd = odd + columns[j + 1] * rows[j + 1]
    return even + odd


def invert(read):
    lane = lax.broadcasted_iota(jnp.int32, (8, 128), 1)
    sub = lax.broadcasted_iota(jnp.int32, (8, 128), 0)
    eye = jnp.where(lane == sub, 1.0, 0.0)

    def eight(_, blocks):
        corner = small_inverse([wide(blocks[0][:, 8 + j : 9 + j]) for j in range(8)], sub)
        columns = [[wide(block[:, 8 + j : 9 + j]) for j in range(8)] for block in blocks[1:]]
        rolled = [pltpu.roll(block, 120, 1) for block in blocks]
        top = jnp.where(lane < 8, eye, rolled[0])
        new = weighted(corner, [wide(top[j : j + 1]) for j in range(8)])
        rows = [wide(new[j : j + 1]) for j in range(8)]
        rest = [jnp.where(lane < 8, 0.0, block) - weighted(cols, rows) for cols, block in zip(columns, rolled[1:])]
        return tuple(rest + [new])

    blocks = lax.fori_loop(0, 16, eight, tuple(pltpu.roll(read(i), 8, 1) for i in range(16)))
    return jnp.concatenate([pltpu.roll(block, 120, 1) for block in blocks], axis=0)


def dot(a, b):
    return lax.dot_general(a, b, (((1,), (0,)), ((), ())), precision=HI, preferred_element_type=jnp.float32)

def solve_kernel(z_ref, u_ref, m_ref):
    step = pl.program_id(0)

    active = is_solver()

    @pl.when(step == 0)
    def _():
        m_ref[...] = jnp.zeros_like(m_ref)
    @pl.when(active)
    def _():
        rows = []
        for g in range(4):
            rows.append(jnp.concatenate([z_ref[g, b] for b in range(8)], axis=1))
        z = jnp.concatenate(rows, axis=0)
        m_ref[...] += lax.dot_general(z, z[:, :512], (((0,), (0,)), ((), ())), precision=HI, preferred_element_type=jnp.float32)

    @pl.when(jnp.logical_and(active, step == 3))
    def _():
        for p in range(4):
            at = 128 * p
            dinv = invert(lambda i: m_ref[at + 8 * i : at + 8 * i + 8, at : at + 128])
            lead = m_ref[at : at + 128, :]
            for low in range(at + 128, 1024, 128):
                w = dot(m_ref[low : low + 128, at : at + 128], dinv)
                for q in range(4):
                    if q != p:
                        m_ref[low : low + 128, 128 * q : 128 * q + 128] -= dot(w, lead[:, 128 * q : 128 * q + 128])
                m_ref[low : low + 128, at : at + 128] = w
        u_ref[...] = m_ref[512:, :]

def solve(z):
    return pl.pallas_call(
        solve_kernel,
        grid=(4,),
        in_specs=[pl.BlockSpec((4, 8, 64, 128), lambda i: (i, 0, 0, 0))],
        out_specs=pl.BlockSpec((512, 512), lambda i: (0, 0)),
        out_shape=jax.ShapeDtypeStruct((512, 512), jnp.float32),
        scratch_shapes=[pltpu.VMEM((1024, 512), jnp.float32)],
        compiler_params=pltpu.CompilerParams(dimension_semantics=("arbitrary",), vmem_limit_bytes=60 * 1024 * 1024),
    )(z)


def orders(pivots, leaf):
    nodes = jnp.stack([32 - (32 >> level) + leaf // (1 << level) for level in range(5)])
    chosen = jnp.take(pivots, nodes, axis=0)
    local = chosen.reshape(5, 16, 32) - 64 * jnp.arange(16, dtype=jnp.int32)[:, None]
    places = jnp.arange(64, dtype=jnp.int32)
    free = jnp.logical_not((local[:, :, :, None] == places).any(2))
    before = (free[:, :, None, :] & (places[None, :] < places[:, None])).sum(-1, dtype=jnp.int32)
    slots = jnp.arange(32, dtype=jnp.int32)[:, None]
    other = jnp.where(free[:, :, None, :] & (before[:, :, None, :] == slots), places, 0).sum(-1, dtype=jnp.int32)
    shift = 64 * (jnp.arange(16, dtype=jnp.int32) % 4)[:, None]
    index = jnp.concatenate([(local + shift).reshape(20, 1, 128), (other + shift).reshape(20, 1, 128)], axis=2)
    return chosen, other, index


def on_device(front_rows, sample_matrix, pivots):
    leaf, grp = lax.axis_index("leaf"), lax.axis_index("grp")
    chosen, other, index = orders(pivots, leaf)
    partial = lax.dot_general(
        sample_matrix, front_rows, (((0,), (1,)), ((), ())), preferred_element_type=jnp.float32
    ).reshape(4, 4, 64, 1024)
    z, top = gathered(partial, index)
    u = solve(z)
    mine = lax.dynamic_index_in_dim(other, grp, 1, keepdims=True)
    bases = spread(u, chosen[:, None, :], mine)
    return (bases[:, None], top)


def solution(mesh):
    return jax.shard_map(
        on_device,
        mesh=mesh,
        in_specs=(P("leaf", "grp"), P("grp", None), P()),
        out_specs=(P(None, "leaf", "grp", None), P("grp", None)),
        check_vma=False,
    )
```

```python
import jax
import jax.numpy as jnp
from jax import lax
from jax.experimental import pallas as pl
from jax.experimental.pallas import tpu as pltpu
from jax.sharding import PartitionSpec as P

HI = lax.Precision.HIGHEST
MESH = pl.DeviceIdType.MESH
SOLVERS = (
    (0, 0, 0, 0), (0, 0, 1, 10), (0, 1, 0, 2), (0, 1, 1, 8), (1, 0, 0, 5), (1, 0, 1, 15),
    (2, 1, 0, 7), (2, 1, 1, 13), (3, 0, 0, 3), (3, 0, 1, 9), (4, 1, 0, 6), (4, 1, 1, 12),
)


def bit(value, place):
    return lax.rem(value // (1 << place), 2)


def flip(value, mask):
    for place in range(4):
        if mask >> place & 1:
            value = value + (1 << place) * (1 - 2 * bit(value, place))
    return value


def send(src, dst, send_sem, recv_sem, device):
    return pltpu.make_async_remote_copy(
        src_ref=src, dst_ref=dst, send_sem=send_sem, recv_sem=recv_sem, device_id=device, device_id_type=MESH
    )


def row_of(table, node):
    rows = lax.broadcasted_iota(jnp.int32, table.shape, 0)
    return jnp.sum(jnp.where(rows == node, table, 0), axis=0, keepdims=True)


def split3(value):
    high = value.astype(jnp.bfloat16)
    rest = value - high.astype(jnp.float32)
    middle = rest.astype(jnp.bfloat16)
    low = (rest - middle.astype(jnp.float32)).astype(jnp.bfloat16)
    return jnp.concatenate([high, middle, low], axis=0)


def permuted(src, order):
    rows = src.shape[0]
    out = jnp.dot(split3(src), order, preferred_element_type=jnp.float32)
    return (out[:rows] + out[rows : 2 * rows]) + out[2 * rows :]


def one_hot_order(pivots, start):
    src = lax.broadcasted_iota(jnp.int32, (256, 128), 0)
    lane = lax.broadcasted_iota(jnp.int32, (256, 128), 1)
    chosen = jnp.where(src == pivots - start, 1.0, 0.0)
    ones = jnp.full((128, 128), 1.0, jnp.bfloat16)
    free = 1.0 - jnp.dot(chosen.astype(jnp.bfloat16), ones, preferred_element_type=jnp.float32)
    row = lax.broadcasted_iota(jnp.int32, (256, 256), 0)
    column = lax.broadcasted_iota(jnp.int32, (256, 256), 1)
    before = jnp.where(jnp.logical_and(column < row, column // 64 == row // 64), 1.0, 0.0).astype(jnp.bfloat16)
    rank = jnp.dot(before, free.astype(jnp.bfloat16), preferred_element_type=jnp.float32)
    place = rank + (32 * (src // 64)).astype(jnp.float32)
    rest = jnp.where(jnp.logical_and(free > 0.5, place == lane.astype(jnp.float32)), 1.0, 0.0)
    return chosen.astype(jnp.bfloat16), rest.astype(jnp.bfloat16)


def gather_kernel(
    front_any, sample_any, pivot_ref, z_ref, top_ref,
    front_ref, sample_ref, turned_ref, p_ref,
    hop1, comb1, near1, sum1, hop2, comb2, near2, order_ref, y_ref,
    a1_ref, a2_ref, a3_ref, r1_ref, r2_ref, r3_ref, r4_ref,
    load_sem, rs_send, rs_recv, leaf_send, leaf_recv, z_send, z_recv, z_local,
):
    leaf, grp = lax.axis_index("leaf"), lax.axis_index("grp")
    y, x = grp // 4, lax.rem(grp, 4)
    core = lax.rem(leaf, 2)
    base = leaf - core

    loads = [
        pltpu.make_async_copy(sample_any, sample_ref, load_sem.at[0]),
        pltpu.make_async_copy(front_any, front_ref, load_sem.at[1]),
    ]
    for load in loads:
        load.start()
    barrier = pltpu.get_barrier_semaphore()
    for other in range(1, 16):
        pl.semaphore_signal(barrier, inc=1, device_id=(leaf, lax.rem(grp + other, 16)), device_id_type=MESH)
        pl.semaphore_signal(barrier, inc=1, device_id=(lax.rem(leaf + other, 16), grp), device_id_type=MESH)

    started = []

    def begin(copy):
        copy.start()
        started.append(copy)
        return copy

    def neighbour(along_x, offset):
        if along_x:
            return (leaf, y * 4 + lax.rem(x + offset, 4))
        return (leaf, lax.rem(y + offset, 4) * 4 + x)

    def source(phase, stream, chunk, sub):
        half = stream % 2
        if phase == 0:
            lanes = pl.ds(512 * half + 256 * (stream // 2), 256)
            if half == 0:
                return p_ref.at[pl.ds(2 * sub, 2), chunk, :, lanes]
            return p_ref.at[chunk, pl.ds(2 * sub, 2), :, lanes]
        return sum1.at[stream, chunk, pl.ds(32 * sub, 32), :]

    def landing(phase, stream, way, sub):
        if phase == 0:
            return near1.at[stream, way, pl.ds(2 * sub, 2), :, :]
        return near2.at[stream, way, pl.ds(32 * sub, 32), :]

    hops, combs = (hop1, hop2), (comb1, comb2)
    rings = {}

    def ring(phase, stream, way, kind, src, dst):
        along_x = (phase == 0) == (stream % 2 == 0)
        to = neighbour(along_x, 1 if way == 0 else 3)
        rings[phase, stream, way, kind] = begin(
            send(src, dst, rs_send.at[phase, stream, way, kind], rs_recv.at[phase, stream, way, kind], to)
        )

    def position(phase, stream):
        return x if (phase == 0) == (stream % 2 == 0) else y

    def ring_hop(phase, stream):
        at = position(phase, stream)
        for way in range(2):
            ring(phase, stream, way, 0, source(phase, stream, lax.rem(at + 2, 4), way), hops[phase].at[stream, way])

    def ring_own(phase, stream):
        at = position(phase, stream)
        for way in range(2):
            chunk = lax.rem(at + (1 if way == 0 else 3), 4)
            ring(phase, stream, way, 1, source(phase, stream, chunk, 1 - way), landing(phase, stream, way, 1 - way))

    def ring_join(phase, stream):
        at = position(phase, stream)
        for way in range(2):
            chunk = lax.rem(at + (1 if way == 0 else 3), 4)
            rings[phase, stream, way, 0].wait_recv()
            combs[phase][stream, way] = hops[phase][stream, way] + source(phase, stream, chunk, way)[...]
            ring(phase, stream, way, 2, combs[phase].at[stream, way], landing(phase, stream, way, way))

    def ring_last(phase, stream):
        for way in range(2):
            for kind in (1, 2):
                rings[phase, stream, way, kind].wait_recv()
        half = stream % 2
        if phase == 0:
            lanes = pl.ds(512 * half + 256 * (stream // 2), 256)
            own = p_ref[:, x, :, lanes] if half == 0 else p_ref[y, :, :, lanes]
            sum1[stream] = (near1[stream, 0] + own) + near1[stream, 1]
            return None
        own = sum1[stream, position(1, stream)]
        return (near2[stream, 0] + own) + near2[stream, 1]

    loads[0].wait()
    for c in range(8):
        turned_ref[128 * c : 128 * c + 128, :] = sample_ref[:, 128 * c : 128 * c + 128].T
    loads[1].wait()
    for stream in range(4):
        low = 512 * (stream % 2) + 256 * (stream // 2)
        for c in range(4):
            product = lax.dot_general(
                turned_ref[256 * c : 256 * c + 256, :], front_ref[low : low + 256, :], (((1,), (1,)), ((), ())),
                preferred_element_type=jnp.float32,
            )
            for b in range(4):
                p_ref[c, b, :, low : low + 256] = product[64 * b : 64 * b + 64]
        if stream == 0:
            pl.semaphore_wait(barrier, 30)
        ring_hop(0, stream)
        if stream < 2:
            ring_own(0, stream)

    def orders(level, block):
        node = 32 - (32 >> level) + leaf // (1 << level)
        chosen, rest = one_hot_order(row_of(pivot_ref[:, 128 * block : 128 * block + 128], node), 256 * block)
        order_ref[4 * level + block, :, 0:128] = chosen
        order_ref[4 * level + block, :, 128:256] = rest

    for block in range(4):
        orders(0, block)
        orders(1, block)
    ring_join(0, 0)
    ring_join(0, 1)
    ring_own(0, 2)
    ring_own(0, 3)
    for block in range(4):
        orders(2, block)
        orders(3, block)
        orders(4, block)
    for stream in (0, 1):
        ring_last(0, stream)
        ring_hop(1, stream)
        ring_own(1, stream)
    ring_join(0, 2)
    ring_join(0, 3)
    ring_join(1, 0)
    ring_join(1, 1)
    for stream in (2, 3):
        ring_last(0, stream)
        ring_hop(1, stream)
        ring_own(1, stream)

    def select(level, block, value):
        chosen = permuted(value, order_ref[4 * level + block])
        y_ref[level, 2 + block] = chosen[:, :128]
        y_ref[level, block + 4 * (block // 2)] = chosen[:, 128:]

    select(0, 0, ring_last(1, 0))
    select(0, 2, ring_last(1, 1))
    ring_join(1, 2)
    ring_join(1, 3)
    select(0, 1, ring_last(1, 2))
    select(0, 3, ring_last(1, 3))

    def each_solver(level, remote, local):
        for number, (of_level, of_core, half, place) in enumerate(SOLVERS):
            if of_level != level:
                continue
            src = y_ref.at[level, pl.ds(2 * half, 6)]

            def to(slot, target):
                return send(src, z_ref.at[slot], z_send.at[number], z_recv.at[slot], (leaf, target))

            @pl.when(jnp.logical_and(core == of_core, grp != place))
            def _():
                remote(to(grp, place))

            @pl.when(jnp.logical_and(core == of_core, grp == place))
            def _():
                local(pltpu.make_async_copy(src, z_ref.at[grp], z_local), to, place)

    def to_solver(level):
        each_solver(level, lambda copy: copy.start(), lambda copy, to, place: copy.start())

    def solver_end(level):
        def collect(copy, to, place):
            copy.wait()
            for source_grp in range(16):
                if source_grp != place:
                    to(source_grp, source_grp).wait_recv()

        each_solver(level, lambda copy: copy.wait_send(), collect)

    def both(first, second):
        return jnp.concatenate([first, second], axis=1)

    up = send(y_ref.at[0, pl.ds(2, 4)], r1_ref, leaf_send.at[0], leaf_recv.at[0], (base, grp))

    @pl.when(core == 1)
    def _():
        up.start()

    def chosen_only(level, block, value):
        return permuted(value, order_ref[4 * level + block][:, :128])

    kept = []

    def share(number, src, dst_ref, slot, recv, to_core, masks, value):
        for n, mask in enumerate(masks):
            copy = send(
                src, dst_ref.at[slot], leaf_send.at[number + n], leaf_recv.at[recv + slot], (flip(base, mask) + to_core, grp)
            )
            if mask == 0:

                @pl.when(core != to_core)
                def _():
                    copy.start()

                @pl.when(core == to_core)
                def _():
                    dst_ref[slot] = value

                kept.append((copy, to_core))
            else:
                begin(copy)

    for i in range(2):
        a1_ref[i] = chosen_only(1, 2 * core + i, both(y_ref[0, 2 + 2 * i], y_ref[0, 3 + 2 * i]))
    part1 = a1_ref[...]
    share(1, a1_ref, r2_ref, lax.rem(leaf, 4), 1, 1, (2, 0), part1)
    part2 = chosen_only(2, lax.rem(leaf, 4), both(part1[0], part1[1]))
    a2_ref[...] = part2
    share(3, a2_ref, r3_ref, lax.rem(leaf, 8), 5, 0, (4, 6, 2, 0), part2)
    zero = jnp.zeros_like(part2)
    spread_out = both(jnp.where(core == 0, part2, zero), jnp.where(core == 0, zero, part2))
    placed = chosen_only(3, lax.rem(leaf, 8) // 2, spread_out)
    part3 = placed[:32] + pltpu.roll(placed[32:], 64, 1)
    a3_ref[...] = part3
    share(7, a3_ref, r4_ref, leaf, 13, 1, (8, 10, 6, 12, 14, 4, 2, 0), part3)
    to_solver(0)

    def arrived(ref, recv, slot):
        @pl.when(slot != lax.rem(leaf, ref.shape[0]))
        def _():
            send(ref.at[slot], ref.at[slot], leaf_send.at[0], leaf_recv.at[recv + slot], (base + 1 - core, grp)).wait_recv()

    @pl.when(core == 0)
    def _():
        for i in range(2):
            select(1, i, both(y_ref[0, 2 + 2 * i], y_ref[0, 3 + 2 * i]))
        send(r1_ref, r1_ref, leaf_send.at[0], leaf_recv.at[0], (base + 1, grp)).wait_recv()
        for i in range(2):
            select(1, 2 + i, both(r1_ref[2 * i], r1_ref[2 * i + 1]))

    to_solver(1)

    @pl.when(core == 1)
    def _():
        for s in range(4):
            arrived(r2_ref, 1, s)
            select(2, s, both(r2_ref[s, 0], r2_ref[s, 1]))

    to_solver(2)

    @pl.when(core == 0)
    def _():
        for s in range(4):
            arrived(r3_ref, 5, 2 * s)
            arrived(r3_ref, 5, 2 * s + 1)
            select(3, s, both(r3_ref[2 * s], r3_ref[2 * s + 1]))

    to_solver(3)

    @pl.when(core == 1)
    def _():
        low_lanes = lax.broadcasted_iota(jnp.int32, (32, 128), 1) < 64
        for s in range(16):
            arrived(r4_ref, 13, s)
        joined = []
        for i in range(8):
            even, odd = r4_ref[2 * i], r4_ref[2 * i + 1]
            upper = jnp.where(low_lanes, even, odd)
            lower = pltpu.roll(jnp.where(low_lanes, odd, even), 64, 1)
            joined.append(jnp.concatenate([upper, lower], axis=0))
        for s in range(4):
            select(4, s, both(joined[2 * s], joined[2 * s + 1]))

    to_solver(4)

    top = send(y_ref.at[4, pl.ds(2, 4)], y_ref.at[4, pl.ds(2, 4)], leaf_send.at[15], leaf_recv.at[29], (base, grp))

    @pl.when(core == 1)
    def _():
        top.start()
        up.wait_send()
        top.wait_send()

    @pl.when(core == 0)
    def _():
        top.wait_recv()

    for b in range(4):
        top_ref[:, 128 * b : 128 * b + 128] = y_ref[4, 2 + b]

    for copy, to_core in kept:

        @pl.when(core != to_core)
        def _():
            copy.wait_send()

    for copy in started:
        copy.wait_send()
    for level in range(5):
        solver_end(level)


def gathered(front_rows, sample_matrix, pivots):
    dma = pltpu.SemaphoreType.DMA
    f32 = lambda *shape: pltpu.VMEM(shape, jnp.float32)
    bf16 = lambda *shape: pltpu.VMEM(shape, jnp.bfloat16)
    anywhere = pl.BlockSpec(memory_space=pl.ANY)
    vmem = pl.BlockSpec(memory_space=pltpu.VMEM)
    return pl.pallas_call(
        gather_kernel,
        out_shape=(jax.ShapeDtypeStruct((16, 6, 64, 128), jnp.float32), jax.ShapeDtypeStruct((64, 512), jnp.float32)),
        in_specs=[anywhere, anywhere, vmem],
        out_specs=(anywhere, vmem),
        scratch_shapes=[
            bf16(1024, 1536), bf16(1536, 1024), bf16(1024, 1536), f32(4, 4, 64, 1024),
            f32(4, 2, 2, 64, 256), f32(4, 2, 2, 64, 256), f32(4, 2, 4, 64, 256), f32(4, 4, 64, 256),
            f32(4, 2, 32, 256), f32(4, 2, 32, 256), f32(4, 2, 64, 256), bf16(20, 256, 256), f32(5, 8, 64, 128),
            f32(2, 64, 128), f32(64, 128), f32(32, 128), f32(4, 64, 128), f32(4, 2, 64, 128), f32(8, 64, 128), f32(16, 32, 128),
            dma((2,)), dma((2, 4, 2, 3)), dma((2, 4, 2, 3)), dma((16,)), dma((30,)), dma((12,)), dma((16,)), dma,
        ],
        compiler_params=pltpu.CompilerParams(collective_id=1, has_side_effects=True, vmem_limit_bytes=56 * 1024 * 1024),
    )(front_rows, sample_matrix, pivots)


def solver_role():
    grp, core = lax.axis_index("grp"), lax.rem(lax.axis_index("leaf"), 2)
    active, half = 0, 0
    for _, of_core, of_half, place in SOLVERS:
        here = jnp.where(jnp.logical_and(core == of_core, grp == place), 1, 0)
        active, half = active + here, half + of_half * here
    return active > 0, half


def spread_kernel(u_ref, pivot_ref, out_ref, rows_ref, u_send, u_recv, u_local):
    leaf, grp = lax.axis_index("leaf"), lax.axis_index("grp")
    core = lax.rem(leaf, 2)
    base = leaf - core
    barrier = pltpu.get_barrier_semaphore()
    for other in range(1, 16):
        pl.semaphore_signal(barrier, inc=1, device_id=(leaf, lax.rem(grp + other, 16)), device_id_type=MESH)
    for other in range(16):
        pl.semaphore_signal(barrier, inc=1, device_id=(base + 1 - core, other), device_id_type=MESH)
    pl.semaphore_wait(barrier, 31)

    def each(level, of_core, half, place, act):
        def to(target_core, target, slot):
            return send(
                u_ref.at[pl.ds(32 * (target - 8 * half), 32)], rows_ref.at[level], u_send.at[slot], u_recv.at[level],
                (base + target_core, target),
            )

        @pl.when(jnp.logical_and(core == of_core, grp == place))
        def _():
            for target in range(8 * half, 8 * half + 8):
                if target != place:
                    act(to(of_core, target, target))
                if level > 0:
                    act(to(1 - of_core, target, 16 + target))

    for solver in SOLVERS:
        each(*solver, lambda copy: copy.start())

    before = jnp.where(
        lax.broadcasted_iota(jnp.int32, (64, 64), 1) < lax.broadcasted_iota(jnp.int32, (64, 64), 0), 1.0, 0.0
    ).astype(jnp.bfloat16)
    ones = jnp.full((512, 128), 1.0, jnp.bfloat16)
    spots = []
    for level in range(5):
        node = 32 - (32 >> level) + leaf // (1 << level)
        at = grp * 64 + lax.broadcasted_iota(jnp.int32, (64, 512), 0)
        is_pivot = jnp.where(at == row_of(pivot_ref[...], node), 1.0, 0.0)
        out_ref[level] = is_pivot
        free = 1.0 - jnp.dot(is_pivot.astype(jnp.bfloat16), ones, preferred_element_type=jnp.float32)
        rank = jnp.dot(before, free.astype(jnp.bfloat16), preferred_element_type=jnp.float32)
        slot = lax.broadcasted_iota(jnp.int32, (64, 128), 1).astype(jnp.float32)
        spots.append(jnp.where(jnp.logical_and(free > 0.5, rank == slot), 1.0, 0.0)[:, :32])

    for level, of_core, half, place in SOLVERS:
        own = jnp.logical_and(core == of_core, grp == place)
        if place // 8 == half:

            @pl.when(own)
            def _():
                copy = pltpu.make_async_copy(u_ref.at[pl.ds(32 * (place - 8 * half), 32)], rows_ref.at[level], u_local)
                copy.start()
                copy.wait()

            gets = jnp.logical_and(grp // 8 == half, jnp.logical_not(own))
        else:
            gets = grp // 8 == half
        if level == 0:
            gets = jnp.logical_and(core == of_core, gets)

        @pl.when(gets)
        def _():
            send(
                u_ref.at[pl.ds(0, 32)], rows_ref.at[level], u_send.at[0], u_recv.at[level], (base + 1 - core, grp)
            ).wait_recv()

    for level in range(5):
        out_ref[level] += lax.dot_general(
            spots[level], rows_ref[level], (((1,), (0,)), ((), ())), precision=HI, preferred_element_type=jnp.float32
        )
    for solver in SOLVERS:
        each(*solver, lambda copy: copy.wait_send())


def spread(u, pivots):
    dma = pltpu.SemaphoreType.DMA
    return pl.pallas_call(
        spread_kernel,
        out_shape=jax.ShapeDtypeStruct((5, 64, 512), jnp.float32),
        in_specs=[pl.BlockSpec(memory_space=pltpu.VMEM)] * 2,
        out_specs=pl.BlockSpec(memory_space=pltpu.VMEM),
        scratch_shapes=[pltpu.VMEM((5, 32, 512), jnp.float32), dma((32,)), dma((5,)), dma],
        compiler_params=pltpu.CompilerParams(collective_id=2, has_side_effects=True, vmem_limit_bytes=16 * 1024 * 1024),
    )(u, pivots)


def wide(value):
    return jnp.broadcast_to(value, (8, 128))


def small_inverse(columns, sub):
    columns = list(columns)
    for k in range(8):
        rows = [wide(column[k : k + 1, :]) for column in columns]
        scale = 1.0 / rows[k]
        here = sub == k
        lead = columns[k]
        for j in range(8):
            if j != k:
                row = rows[j] * scale
                columns[j] = jnp.where(here, row, columns[j] - lead * row)
        columns[k] = jnp.where(here, scale, -(lead * scale))
    return columns


def weighted(columns, rows):
    even, odd = columns[0] * rows[0], columns[1] * rows[1]
    for j in range(2, 8, 2):
        even = even + columns[j] * rows[j]
        odd = odd + columns[j + 1] * rows[j + 1]
    return even + odd


def invert(read):
    lane = lax.broadcasted_iota(jnp.int32, (8, 128), 1)
    sub = lax.broadcasted_iota(jnp.int32, (8, 128), 0)
    eye = jnp.where(lane == sub, 1.0, 0.0)

    def eight(_, blocks):
        corner = small_inverse([wide(blocks[0][:, 8 + j : 9 + j]) for j in range(8)], sub)
        columns = [[wide(block[:, 8 + j : 9 + j]) for j in range(8)] for block in blocks[1:]]
        rolled = [pltpu.roll(block, 120, 1) for block in blocks]
        top = jnp.where(lane < 8, eye, rolled[0])
        new = weighted(corner, [wide(top[j : j + 1]) for j in range(8)])
        rows = [wide(new[j : j + 1]) for j in range(8)]
        rest = [jnp.where(lane < 8, 0.0, block) - weighted(cols, rows) for cols, block in zip(columns, rolled[1:])]
        return tuple(rest + [new])

    blocks = lax.fori_loop(0, 16, eight, tuple(pltpu.roll(read(i), 8, 1) for i in range(16)))
    return jnp.concatenate([pltpu.roll(block, 120, 1) for block in blocks], axis=0)


def dot(a, b):
    return lax.dot_general(a, b, (((1,), (0,)), ((), ())), precision=HI, preferred_element_type=jnp.float32)


def solve_kernel(z_ref, u_ref, m_ref):
    step = pl.program_id(0)
    active, half = solver_role()

    @pl.when(step == 0)
    def _():
        m_ref[...] = jnp.zeros_like(m_ref)

    @pl.when(active)
    def _():
        rows = []
        for g in range(4):
            skeleton = [z_ref[g, 2 - 2 * half + b] for b in range(4)]
            rows.append(jnp.concatenate(skeleton + [z_ref[g, 4 * half + b] for b in range(2)], axis=1))
        z = jnp.concatenate(rows, axis=0)
        m_ref[...] += lax.dot_general(
            z, z[:, :512], (((0,), (0,)), ((), ())), precision=HI, preferred_element_type=jnp.float32
        )

    @pl.when(jnp.logical_and(active, step == 3))
    def _():
        for p in range(4):
            at = 128 * p
            dinv = invert(lambda i: m_ref[at + 8 * i : at + 8 * i + 8, at : at + 128])
            lead = m_ref[at : at + 128, :]
            for low in range(at + 128, 768, 128):
                w = dot(m_ref[low : low + 128, at : at + 128], dinv)
                for q in range(4):
                    if q != p:
                        m_ref[low : low + 128, 128 * q : 128 * q + 128] -= dot(w, lead[:, 128 * q : 128 * q + 128])
                m_ref[low : low + 128, at : at + 128] = w
        u_ref[...] = m_ref[512:, :]


def solve(z):
    return pl.pallas_call(
        solve_kernel,
        grid=(4,),
        in_specs=[pl.BlockSpec((4, 6, 64, 128), lambda i: (i, 0, 0, 0))],
        out_specs=pl.BlockSpec((256, 512), lambda i: (0, 0)),
        out_shape=jax.ShapeDtypeStruct((256, 512), jnp.float32),
        scratch_shapes=[pltpu.VMEM((768, 512), jnp.float32)],
        compiler_params=pltpu.CompilerParams(dimension_semantics=("arbitrary",), vmem_limit_bytes=56 * 1024 * 1024),
    )(z)


def on_device(front_rows, sample_matrix, pivots):
    z, top = gathered(front_rows, sample_matrix, pivots)
    bases = spread(solve(z), pivots)
    return (bases[:, None], top)


def solution(mesh):
    return jax.shard_map(
        on_device,
        mesh=mesh,
        in_specs=(P("leaf", "grp"), P("grp", None), P()),
        out_specs=(P(None, "leaf", "grp", None), P("grp", None)),
        check_vma=False,
    )
```

```python
import jax
import jax.numpy as jnp
from jax import lax
from jax.experimental import pallas as pl
from jax.experimental.pallas import tpu as pltpu
from jax.sharding import PartitionSpec as P

HI = lax.Precision.HIGHEST
MESH = pl.DeviceIdType.MESH
ROOTS = ((8, 7, 5), (2, 10, 13))
LEVELS = ((0, 1, 3), (0, 2, 4))
FIRST = (
    ((4, 4, 12, 12, 8, 8, 11, 8, 8, 8, 9, 8, 8, 9, 11, 12), (1, 2, 2, 2, 3, 6, 2, 6, 1, 14, 6, 14, 3, 2, 2, 2)),
    ((7, 4, 6, 7, 7, 6, 7, 7, 11, 4, 7, 7, 3, 3, 7, 11), (6, 14, 6, 14, 11, 9, 10, 10, 9, 10, 10, 10, 9, 10, 10, 11)),
    ((5, 5, 5, 4, 5, 5, 5, 6, 9, 5, 9, 6, 1, 9, 1, 4), (13, 13, 13, 12, 1, 1, 9, 9, 13, 13, 14, 12, 13, 13, 13, 14)),
)
SLOT = (
    ((0, 1, 0, 1, 0, 0, 0, 0, 0, 0, 0, 0, 0, 1, 1, 2), (0, 0, 0, 0, 0, 0, 0, 1, 1, 0, 2, 1, 1, 0, 0, 0)),
    ((0, 0, 0, 0, 0, 1, 0, 0, 0, 1, 0, 0, 0, 1, 0, 1), (0, 0, 1, 1, 0, 0, 0, 0, 1, 0, 0, 0, 2, 0, 0, 1)),
    ((0, 0, 0, 0, 0, 0, 0, 0, 0, 0, 1, 1, 0, 2, 1, 1), (0, 0, 0, 0, 0, 1, 0, 1, 0, 0, 0, 1, 0, 0, 0, 1)),
)
PASS_ON = (
    (
        ((0, 0, 0, 0, 1, 0, 0, 0, 0, 11, 0, 7, 3, 0, 0, 0), (0, 1, 0, 5, 0, 0, 6, 0, 0, 0, 0, 0, 0, 0, 10, 0)),
        ((0, 0, 0, 0, 2, 0, 0, 0, 0, 14, 0, 15, 4, 0, 0, 0), (0, 9, 0, 13, 0, 0, 8, 0, 0, 0, 0, 0, 0, 0, 12, 0)),
        ((0, 0, 0, 0, 0, 0, 0, 0, 0, 0, 0, 0, 16, 0, 0, 0), (0, 0, 0, 0, 0, 0, 11, 0, 0, 0, 0, 0, 0, 0, 0, 0)),
    ),
    (
        ((0, 0, 0, 13, 2, 0, 3, 0, 0, 0, 0, 9, 0, 0, 0, 0), (0, 0, 0, 0, 0, 0, 1, 0, 0, 6, 0, 5, 0, 0, 2, 0)),
        ((0, 0, 0, 14, 10, 0, 6, 0, 0, 0, 0, 16, 0, 0, 0, 0), (0, 0, 0, 0, 0, 0, 3, 0, 0, 9, 0, 16, 0, 0, 4, 0)),
        ((0, 0, 0, 0, 0, 0, 0, 0, 0, 0, 0, 0, 0, 0, 0, 0), (0, 0, 0, 0, 0, 0, 0, 0, 0, 13, 0, 0, 0, 0, 0, 0)),
    ),
    (
        ((0, 13, 0, 0, 4, 0, 8, 0, 0, 9, 0, 0, 0, 0, 0, 0), (0, 5, 0, 0, 0, 0, 0, 0, 0, 7, 0, 0, 4, 0, 11, 0)),
        ((0, 15, 0, 0, 16, 0, 12, 0, 0, 11, 0, 0, 0, 0, 0, 0), (0, 6, 0, 0, 0, 0, 0, 0, 0, 8, 0, 0, 12, 0, 16, 0)),
        ((0, 0, 0, 0, 0, 0, 0, 0, 0, 14, 0, 0, 0, 0, 0, 0), (0, 0, 0, 0, 0, 0, 0, 0, 0, 0, 0, 0, 0, 0, 0, 0)),
    ),
)


def lookup(table, core, grp):
    at, value = 16 * core + grp, 0
    for position, entry in enumerate(table[0] + table[1]):
        if entry:
            value = value + jnp.where(at == position, entry, 0)
    return value


def roles():
    grp, core = lax.axis_index("grp"), lax.rem(lax.axis_index("leaf"), 2)
    main, twin = 0, 0
    for of_core in range(2):
        for root in ROOTS[of_core]:
            here = jnp.where(grp == root, 1, 0)
            main = main + here * jnp.where(core == of_core, 1, 0)
            twin = twin + here * jnp.where(core == of_core, 0, 1)
    return main, twin


def bit(value, place):
    return lax.rem(value // (1 << place), 2)


def flip(value, mask):
    for place in range(4):
        if mask >> place & 1:
            value = value + (1 << place) * (1 - 2 * bit(value, place))
    return value


def send(src, dst, send_sem, recv_sem, device):
    return pltpu.make_async_remote_copy(
        src_ref=src, dst_ref=dst, send_sem=send_sem, recv_sem=recv_sem, device_id=device, device_id_type=MESH
    )


def row_of(table, node):
    rows = lax.broadcasted_iota(jnp.int32, table.shape, 0)
    return jnp.sum(jnp.where(rows == node, table, 0), axis=0, keepdims=True)


def split3(value):
    high = value.astype(jnp.bfloat16)
    rest = value - high.astype(jnp.float32)
    middle = rest.astype(jnp.bfloat16)
    low = (rest - middle.astype(jnp.float32)).astype(jnp.bfloat16)
    return jnp.concatenate([high, middle, low], axis=0)


def permuted(src, order):
    rows = src.shape[0]
    out = jnp.dot(split3(src), order, preferred_element_type=jnp.float32)
    return (out[:rows] + out[rows : 2 * rows]) + out[2 * rows :]


def one_hot_order(pivots, start):
    src = lax.broadcasted_iota(jnp.int32, (256, 128), 0)
    lane = lax.broadcasted_iota(jnp.int32, (256, 128), 1)
    chosen = jnp.where(src == pivots - start, 1.0, 0.0)
    ones = jnp.full((128, 128), 1.0, jnp.bfloat16)
    free = 1.0 - jnp.dot(chosen.astype(jnp.bfloat16), ones, preferred_element_type=jnp.float32)
    row = lax.broadcasted_iota(jnp.int32, (256, 256), 0)
    column = lax.broadcasted_iota(jnp.int32, (256, 256), 1)
    before = jnp.where(jnp.logical_and(column < row, column // 64 == row // 64), 1.0, 0.0).astype(jnp.bfloat16)
    rank = jnp.dot(before, free.astype(jnp.bfloat16), preferred_element_type=jnp.float32)
    place = rank + (32 * (src // 64)).astype(jnp.float32)
    rest = jnp.where(jnp.logical_and(free > 0.5, place == lane.astype(jnp.float32)), 1.0, 0.0)
    return chosen.astype(jnp.bfloat16), rest.astype(jnp.bfloat16)


def gather_kernel(
    front_any, sample_any, pivot_ref, out_ref, top_ref,
    front_ref, sample_ref, turned_ref, p_ref,
    hop1, comb1, near1, sum1, hop2, comb2, near2, order_ref, y_ref,
    a1_ref, a2_ref, a3_ref, r1_ref, r2_ref, r3_ref, r4_ref, rt_ref, relay_ref, z_ref, m_ref, spot_ref, rows_ref,
    load_sem, rs_send, rs_recv, leaf_send, leaf_recv, y_send, relay_send, relay_recv, z_recv, z_local, twin_send, twin_recv,
    u_send, u_recv, u_onward,
):
    leaf, grp = lax.axis_index("leaf"), lax.axis_index("grp")
    y, x = grp // 4, lax.rem(grp, 4)
    core = lax.rem(leaf, 2)
    base = leaf - core

    loads = [
        pltpu.make_async_copy(sample_any, sample_ref, load_sem.at[0]),
        pltpu.make_async_copy(front_any, front_ref, load_sem.at[1]),
    ]
    for load in loads:
        load.start()
    barrier = pltpu.get_barrier_semaphore()
    for other in range(1, 16):
        pl.semaphore_signal(barrier, inc=1, device_id=(leaf, lax.rem(grp + other, 16)), device_id_type=MESH)
        pl.semaphore_signal(barrier, inc=1, device_id=(lax.rem(leaf + other, 16), grp), device_id_type=MESH)

    started = []

    def begin(copy):
        copy.start()
        started.append(copy)
        return copy

    def neighbour(along_x, offset):
        if along_x:
            return (leaf, y * 4 + lax.rem(x + offset, 4))
        return (leaf, lax.rem(y + offset, 4) * 4 + x)

    def source(phase, stream, chunk, sub):
        half = stream % 2
        if phase == 0:
            lanes = pl.ds(512 * half + 256 * (stream // 2), 256)
            if half == 0:
                return p_ref.at[pl.ds(2 * sub, 2), chunk, :, lanes]
            return p_ref.at[chunk, pl.ds(2 * sub, 2), :, lanes]
        return sum1.at[stream, chunk, pl.ds(32 * sub, 32), :]

    def landing(phase, stream, way, sub):
        if phase == 0:
            return near1.at[stream, way, pl.ds(2 * sub, 2), :, :]
        return near2.at[stream, way, pl.ds(32 * sub, 32), :]

    hops, combs = (hop1, hop2), (comb1, comb2)
    rings = {}

    def ring(phase, stream, way, kind, src, dst):
        along_x = (phase == 0) == (stream % 2 == 0)
        to = neighbour(along_x, 1 if way == 0 else 3)
        rings[phase, stream, way, kind] = begin(
            send(src, dst, rs_send.at[phase, stream, way, kind], rs_recv.at[phase, stream, way, kind], to)
        )

    def position(phase, stream):
        return x if (phase == 0) == (stream % 2 == 0) else y

    def ring_hop(phase, stream):
        at = position(phase, stream)
        for way in range(2):
            ring(phase, stream, way, 0, source(phase, stream, lax.rem(at + 2, 4), way), hops[phase].at[stream, way])

    def ring_own(phase, stream):
        at = position(phase, stream)
        for way in range(2):
            chunk = lax.rem(at + (1 if way == 0 else 3), 4)
            ring(phase, stream, way, 1, source(phase, stream, chunk, 1 - way), landing(phase, stream, way, 1 - way))

    def ring_join(phase, stream):
        at = position(phase, stream)
        for way in range(2):
            chunk = lax.rem(at + (1 if way == 0 else 3), 4)
            rings[phase, stream, way, 0].wait_recv()
            combs[phase][stream, way] = hops[phase][stream, way] + source(phase, stream, chunk, way)[...]
            ring(phase, stream, way, 2, combs[phase].at[stream, way], landing(phase, stream, way, way))

    def ring_last(phase, stream):
        for way in range(2):
            for kind in (1, 2):
                rings[phase, stream, way, kind].wait_recv()
        half = stream % 2
        if phase == 0:
            lanes = pl.ds(512 * half + 256 * (stream // 2), 256)
            own = p_ref[:, x, :, lanes] if half == 0 else p_ref[y, :, :, lanes]
            sum1[stream] = (near1[stream, 0] + own) + near1[stream, 1]
            return None
        own = sum1[stream, position(1, stream)]
        return (near2[stream, 0] + own) + near2[stream, 1]

    loads[0].wait()
    for c in range(8):
        turned_ref[128 * c : 128 * c + 128, :] = sample_ref[:, 128 * c : 128 * c + 128].T
    loads[1].wait()
    for stream in range(4):
        low = 512 * (stream % 2) + 256 * (stream // 2)
        for c in range(4):
            product = lax.dot_general(
                turned_ref[256 * c : 256 * c + 256, :], front_ref[low : low + 256, :], (((1,), (1,)), ((), ())),
                preferred_element_type=jnp.float32,
            )
            for b in range(4):
                p_ref[c, b, :, low : low + 256] = product[64 * b : 64 * b + 64]
        if stream == 0:
            pl.semaphore_wait(barrier, 30)
        ring_hop(0, stream)
        if stream < 2:
            ring_own(0, stream)

    def orders(level, block):
        node = 32 - (32 >> level) + leaf // (1 << level)
        chosen, rest = one_hot_order(row_of(pivot_ref[:, 128 * block : 128 * block + 128], node), 256 * block)
        order_ref[4 * level + block, :, 0:128] = chosen
        order_ref[4 * level + block, :, 128:256] = rest

    for block in range(4):
        orders(0, block)
        orders(1, block)
    ring_join(0, 0)
    ring_join(0, 1)
    ring_own(0, 2)
    ring_own(0, 3)
    for block in range(4):
        orders(2, block)
        orders(3, block)
        orders(4, block)
    for stream in (0, 1):
        ring_last(0, stream)
        ring_hop(1, stream)
        ring_own(1, stream)
    ring_join(0, 2)
    ring_join(0, 3)
    ring_join(1, 0)
    ring_join(1, 1)
    for stream in (2, 3):
        ring_last(0, stream)
        ring_hop(1, stream)
        ring_own(1, stream)

    def select(level, block, value):
        chosen = permuted(value, order_ref[4 * level + block])
        task = (level + 1) // 2
        y_ref[task, 2 + block] = chosen[:, :128]
        y_ref[task, block + 4 * (block // 2)] = chosen[:, 128:]

    select(0, 0, ring_last(1, 0))
    select(0, 2, ring_last(1, 1))
    ring_join(1, 2)
    ring_join(1, 3)
    select(0, 1, ring_last(1, 2))
    select(0, 3, ring_last(1, 3))

    def own_slice(task, act, local=True):
        root = ROOTS[0][task] + core * (ROOTS[1][task] - ROOTS[0][task])
        first, slot = lookup(FIRST[task], core, grp), lookup(SLOT[task], core, grp)
        src = y_ref.at[task]

        @pl.when(jnp.logical_and(first == root, grp != root))
        def _():
            act(send(src, z_ref.at[grp], y_send.at[task], z_recv.at[grp], (leaf, root)))

        @pl.when(first != root)
        def _():
            act(send(src, relay_ref.at[task, slot], y_send.at[task], relay_recv.at[task, slot], (leaf, first)))

        if local:

            @pl.when(grp == root)
            def _():
                act(pltpu.make_async_copy(src, z_ref.at[grp], z_local))

    def to_root(task):
        own_slice(task, lambda copy: copy.start())

    def pass_on(task, act):
        root = ROOTS[0][task] + core * (ROOTS[1][task] - ROOTS[0][task])
        for slot in range(3):
            source_grp = lookup(PASS_ON[task][slot], core, grp)

            @pl.when(source_grp > 0)
            def _():
                held = relay_ref.at[task, slot]
                act(
                    send(held, held, y_send.at[task], relay_recv.at[task, slot], (leaf, root)),
                    send(held, z_ref.at[source_grp - 1], relay_send.at[task, slot], z_recv.at[source_grp - 1], (leaf, root)),
                )

    def relay(task):
        def act(landed, onward):
            landed.wait_recv()
            onward.start()

        pass_on(task, act)

    def both(first, second):
        return jnp.concatenate([first, second], axis=1)

    to_root(0)
    up = send(y_ref.at[0, pl.ds(2, 4)], r1_ref, leaf_send.at[0], leaf_recv.at[0], (base, grp))

    @pl.when(core == 1)
    def _():
        up.start()

    def chosen_only(level, block, value):
        return permuted(value, order_ref[4 * level + block][:, :128])

    kept = []

    def share(number, src, dst_ref, slot, recv, to_core, masks, value):
        for n, mask in enumerate(masks):
            copy = send(
                src, dst_ref.at[slot], leaf_send.at[number + n], leaf_recv.at[recv + slot], (flip(base, mask) + to_core, grp)
            )
            if mask == 0:

                @pl.when(core != to_core)
                def _():
                    copy.start()

                @pl.when(core == to_core)
                def _():
                    dst_ref[slot] = value

                kept.append((copy, to_core))
            else:
                begin(copy)

    for i in range(2):
        a1_ref[i] = chosen_only(1, 2 * core + i, both(y_ref[0, 2 + 2 * i], y_ref[0, 3 + 2 * i]))
    part1 = a1_ref[...]
    share(1, a1_ref, r2_ref, lax.rem(leaf, 4), 1, 1, (2, 0), part1)
    part2 = chosen_only(2, lax.rem(leaf, 4), both(part1[0], part1[1]))
    a2_ref[...] = part2
    share(3, a2_ref, r3_ref, lax.rem(leaf, 8), 5, 0, (4, 6, 2, 0), part2)
    zero = jnp.zeros_like(part2)
    spread_out = both(jnp.where(core == 0, part2, zero), jnp.where(core == 0, zero, part2))
    placed = chosen_only(3, lax.rem(leaf, 8) // 2, spread_out)
    part3 = placed[:32] + pltpu.roll(placed[32:], 64, 1)
    a3_ref[...] = part3
    share(7, a3_ref, r4_ref, leaf, 13, 1, (8, 10, 6, 12, 14, 4, 2, 0), part3)

    def arrived(ref, recv, slot):
        @pl.when(slot != lax.rem(leaf, ref.shape[0]))
        def _():
            send(ref.at[slot], ref.at[slot], leaf_send.at[0], leaf_recv.at[recv + slot], (base + 1 - core, grp)).wait_recv()

    @pl.when(core == 0)
    def _():
        for i in range(2):
            select(1, i, both(y_ref[0, 2 + 2 * i], y_ref[0, 3 + 2 * i]))
        send(r1_ref, r1_ref, leaf_send.at[0], leaf_recv.at[0], (base + 1, grp)).wait_recv()
        for i in range(2):
            select(1, 2 + i, both(r1_ref[2 * i], r1_ref[2 * i + 1]))

    @pl.when(core == 1)
    def _():
        for s in range(4):
            arrived(r2_ref, 1, s)
            select(2, s, both(r2_ref[s, 0], r2_ref[s, 1]))

    to_root(1)
    relay(0)

    @pl.when(core == 0)
    def _():
        for s in range(4):
            arrived(r3_ref, 5, 2 * s)
            arrived(r3_ref, 5, 2 * s + 1)
            select(3, s, both(r3_ref[2 * s], r3_ref[2 * s + 1]))

    @pl.when(core == 1)
    def _():
        low_lanes = lax.broadcasted_iota(jnp.int32, (32, 128), 1) < 64
        for s in range(16):
            arrived(r4_ref, 13, s)
        joined = []
        for i in range(8):
            even, odd = r4_ref[2 * i], r4_ref[2 * i + 1]
            upper = jnp.where(low_lanes, even, odd)
            lower = pltpu.roll(jnp.where(low_lanes, odd, even), 64, 1)
            joined.append(jnp.concatenate([upper, lower], axis=0))
        for s in range(4):
            select(4, s, both(joined[2 * s], joined[2 * s + 1]))

    to_root(2)
    relay(1)
    relay(2)

    top = send(y_ref.at[2, pl.ds(2, 4)], rt_ref, leaf_send.at[15], leaf_recv.at[29], (base, grp))

    @pl.when(core == 1)
    def _():
        top.start()

    earlier = jnp.where(
        lax.broadcasted_iota(jnp.int32, (64, 64), 1) < lax.broadcasted_iota(jnp.int32, (64, 64), 0), 1.0, 0.0
    ).astype(jnp.bfloat16)
    ones = jnp.full((512, 128), 1.0, jnp.bfloat16)
    for level in range(5):
        node = 32 - (32 >> level) + leaf // (1 << level)
        place = grp * 64 + lax.broadcasted_iota(jnp.int32, (64, 512), 0)
        is_pivot = jnp.where(place == row_of(pivot_ref[...], node), 1.0, 0.0)
        out_ref[level] = is_pivot
        free = 1.0 - jnp.dot(is_pivot.astype(jnp.bfloat16), ones, preferred_element_type=jnp.float32)
        rank = jnp.dot(earlier, free.astype(jnp.bfloat16), preferred_element_type=jnp.float32)
        lane = lax.broadcasted_iota(jnp.int32, (64, 128), 1).astype(jnp.float32)
        spot_ref[level] = jnp.where(jnp.logical_and(free > 0.5, rank == lane), 1.0, 0.0)

    is_main, is_twin = roles()
    twin_leaf = base + 1 - core
    coming = ((0, 0), (0, 1), (0, 3), (1, 0), (3, 0), (0, 2), (2, 0), (1, 1), (1, 3), (3, 1), (3, 3), (1, 2), (3, 2), (2, 1), (2, 3), (2, 2))

    def to_twin(at):
        part = z_ref.at[at, pl.ds(2, 6)]
        return send(part, part, twin_send.at[at], twin_recv.at[at], (twin_leaf, grp))

    for group in range(4):
        places = [lax.rem(y + dy, 4) * 4 + lax.rem(x + dx, 4) for dy, dx in coming[4 * group : 4 * group + 4]]

        @pl.when(is_main > 0)
        def _():
            for n, at in enumerate(places):
                if group == 0 and n == 0:
                    pltpu.make_async_copy(y_ref.at[0], z_ref.at[at], z_local).wait()
                else:
                    send(y_ref.at[0], z_ref.at[at], y_send.at[0], z_recv.at[at], (twin_leaf, grp)).wait_recv()
                to_twin(at).start()

        @pl.when(is_twin > 0)
        def _():
            for at in places:
                to_twin(at).wait_recv()

        @pl.when(is_main + is_twin > 0)
        def _():
            rows = []
            for at in places:
                blocks = [z_ref[at, 2 + b] for b in range(4)] + [z_ref[at, 6 * is_twin + b] for b in range(2)]
                rows.append(jnp.concatenate(blocks, axis=1))
            z = jnp.concatenate(rows, axis=0)
            gram = lax.dot_general(
                z, z[:, :512], (((0,), (0,)), ((), ())), precision=HI, preferred_element_type=jnp.float32
            )
            if group == 0:
                m_ref[...] = gram
            else:
                m_ref[...] += gram

    @pl.when(is_main + is_twin > 0)
    def _():
        solve_in_place(m_ref)

    def each(level, of_core, half, place, to_core, act):
        @pl.when(jnp.logical_and(core == of_core, grp == place))
        def _():
            for target in range(8 * half, 8 * half + 8):
                if (target, to_core) != (place, of_core):
                    act(
                        send(
                            m_ref.at[pl.ds(512 + 32 * (target - 8 * half), 32)], rows_ref.at[level],
                            u_send.at[target], u_recv.at[level], (base + to_core, target),
                        )
                    )

    for sender in senders():
        each(*sender, lambda copy: copy.start())

    block_half = grp // 8

    def onward(level):
        return send(rows_ref.at[level], rows_ref.at[level], u_onward.at[level], u_recv.at[level], (twin_leaf, grp))

    def served_here(of_core):
        return core == of_core + block_half * (1 - 2 * of_core)

    for of_core in range(2):
        for task in range(3):
            level, root = LEVELS[of_core][task], ROOTS[of_core][task]
            direct = core == of_core if task == 0 else served_here(of_core)
            is_root = grp == root
            if task == 0:
                is_root = jnp.logical_and(is_root, block_half == 0)

            @pl.when(jnp.logical_and(direct, is_root))
            def _():
                low = 512 + 32 * (root % 8)
                rows_ref[level] = m_ref[low : low + 32, :]

            @pl.when(jnp.logical_and(direct, jnp.logical_not(is_root)))
            def _():
                onward(level).wait_recv()

            if task > 0:

                @pl.when(direct)
                def _():
                    onward(level).start()

    for of_core in range(2):
        for task in (1, 2):
            level = LEVELS[of_core][task]

            @pl.when(jnp.logical_not(served_here(of_core)))
            def _():
                onward(level).wait_recv()

    for level in range(5):
        out_ref[level] += lax.dot_general(
            spot_ref[level][:, :32], rows_ref[level], (((1,), (0,)), ((), ())),
            precision=HI, preferred_element_type=jnp.float32,
        )
    for sender in senders():
        each(*sender, lambda copy: copy.wait_send())
    for of_core in range(2):
        for task in (1, 2):
            level = LEVELS[of_core][task]

            @pl.when(served_here(of_core))
            def _():
                onward(level).wait_send()

    @pl.when(core == 1)
    def _():
        for b in range(4):
            top_ref[:, 128 * b : 128 * b + 128] = y_ref[2, 2 + b]
        up.wait_send()
        top.wait_send()

    @pl.when(core == 0)
    def _():
        top.wait_recv()
        for b in range(4):
            top_ref[:, 128 * b : 128 * b + 128] = rt_ref[b]

    @pl.when(is_main > 0)
    def _():
        for at in range(16):
            to_twin(at).wait_send()

    for copy, to_core in kept:

        @pl.when(core != to_core)
        def _():
            copy.wait_send()

    for copy in started:
        copy.wait_send()
    for task in range(3):
        own_slice(task, lambda copy: copy.wait_send(), local=False)
        pass_on(task, lambda landed, onward: onward.wait_send())


def gathered(front_rows, sample_matrix, pivots):
    dma = pltpu.SemaphoreType.DMA
    f32 = lambda *shape: pltpu.VMEM(shape, jnp.float32)
    bf16 = lambda *shape: pltpu.VMEM(shape, jnp.bfloat16)
    anywhere = pl.BlockSpec(memory_space=pl.ANY)
    vmem = pl.BlockSpec(memory_space=pltpu.VMEM)
    return pl.pallas_call(
        gather_kernel,
        out_shape=(jax.ShapeDtypeStruct((5, 64, 512), jnp.float32), jax.ShapeDtypeStruct((64, 512), jnp.float32)),
        in_specs=[anywhere, anywhere, vmem],
        out_specs=(vmem, vmem),
        scratch_shapes=[
            bf16(1024, 1536), bf16(1536, 1024), bf16(1024, 1536), f32(4, 4, 64, 1024),
            f32(4, 2, 2, 64, 256), f32(4, 2, 2, 64, 256), f32(4, 2, 4, 64, 256), f32(4, 4, 64, 256),
            f32(4, 2, 32, 256), f32(4, 2, 32, 256), f32(4, 2, 64, 256), bf16(20, 256, 256), f32(3, 8, 64, 128),
            f32(2, 64, 128), f32(64, 128), f32(32, 128), f32(4, 64, 128), f32(4, 2, 64, 128), f32(8, 64, 128), f32(16, 32, 128),
            f32(4, 64, 128), f32(3, 3, 8, 64, 128), f32(16, 8, 64, 128),
            f32(768, 512), f32(5, 64, 128), f32(5, 32, 512),
            dma((2,)), dma((2, 4, 2, 3)), dma((2, 4, 2, 3)), dma((16,)), dma((30,)),
            dma((3,)), dma((3, 3)), dma((3, 3)), dma((16,)), dma, dma((16,)), dma((16,)),
            dma((16,)), dma((5,)), dma((5,)),
        ],
        compiler_params=pltpu.CompilerParams(collective_id=1, has_side_effects=True, vmem_limit_bytes=56 * 1024 * 1024),
    )(front_rows, sample_matrix, pivots)


def senders():
    for core in range(2):
        for task in range(3):
            level, root = LEVELS[core][task], ROOTS[core][task]
            for half in range(2):
                sender = core if half == 0 else 1 - core
                yield level, sender, half, root, core if level == 0 else sender


def wide(value):
    return jnp.broadcast_to(value, (8, 128))


def small_inverse(columns, sub):
    columns = list(columns)
    for k in range(8):
        rows = [wide(column[k : k + 1, :]) for column in columns]
        scale = 1.0 / rows[k]
        here = sub == k
        lead = columns[k]
        for j in range(8):
            if j != k:
                row = rows[j] * scale
                columns[j] = jnp.where(here, row, columns[j] - lead * row)
        columns[k] = jnp.where(here, scale, -(lead * scale))
    return columns


def weighted(columns, rows):
    even, odd = columns[0] * rows[0], columns[1] * rows[1]
    for j in range(2, 8, 2):
        even = even + columns[j] * rows[j]
        odd = odd + columns[j + 1] * rows[j + 1]
    return even + odd


def invert(read):
    lane = lax.broadcasted_iota(jnp.int32, (8, 128), 1)
    sub = lax.broadcasted_iota(jnp.int32, (8, 128), 0)
    eye = jnp.where(lane == sub, 1.0, 0.0)

    def eight(_, blocks):
        corner = small_inverse([wide(blocks[0][:, 8 + j : 9 + j]) for j in range(8)], sub)
        columns = [[wide(block[:, 8 + j : 9 + j]) for j in range(8)] for block in blocks[1:]]
        rolled = [pltpu.roll(block, 120, 1) for block in blocks]
        top = jnp.where(lane < 8, eye, rolled[0])
        new = weighted(corner, [wide(top[j : j + 1]) for j in range(8)])
        rows = [wide(new[j : j + 1]) for j in range(8)]
        rest = [jnp.where(lane < 8, 0.0, block) - weighted(cols, rows) for cols, block in zip(columns, rolled[1:])]
        return tuple(rest + [new])

    blocks = lax.fori_loop(0, 16, eight, tuple(pltpu.roll(read(i), 8, 1) for i in range(16)))
    return jnp.concatenate([pltpu.roll(block, 120, 1) for block in blocks], axis=0)


def dot(a, b):
    return lax.dot_general(a, b, (((1,), (0,)), ((), ())), precision=HI, preferred_element_type=jnp.float32)


def solve_in_place(m_ref):
    for p in range(4):
        at = 128 * p
        dinv = invert(lambda i: m_ref[at + 8 * i : at + 8 * i + 8, at : at + 128])
        lead = m_ref[at : at + 128, :]
        for low in range(at + 128, 768, 128):
            w = dot(m_ref[low : low + 128, at : at + 128], dinv)
            for q in range(4):
                if q != p:
                    m_ref[low : low + 128, 128 * q : 128 * q + 128] -= dot(w, lead[:, 128 * q : 128 * q + 128])
            m_ref[low : low + 128, at : at + 128] = w


def on_device(front_rows, sample_matrix, pivots):
    bases, top = gathered(front_rows, sample_matrix, pivots)
    return (bases[:, None], top)


def solution(mesh):
    return jax.shard_map(
        on_device,
        mesh=mesh,
        in_specs=(P("leaf", "grp"), P("grp", None), P()),
        out_specs=(P(None, "leaf", "grp", None), P("grp", None)),
        check_vma=False,
    )
```

```python
import jax
import jax.numpy as jnp
from jax import lax
from jax.experimental import pallas as pl
from jax.experimental.pallas import tpu as pltpu
from jax.sharding import PartitionSpec as P

HI = lax.Precision.HIGHEST
MESH = pl.DeviceIdType.MESH
PARTS = 2
ROOTS = ((8, 7, 5), (2, 10, 13))
LEVELS = ((0, 1, 3), (0, 2, 4))
FIRST = (
    ((4, 4, 12, 12, 8, 8, 11, 8, 8, 8, 9, 8, 8, 9, 11, 12), (1, 2, 2, 2, 3, 6, 2, 6, 1, 14, 6, 14, 3, 2, 2, 2)),
    ((7, 4, 6, 7, 7, 6, 7, 7, 11, 4, 7, 7, 3, 3, 7, 11), (6, 14, 6, 14, 11, 9, 10, 10, 9, 10, 10, 10, 9, 10, 10, 11)),
    ((5, 5, 5, 4, 5, 5, 5, 6, 9, 5, 9, 6, 1, 9, 1, 4), (13, 13, 13, 12, 1, 1, 9, 9, 13, 13, 14, 12, 13, 13, 13, 14)),
)
SLOT = (
    ((0, 1, 0, 1, 0, 0, 0, 0, 0, 0, 0, 0, 0, 1, 1, 2), (0, 0, 0, 0, 0, 0, 0, 1, 1, 0, 2, 1, 1, 0, 0, 0)),
    ((0, 0, 0, 0, 0, 1, 0, 0, 0, 1, 0, 0, 0, 1, 0, 1), (0, 0, 1, 1, 0, 0, 0, 0, 1, 0, 0, 0, 2, 0, 0, 1)),
    ((0, 0, 0, 0, 0, 0, 0, 0, 0, 0, 1, 1, 0, 2, 1, 1), (0, 0, 0, 0, 0, 1, 0, 1, 0, 0, 0, 1, 0, 0, 0, 1)),
)
PASS_ON = (
    (
        ((0, 0, 0, 0, 1, 0, 0, 0, 0, 11, 0, 7, 3, 0, 0, 0), (0, 1, 0, 5, 0, 0, 6, 0, 0, 0, 0, 0, 0, 0, 10, 0)),
        ((0, 0, 0, 0, 2, 0, 0, 0, 0, 14, 0, 15, 4, 0, 0, 0), (0, 9, 0, 13, 0, 0, 8, 0, 0, 0, 0, 0, 0, 0, 12, 0)),
        ((0, 0, 0, 0, 0, 0, 0, 0, 0, 0, 0, 0, 16, 0, 0, 0), (0, 0, 0, 0, 0, 0, 11, 0, 0, 0, 0, 0, 0, 0, 0, 0)),
    ),
    (
        ((0, 0, 0, 13, 2, 0, 3, 0, 0, 0, 0, 9, 0, 0, 0, 0), (0, 0, 0, 0, 0, 0, 1, 0, 0, 6, 0, 5, 0, 0, 2, 0)),
        ((0, 0, 0, 14, 10, 0, 6, 0, 0, 0, 0, 16, 0, 0, 0, 0), (0, 0, 0, 0, 0, 0, 3, 0, 0, 9, 0, 16, 0, 0, 4, 0)),
        ((0, 0, 0, 0, 0, 0, 0, 0, 0, 0, 0, 0, 0, 0, 0, 0), (0, 0, 0, 0, 0, 0, 0, 0, 0, 13, 0, 0, 0, 0, 0, 0)),
    ),
    (
        ((0, 13, 0, 0, 4, 0, 8, 0, 0, 9, 0, 0, 0, 0, 0, 0), (0, 5, 0, 0, 0, 0, 0, 0, 0, 7, 0, 0, 4, 0, 11, 0)),
        ((0, 15, 0, 0, 16, 0, 12, 0, 0, 11, 0, 0, 0, 0, 0, 0), (0, 6, 0, 0, 0, 0, 0, 0, 0, 8, 0, 0, 12, 0, 16, 0)),
        ((0, 0, 0, 0, 0, 0, 0, 0, 0, 14, 0, 0, 0, 0, 0, 0), (0, 0, 0, 0, 0, 0, 0, 0, 0, 0, 0, 0, 0, 0, 0, 0)),
    ),
)


def lookup(table, core, grp):
    at, value = 16 * core + grp, 0
    for position, entry in enumerate(table[0] + table[1]):
        if entry:
            value = value + jnp.where(at == position, entry, 0)
    return value


def roles():
    grp, core = lax.axis_index("grp"), lax.rem(lax.axis_index("leaf"), 2)
    main, twin = 0, 0
    for of_core in range(2):
        for root in ROOTS[of_core]:
            here = jnp.where(grp == root, 1, 0)
            main = main + here * jnp.where(core == of_core, 1, 0)
            twin = twin + here * jnp.where(core == of_core, 0, 1)
    return main, twin


def bit(value, place):
    return lax.rem(value // (1 << place), 2)


def flip(value, mask):
    for place in range(4):
        if mask >> place & 1:
            value = value + (1 << place) * (1 - 2 * bit(value, place))
    return value


def send(src, dst, send_sem, recv_sem, device):
    return pltpu.make_async_remote_copy(
        src_ref=src, dst_ref=dst, send_sem=send_sem, recv_sem=recv_sem, device_id=device, device_id_type=MESH
    )


def row_of(table, node):
    rows = lax.broadcasted_iota(jnp.int32, table.shape, 0)
    return jnp.sum(jnp.where(rows == node, table, 0), axis=0, keepdims=True)


def split3(value):
    high = value.astype(jnp.bfloat16)
    rest = value - high.astype(jnp.float32)
    middle = rest.astype(jnp.bfloat16)
    low = (rest - middle.astype(jnp.float32)).astype(jnp.bfloat16)
    return jnp.concatenate([high, middle, low], axis=0)


def permuted(src, order):
    rows = src.shape[0]
    out = jnp.dot(split3(src), order, preferred_element_type=jnp.float32)
    return (out[:rows] + out[rows : 2 * rows]) + out[2 * rows :]


def one_hot_order(pivots, start):
    src = lax.broadcasted_iota(jnp.int32, (256, 128), 0)
    lane = lax.broadcasted_iota(jnp.int32, (256, 128), 1)
    chosen = jnp.where(src == pivots - start, 1.0, 0.0)
    ones = jnp.full((128, 128), 1.0, jnp.bfloat16)
    free = 1.0 - jnp.dot(chosen.astype(jnp.bfloat16), ones, preferred_element_type=jnp.float32)
    row = lax.broadcasted_iota(jnp.int32, (256, 256), 0)
    column = lax.broadcasted_iota(jnp.int32, (256, 256), 1)
    before = jnp.where(jnp.logical_and(column < row, column // 64 == row // 64), 1.0, 0.0).astype(jnp.bfloat16)
    rank = jnp.dot(before, free.astype(jnp.bfloat16), preferred_element_type=jnp.float32)
    place = rank + (32 * (src // 64)).astype(jnp.float32)
    rest = jnp.where(jnp.logical_and(free > 0.5, place == lane.astype(jnp.float32)), 1.0, 0.0)
    return chosen.astype(jnp.bfloat16), rest.astype(jnp.bfloat16)


def gather_kernel(
    front_any, sample_any, pivot_ref, out_ref, top_ref,
    front_ref, sample_ref, turned_ref, p_ref,
    hop1, comb1, near1, sum1, hop2, comb2, near2, order_ref, y_ref,
    a1_ref, a2_ref, a3_ref, r1_ref, r2_ref, r3_ref, r4_ref, rt_ref, relay_ref, z_ref, m_ref, spot_ref, rows_ref,
    load_sem, rs_send, rs_recv, leaf_send, leaf_recv, y_send, relay_send, relay_recv, z_recv, z_local, twin_send, twin_recv,
    u_send, u_recv, u_onward,
):
    leaf, grp = lax.axis_index("leaf"), lax.axis_index("grp")
    y, x = grp // 4, lax.rem(grp, 4)
    core = lax.rem(leaf, 2)
    base = leaf - core

    loads = [
        pltpu.make_async_copy(sample_any.at[pl.ds(512 * r, 512)], sample_ref.at[pl.ds(512 * r, 512)], load_sem.at[r])
        for r in range(3)
    ]
    for quarter in range(4):
        rows = pl.ds(512 * (quarter % 2) + 256 * (quarter // 2), 256)
        loads.append(pltpu.make_async_copy(front_any.at[rows], front_ref.at[rows], load_sem.at[3 + quarter]))
    for load in loads:
        load.start()
    barrier = pltpu.get_barrier_semaphore()
    for other in range(1, 16):
        pl.semaphore_signal(barrier, inc=1, device_id=(leaf, lax.rem(grp + other, 16)), device_id_type=MESH)
        pl.semaphore_signal(barrier, inc=1, device_id=(lax.rem(leaf + other, 16), grp), device_id_type=MESH)

    started = []

    def begin(copy):
        copy.start()
        started.append(copy)
        return copy

    def neighbour(along_x, offset):
        if along_x:
            return (leaf, y * 4 + lax.rem(x + offset, 4))
        return (leaf, lax.rem(y + offset, 4) * 4 + x)

    def source(phase, stream, chunk, sub):
        half = stream % 2
        if phase == 0:
            lanes = pl.ds(512 * half + 256 * (stream // 2), 256)
            if half == 0:
                return p_ref.at[pl.ds(2 * sub, 2), chunk, :, lanes]
            return p_ref.at[chunk, pl.ds(2 * sub, 2), :, lanes]
        return sum1.at[stream, chunk, pl.ds(32 * sub, 32), :]

    def landing(phase, stream, way, sub):
        if phase == 0:
            return near1.at[stream, way, pl.ds(2 * sub, 2), :, :]
        return near2.at[stream, way, pl.ds(32 * sub, 32), :]

    hops, combs = (hop1, hop2), (comb1, comb2)
    rings = {}

    def ring(phase, stream, way, kind, src, dst):
        along_x = (phase == 0) == (stream % 2 == 0)
        to = neighbour(along_x, 1 if way == 0 else 3)
        rings[phase, stream, way, kind] = begin(
            send(src, dst, rs_send.at[phase, stream, way, kind], rs_recv.at[phase, stream, way, kind], to)
        )

    def position(phase, stream):
        return x if (phase == 0) == (stream % 2 == 0) else y

    def ring_hop(phase, stream):
        at = position(phase, stream)
        for way in range(2):
            ring(phase, stream, way, 0, source(phase, stream, lax.rem(at + 2, 4), way), hops[phase].at[stream, way])

    def ring_own(phase, stream):
        at = position(phase, stream)
        for way in range(2):
            chunk = lax.rem(at + (1 if way == 0 else 3), 4)
            ring(phase, stream, way, 1, source(phase, stream, chunk, 1 - way), landing(phase, stream, way, 1 - way))

    def ring_join(phase, stream):
        at = position(phase, stream)
        for way in range(2):
            chunk = lax.rem(at + (1 if way == 0 else 3), 4)
            rings[phase, stream, way, 0].wait_recv()
            combs[phase][stream, way] = hops[phase][stream, way] + source(phase, stream, chunk, way)[...]
            ring(phase, stream, way, 2, combs[phase].at[stream, way], landing(phase, stream, way, way))

    def ring_last(phase, stream):
        for way in range(2):
            for kind in (1, 2):
                rings[phase, stream, way, kind].wait_recv()
        half = stream % 2
        if phase == 0:
            lanes = pl.ds(512 * half + 256 * (stream // 2), 256)
            own = p_ref[:, x, :, lanes] if half == 0 else p_ref[y, :, :, lanes]
            sum1[stream] = (near1[stream, 0] + own) + near1[stream, 1]
            return None
        own = sum1[stream, position(1, stream)]
        return (near2[stream, 0] + own) + near2[stream, 1]

    for r in range(3):
        loads[r].wait()
        for c in range(8):
            turned_ref[128 * c : 128 * c + 128, 512 * r : 512 * r + 512] = sample_ref[
                512 * r : 512 * r + 512, 128 * c : 128 * c + 128
            ].T
    for quarter in range(4):
        low = 512 * (quarter % 2) + 256 * (quarter // 2)
        loads[3 + quarter].wait()
        for c in range(4):
            product = lax.dot_general(
                turned_ref[256 * c : 256 * c + 256, :], front_ref[low : low + 256, :], (((1,), (1,)), ((), ())),
                preferred_element_type=jnp.float32,
            )
            for b in range(4):
                p_ref[c, b, :, low : low + 256] = product[64 * b : 64 * b + 64]
        if quarter == 0:
            pl.semaphore_wait(barrier, 30)
        for n in range(PARTS // 2):
            stream = quarter % 2 + 2 * (PARTS // 2 * (quarter // 2) + n)
            ring_hop(0, stream)
            if stream < 2:
                ring_own(0, stream)

    def orders(level, block):
        node = 32 - (32 >> level) + leaf // (1 << level)
        chosen, rest = one_hot_order(row_of(pivot_ref[:, 128 * block : 128 * block + 128], node), 256 * block)
        order_ref[4 * level + block, :, 0:128] = chosen
        order_ref[4 * level + block, :, 128:256] = rest

    def select(level, block, value):
        chosen = permuted(value, order_ref[4 * level + block])
        task = (level + 1) // 2
        y_ref[task, 2 + block] = chosen[:, :128]
        y_ref[task, block + 4 * (block // 2)] = chosen[:, 128:]

    done = {}
    for step in range(PARTS + 3):
        if step < PARTS:
            for half in range(2):
                ring_join(0, 2 * step + half)
            if step + 1 < PARTS:
                for half in range(2):
                    ring_own(0, 2 * step + 2 + half)
        if step == 0:
            for level in range(5):
                for block in range(4):
                    orders(level, block)
        if 1 <= step <= PARTS:
            for half in range(2):
                ring_last(0, 2 * step - 2 + half)
                ring_hop(1, 2 * step - 2 + half)
                ring_own(1, 2 * step - 2 + half)
        if 2 <= step <= PARTS + 1:
            for half in range(2):
                ring_join(1, 2 * step - 4 + half)
        if step >= 3:
            part = step - 3
            for half in range(2):
                done[half, part] = ring_last(1, 2 * part + half)
            each = PARTS // 2
            if (part + 1) % each == 0:
                for half in range(2):
                    value = jnp.concatenate([done[half, part + 1 - each + n] for n in range(each)], axis=1)
                    select(0, 2 * half + part // each, value)

    def own_slice(task, act, local=True):
        root = ROOTS[0][task] + core * (ROOTS[1][task] - ROOTS[0][task])
        first, slot = lookup(FIRST[task], core, grp), lookup(SLOT[task], core, grp)
        src = y_ref.at[task]

        @pl.when(jnp.logical_and(first == root, grp != root))
        def _():
            act(send(src, z_ref.at[grp], y_send.at[task], z_recv.at[grp], (leaf, root)))

        @pl.when(first != root)
        def _():
            act(send(src, relay_ref.at[task, slot], y_send.at[task], relay_recv.at[task, slot], (leaf, first)))

        if local:

            @pl.when(grp == root)
            def _():
                act(pltpu.make_async_copy(src, z_ref.at[grp], z_local))

    def to_root(task):
        own_slice(task, lambda copy: copy.start())

    def pass_on(task, act):
        root = ROOTS[0][task] + core * (ROOTS[1][task] - ROOTS[0][task])
        for slot in range(3):
            source_grp = lookup(PASS_ON[task][slot], core, grp)

            @pl.when(source_grp > 0)
            def _():
                held = relay_ref.at[task, slot]
                act(
                    send(held, held, y_send.at[task], relay_recv.at[task, slot], (leaf, root)),
                    send(held, z_ref.at[source_grp - 1], relay_send.at[task, slot], z_recv.at[source_grp - 1], (leaf, root)),
                )

    def relay(task):
        def act(landed, onward):
            landed.wait_recv()
            onward.start()

        pass_on(task, act)

    def both(first, second):
        return jnp.concatenate([first, second], axis=1)

    to_root(0)
    up = send(y_ref.at[0, pl.ds(2, 4)], r1_ref, leaf_send.at[0], leaf_recv.at[0], (base, grp))

    @pl.when(core == 1)
    def _():
        up.start()

    def chosen_only(level, block, value):
        return permuted(value, order_ref[4 * level + block][:, :128])

    kept = []

    def share(number, src, dst_ref, slot, recv, to_core, masks, value):
        for n, mask in enumerate(masks):
            copy = send(
                src, dst_ref.at[slot], leaf_send.at[number + n], leaf_recv.at[recv + slot], (flip(base, mask) + to_core, grp)
            )
            if mask == 0:

                @pl.when(core != to_core)
                def _():
                    copy.start()

                @pl.when(core == to_core)
                def _():
                    dst_ref[slot] = value

                kept.append((copy, to_core))
            else:
                begin(copy)

    for i in range(2):
        a1_ref[i] = chosen_only(1, 2 * core + i, both(y_ref[0, 2 + 2 * i], y_ref[0, 3 + 2 * i]))
    part1 = a1_ref[...]
    share(1, a1_ref, r2_ref, lax.rem(leaf, 4), 1, 1, (2, 0), part1)
    part2 = chosen_only(2, lax.rem(leaf, 4), both(part1[0], part1[1]))
    a2_ref[...] = part2
    share(3, a2_ref, r3_ref, lax.rem(leaf, 8), 5, 0, (4, 6, 2, 0), part2)
    zero = jnp.zeros_like(part2)
    spread_out = both(jnp.where(core == 0, part2, zero), jnp.where(core == 0, zero, part2))
    placed = chosen_only(3, lax.rem(leaf, 8) // 2, spread_out)
    part3 = placed[:32] + pltpu.roll(placed[32:], 64, 1)
    a3_ref[...] = part3
    share(7, a3_ref, r4_ref, leaf, 13, 1, (8, 10, 6, 12, 14, 4, 2, 0), part3)

    def arrived(ref, recv, slot):
        @pl.when(slot != lax.rem(leaf, ref.shape[0]))
        def _():
            send(ref.at[slot], ref.at[slot], leaf_send.at[0], leaf_recv.at[recv + slot], (base + 1 - core, grp)).wait_recv()

    @pl.when(core == 0)
    def _():
        for i in range(2):
            select(1, i, both(y_ref[0, 2 + 2 * i], y_ref[0, 3 + 2 * i]))
        send(r1_ref, r1_ref, leaf_send.at[0], leaf_recv.at[0], (base + 1, grp)).wait_recv()
        for i in range(2):
            select(1, 2 + i, both(r1_ref[2 * i], r1_ref[2 * i + 1]))

    @pl.when(core == 1)
    def _():
        for s in range(4):
            arrived(r2_ref, 1, s)
            select(2, s, both(r2_ref[s, 0], r2_ref[s, 1]))

    to_root(1)
    relay(0)

    @pl.when(core == 0)
    def _():
        for s in range(4):
            arrived(r3_ref, 5, 2 * s)
            arrived(r3_ref, 5, 2 * s + 1)
            select(3, s, both(r3_ref[2 * s], r3_ref[2 * s + 1]))

    @pl.when(core == 1)
    def _():
        low_lanes = lax.broadcasted_iota(jnp.int32, (32, 128), 1) < 64
        for s in range(16):
            arrived(r4_ref, 13, s)
        joined = []
        for i in range(8):
            even, odd = r4_ref[2 * i], r4_ref[2 * i + 1]
            upper = jnp.where(low_lanes, even, odd)
            lower = pltpu.roll(jnp.where(low_lanes, odd, even), 64, 1)
            joined.append(jnp.concatenate([upper, lower], axis=0))
        for s in range(4):
            select(4, s, both(joined[2 * s], joined[2 * s + 1]))

    to_root(2)
    relay(1)
    relay(2)

    top = send(y_ref.at[2, pl.ds(2, 4)], rt_ref, leaf_send.at[15], leaf_recv.at[29], (base, grp))

    @pl.when(core == 1)
    def _():
        top.start()

    earlier = jnp.where(
        lax.broadcasted_iota(jnp.int32, (64, 64), 1) < lax.broadcasted_iota(jnp.int32, (64, 64), 0), 1.0, 0.0
    ).astype(jnp.bfloat16)
    ones = jnp.full((512, 128), 1.0, jnp.bfloat16)
    for level in range(5):
        node = 32 - (32 >> level) + leaf // (1 << level)
        place = grp * 64 + lax.broadcasted_iota(jnp.int32, (64, 512), 0)
        is_pivot = jnp.where(place == row_of(pivot_ref[...], node), 1.0, 0.0)
        out_ref[level] = is_pivot
        free = 1.0 - jnp.dot(is_pivot.astype(jnp.bfloat16), ones, preferred_element_type=jnp.float32)
        rank = jnp.dot(earlier, free.astype(jnp.bfloat16), preferred_element_type=jnp.float32)
        lane = lax.broadcasted_iota(jnp.int32, (64, 128), 1).astype(jnp.float32)
        spot_ref[level] = jnp.where(jnp.logical_and(free > 0.5, rank == lane), 1.0, 0.0)

    is_main, is_twin = roles()
    twin_leaf = base + 1 - core
    coming = ((0, 0), (0, 1), (0, 3), (1, 0), (3, 0), (0, 2), (2, 0), (1, 1), (1, 3), (3, 1), (3, 3), (1, 2), (3, 2), (2, 1), (2, 3), (2, 2))

    def to_twin(at):
        part = z_ref.at[at, pl.ds(2, 6)]
        return send(part, part, twin_send.at[at], twin_recv.at[at], (twin_leaf, grp))

    for group in range(4):
        places = [lax.rem(y + dy, 4) * 4 + lax.rem(x + dx, 4) for dy, dx in coming[4 * group : 4 * group + 4]]

        @pl.when(is_main > 0)
        def _():
            for n, at in enumerate(places):
                if group == 0 and n == 0:
                    pltpu.make_async_copy(y_ref.at[0], z_ref.at[at], z_local).wait()
                else:
                    send(y_ref.at[0], z_ref.at[at], y_send.at[0], z_recv.at[at], (twin_leaf, grp)).wait_recv()
                to_twin(at).start()

        @pl.when(is_twin > 0)
        def _():
            for at in places:
                to_twin(at).wait_recv()

        @pl.when(is_main + is_twin > 0)
        def _():
            rows = []
            for at in places:
                blocks = [z_ref[at, 2 + b] for b in range(4)] + [z_ref[at, 6 * is_twin + b] for b in range(2)]
                rows.append(jnp.concatenate(blocks, axis=1))
            z = jnp.concatenate(rows, axis=0)
            gram = lax.dot_general(
                z, z[:, :512], (((0,), (0,)), ((), ())), precision=HI, preferred_element_type=jnp.float32
            )
            if group == 0:
                m_ref[...] = gram
            else:
                m_ref[...] += gram

    @pl.when(is_main + is_twin > 0)
    def _():
        solve_in_place(m_ref)

    def each(level, of_core, half, place, to_core, act):
        @pl.when(jnp.logical_and(core == of_core, grp == place))
        def _():
            for target in range(8 * half, 8 * half + 8):
                if (target, to_core) != (place, of_core):
                    act(
                        send(
                            m_ref.at[pl.ds(512 + 32 * (target - 8 * half), 32)], rows_ref.at[level],
                            u_send.at[target], u_recv.at[level], (base + to_core, target),
                        )
                    )

    for sender in senders():
        each(*sender, lambda copy: copy.start())

    block_half = grp // 8

    def onward(level):
        return send(rows_ref.at[level], rows_ref.at[level], u_onward.at[level], u_recv.at[level], (twin_leaf, grp))

    def served_here(of_core):
        return core == of_core + block_half * (1 - 2 * of_core)

    for of_core in range(2):
        for task in range(3):
            level, root = LEVELS[of_core][task], ROOTS[of_core][task]
            direct = core == of_core if task == 0 else served_here(of_core)
            is_root = grp == root
            if task == 0:
                is_root = jnp.logical_and(is_root, block_half == 0)

            @pl.when(jnp.logical_and(direct, is_root))
            def _():
                low = 512 + 32 * (root % 8)
                rows_ref[level] = m_ref[low : low + 32, :]

            @pl.when(jnp.logical_and(direct, jnp.logical_not(is_root)))
            def _():
                onward(level).wait_recv()

            if task > 0:

                @pl.when(direct)
                def _():
                    onward(level).start()

    for of_core in range(2):
        for task in (1, 2):
            level = LEVELS[of_core][task]

            @pl.when(jnp.logical_not(served_here(of_core)))
            def _():
                onward(level).wait_recv()

    for level in range(5):
        spot = spot_ref[level][:, :32].astype(jnp.bfloat16)
        out_ref[level] += jnp.dot(
            jnp.concatenate([spot, spot, spot], axis=1), split3(rows_ref[level]), preferred_element_type=jnp.float32
        )
    for sender in senders():
        each(*sender, lambda copy: copy.wait_send())
    for of_core in range(2):
        for task in (1, 2):
            level = LEVELS[of_core][task]

            @pl.when(served_here(of_core))
            def _():
                onward(level).wait_send()

    @pl.when(core == 1)
    def _():
        for b in range(4):
            top_ref[:, 128 * b : 128 * b + 128] = y_ref[2, 2 + b]
        up.wait_send()
        top.wait_send()

    @pl.when(core == 0)
    def _():
        top.wait_recv()
        for b in range(4):
            top_ref[:, 128 * b : 128 * b + 128] = rt_ref[b]

    @pl.when(is_main > 0)
    def _():
        for at in range(16):
            to_twin(at).wait_send()

    for copy, to_core in kept:

        @pl.when(core != to_core)
        def _():
            copy.wait_send()

    for copy in started:
        copy.wait_send()
    for task in range(3):
        own_slice(task, lambda copy: copy.wait_send(), local=False)
        pass_on(task, lambda landed, onward: onward.wait_send())


def gathered(front_rows, sample_matrix, pivots):
    dma = pltpu.SemaphoreType.DMA
    f32 = lambda *shape: pltpu.VMEM(shape, jnp.float32)
    bf16 = lambda *shape: pltpu.VMEM(shape, jnp.bfloat16)
    anywhere = pl.BlockSpec(memory_space=pl.ANY)
    vmem = pl.BlockSpec(memory_space=pltpu.VMEM)
    return pl.pallas_call(
        gather_kernel,
        out_shape=(jax.ShapeDtypeStruct((5, 64, 512), jnp.float32), jax.ShapeDtypeStruct((64, 512), jnp.float32)),
        in_specs=[anywhere, anywhere, vmem],
        out_specs=(vmem, vmem),
        scratch_shapes=[
            bf16(1024, 1536), bf16(1536, 1024), bf16(1024, 1536), f32(4, 4, 64, 1024),
            f32(4, 2, 2, 64, 256), f32(4, 2, 2, 64, 256), f32(4, 2, 4, 64, 256), f32(4, 4, 64, 256),
            f32(4, 2, 32, 256), f32(4, 2, 32, 256), f32(4, 2, 64, 256), bf16(20, 256, 256), f32(3, 8, 64, 128),
            f32(2, 64, 128), f32(64, 128), f32(32, 128), f32(4, 64, 128), f32(4, 2, 64, 128), f32(8, 64, 128), f32(16, 32, 128),
            f32(4, 64, 128), f32(3, 3, 8, 64, 128), f32(16, 8, 64, 128),
            f32(768, 512), f32(5, 64, 128), f32(5, 32, 512),
            dma((7,)), dma((2, 4, 2, 3)), dma((2, 4, 2, 3)), dma((16,)), dma((30,)),
            dma((3,)), dma((3, 3)), dma((3, 3)), dma((16,)), dma, dma((16,)), dma((16,)),
            dma((16,)), dma((5,)), dma((5,)),
        ],
        compiler_params=pltpu.CompilerParams(collective_id=1, has_side_effects=True, vmem_limit_bytes=44 * 1024 * 1024),
    )(front_rows, sample_matrix, pivots)


def senders():
    for core in range(2):
        for task in range(3):
            level, root = LEVELS[core][task], ROOTS[core][task]
            for half in range(2):
                sender = core if half == 0 else 1 - core
                yield level, sender, half, root, core if level == 0 else sender


def wide(value):
    return jnp.broadcast_to(value, (8, 128))


def small_inverse(columns, sub):
    columns = list(columns)
    for k in range(8):
        rows = [wide(column[k : k + 1, :]) for column in columns]
        scale = 1.0 / rows[k]
        here = sub == k
        lead = columns[k]
        for j in range(8):
            if j != k:
                row = rows[j] * scale
                columns[j] = jnp.where(here, row, columns[j] - lead * row)
        columns[k] = jnp.where(here, scale, -(lead * scale))
    return columns


def weighted(columns, rows):
    even, odd = columns[0] * rows[0], columns[1] * rows[1]
    for j in range(2, 8, 2):
        even = even + columns[j] * rows[j]
        odd = odd + columns[j + 1] * rows[j + 1]
    return even + odd


def eliminate(read):
    lane = lax.broadcasted_iota(jnp.int32, (8, 128), 1)
    sub = lax.broadcasted_iota(jnp.int32, (8, 128), 0)
    eye = jnp.where(lane == sub, 1.0, 0.0)

    def eight(_, blocks):
        corner = small_inverse([wide(blocks[0][:, 8 + j : 9 + j]) for j in range(8)], sub)
        columns = [[wide(block[:, 8 + j : 9 + j]) for j in range(8)] for block in blocks[1:]]
        rolled = [pltpu.roll(block, 120, 1) for block in blocks]
        top = jnp.where(lane < 8, eye, rolled[0])
        new = weighted(corner, [wide(top[j : j + 1]) for j in range(8)])
        rows = [wide(new[j : j + 1]) for j in range(8)]
        rest = [jnp.where(lane < 8, 0.0, block) - weighted(cols, rows) for cols, block in zip(columns, rolled[1:])]
        return tuple(rest + [new])

    blocks = lax.fori_loop(0, 8, eight, tuple(pltpu.roll(read(i), 8, 1) for i in range(8)))
    return jnp.concatenate([pltpu.roll(block, 56, 1) for block in blocks], axis=0)


def invert(block):
    upper, lower = block[:64], block[64:]
    lane = lax.broadcasted_iota(jnp.int32, (64, 128), 1)
    first = eliminate(lambda i: upper[8 * i : 8 * i + 8])
    reduced = pltpu.roll(jnp.where(lane < 64, 0.0, lower) - dot(lower[:, :64], first), 64, 1)
    second = eliminate(lambda i: reduced[8 * i : 8 * i + 8])
    bottom = pltpu.roll(second, 64, 1)
    across = pltpu.roll(first, 64, 1)[:, :64]
    top = jnp.where(lane < 64, first, 0.0) - dot(across, bottom)
    return jnp.concatenate([top, bottom], axis=0)


def dot(a, b):
    return lax.dot_general(a, b, (((1,), (0,)), ((), ())), precision=HI, preferred_element_type=jnp.float32)


def dot6(a, b):
    n = a.shape[0]
    ah, am, al = (split3(a)[k * n : k * n + n] for k in range(3))
    bh, bm, bl = (split3(b)[k * 128 : k * 128 + 128] for k in range(3))
    left1 = jnp.concatenate([ah, am], axis=1)
    d = lambda u, v: jnp.dot(u, v, preferred_element_type=jnp.float32)
    small = d(left1, jnp.concatenate([bl, bm], axis=0)) + d(jnp.concatenate([al, am], axis=1), jnp.concatenate([bh, bh], axis=0))
    return small + d(jnp.concatenate([ah, ah], axis=1), jnp.concatenate([bm, bh], axis=0))


def solve_in_place(m_ref):
    for p in range(4):
        at = 128 * p
        dinv = invert(m_ref[at : at + 128, at : at + 128])
        others = [q for q in range(4) if q != p]
        lead = jnp.concatenate([m_ref[at : at + 128, 128 * q : 128 * q + 128] for q in others], axis=1)
        both_sides = dot(dinv, lead)
        change = dot6(m_ref[at + 128 :, at : at + 128], jnp.concatenate([both_sides, dinv], axis=1))
        for n, q in enumerate(others):
            m_ref[at + 128 :, 128 * q : 128 * q + 128] -= change[:, 128 * n : 128 * n + 128]
        m_ref[at + 128 :, at : at + 128] = change[:, 384:]


def on_device(front_rows, sample_matrix, pivots):
    bases, top = gathered(front_rows, sample_matrix, pivots)
    return (bases[:, None], top)


def solution(mesh):
    return jax.shard_map(
        on_device,
        mesh=mesh,
        in_specs=(P("leaf", "grp"), P("grp", None), P()),
        out_specs=(P(None, "leaf", "grp", None), P("grp", None)),
        check_vma=False,
    )
```

```python
import jax
import jax.numpy as jnp
from jax import lax
from jax.experimental import pallas as pl
from jax.experimental.pallas import tpu as pltpu
from jax.sharding import PartitionSpec as P

HI = lax.Precision.HIGHEST
MESH = pl.DeviceIdType.MESH
PARTS = 2
ROOTS = ((8, 7, 5), (2, 10, 13))
LEVELS = ((0, 1, 3), (0, 2, 4))
FIRST = (
    ((4, 4, 12, 12, 8, 8, 11, 8, 8, 8, 9, 8, 8, 9, 11, 12), (1, 2, 2, 2, 3, 6, 2, 6, 1, 14, 6, 14, 3, 2, 2, 2)),
    ((7, 4, 6, 7, 7, 6, 7, 7, 11, 4, 7, 7, 3, 3, 7, 11), (6, 14, 6, 14, 11, 9, 10, 10, 9, 10, 10, 10, 9, 10, 10, 11)),
    ((5, 5, 5, 4, 5, 5, 5, 6, 9, 5, 9, 6, 1, 9, 1, 4), (13, 13, 13, 12, 1, 1, 9, 9, 13, 13, 14, 12, 13, 13, 13, 14)),
)
SLOT = (
    ((0, 1, 0, 1, 0, 0, 0, 0, 0, 0, 0, 0, 0, 1, 1, 2), (0, 0, 0, 0, 0, 0, 0, 1, 1, 0, 2, 1, 1, 0, 0, 0)),
    ((0, 0, 0, 0, 0, 1, 0, 0, 0, 1, 0, 0, 0, 1, 0, 1), (0, 0, 1, 1, 0, 0, 0, 0, 1, 0, 0, 0, 2, 0, 0, 1)),
    ((0, 0, 0, 0, 0, 0, 0, 0, 0, 0, 1, 1, 0, 2, 1, 1), (0, 0, 0, 0, 0, 1, 0, 1, 0, 0, 0, 1, 0, 0, 0, 1)),
)
PASS_ON = (
    (
        ((0, 0, 0, 0, 1, 0, 0, 0, 0, 11, 0, 7, 3, 0, 0, 0), (0, 1, 0, 5, 0, 0, 6, 0, 0, 0, 0, 0, 0, 0, 10, 0)),
        ((0, 0, 0, 0, 2, 0, 0, 0, 0, 14, 0, 15, 4, 0, 0, 0), (0, 9, 0, 13, 0, 0, 8, 0, 0, 0, 0, 0, 0, 0, 12, 0)),
        ((0, 0, 0, 0, 0, 0, 0, 0, 0, 0, 0, 0, 16, 0, 0, 0), (0, 0, 0, 0, 0, 0, 11, 0, 0, 0, 0, 0, 0, 0, 0, 0)),
    ),
    (
        ((0, 0, 0, 13, 2, 0, 3, 0, 0, 0, 0, 9, 0, 0, 0, 0), (0, 0, 0, 0, 0, 0, 1, 0, 0, 6, 0, 5, 0, 0, 2, 0)),
        ((0, 0, 0, 14, 10, 0, 6, 0, 0, 0, 0, 16, 0, 0, 0, 0), (0, 0, 0, 0, 0, 0, 3, 0, 0, 9, 0, 16, 0, 0, 4, 0)),
        ((0, 0, 0, 0, 0, 0, 0, 0, 0, 0, 0, 0, 0, 0, 0, 0), (0, 0, 0, 0, 0, 0, 0, 0, 0, 13, 0, 0, 0, 0, 0, 0)),
    ),
    (
        ((0, 13, 0, 0, 4, 0, 8, 0, 0, 9, 0, 0, 0, 0, 0, 0), (0, 5, 0, 0, 0, 0, 0, 0, 0, 7, 0, 0, 4, 0, 11, 0)),
        ((0, 15, 0, 0, 16, 0, 12, 0, 0, 11, 0, 0, 0, 0, 0, 0), (0, 6, 0, 0, 0, 0, 0, 0, 0, 8, 0, 0, 12, 0, 16, 0)),
        ((0, 0, 0, 0, 0, 0, 0, 0, 0, 14, 0, 0, 0, 0, 0, 0), (0, 0, 0, 0, 0, 0, 0, 0, 0, 0, 0, 0, 0, 0, 0, 0)),
    ),
)


def lookup(table, core, grp):
    at, value = 16 * core + grp, 0
    for position, entry in enumerate(table[0] + table[1]):
        if entry:
            value = value + jnp.where(at == position, entry, 0)
    return value


def roles():
    grp, core = lax.axis_index("grp"), lax.rem(lax.axis_index("leaf"), 2)
    main, twin = 0, 0
    for of_core in range(2):
        for root in ROOTS[of_core]:
            here = jnp.where(grp == root, 1, 0)
            main = main + here * jnp.where(core == of_core, 1, 0)
            twin = twin + here * jnp.where(core == of_core, 0, 1)
    return main, twin


def bit(value, place):
    return lax.rem(value // (1 << place), 2)


def flip(value, mask):
    for place in range(4):
        if mask >> place & 1:
            value = value + (1 << place) * (1 - 2 * bit(value, place))
    return value


def send(src, dst, send_sem, recv_sem, device):
    return pltpu.make_async_remote_copy(
        src_ref=src, dst_ref=dst, send_sem=send_sem, recv_sem=recv_sem, device_id=device, device_id_type=MESH
    )


def row_of(table, node):
    rows = lax.broadcasted_iota(jnp.int32, table.shape, 0)
    return jnp.sum(jnp.where(rows == node, table, 0), axis=0, keepdims=True)


def split3(value):
    high = value.astype(jnp.bfloat16)
    rest = value - high.astype(jnp.float32)
    middle = rest.astype(jnp.bfloat16)
    low = (rest - middle.astype(jnp.float32)).astype(jnp.bfloat16)
    return jnp.concatenate([high, middle, low], axis=0)


def permuted(src, order):
    rows = src.shape[0]
    out = jnp.dot(split3(src), order, preferred_element_type=jnp.float32)
    return (out[:rows] + out[rows : 2 * rows]) + out[2 * rows :]


def one_hot_order(pivots, start):
    src = lax.broadcasted_iota(jnp.int32, (256, 128), 0)
    lane = lax.broadcasted_iota(jnp.int32, (256, 128), 1)
    chosen = jnp.where(src == pivots - start, 1.0, 0.0)
    ones = jnp.full((128, 128), 1.0, jnp.bfloat16)
    free = 1.0 - jnp.dot(chosen.astype(jnp.bfloat16), ones, preferred_element_type=jnp.float32)
    row = lax.broadcasted_iota(jnp.int32, (256, 256), 0)
    column = lax.broadcasted_iota(jnp.int32, (256, 256), 1)
    before = jnp.where(jnp.logical_and(column < row, column // 64 == row // 64), 1.0, 0.0).astype(jnp.bfloat16)
    rank = jnp.dot(before, free.astype(jnp.bfloat16), preferred_element_type=jnp.float32)
    place = rank + (32 * (src // 64)).astype(jnp.float32)
    rest = jnp.where(jnp.logical_and(free > 0.5, place == lane.astype(jnp.float32)), 1.0, 0.0)
    return chosen.astype(jnp.bfloat16), rest.astype(jnp.bfloat16)


def gather_kernel(
    front_any, sample_any, pivot_ref, out_ref, top_ref,
    front_ref, sample_ref, turned_ref, p_ref,
    hop1, comb1, near1, sum1, hop2, comb2, near2, order_ref, y_ref,
    a1_ref, a2_ref, a3_ref, r1_ref, r2_ref, r3_ref, r4_ref, rt_ref, relay_ref, z_ref, m_ref, spot_ref, rows_ref,
    load_sem, rs_send, rs_recv, leaf_send, leaf_recv, y_send, relay_send, relay_recv, z_recv, z_local, twin_send, twin_recv,
    u_send, u_recv, u_onward,
):
    leaf, grp = lax.axis_index("leaf"), lax.axis_index("grp")
    y, x = grp // 4, lax.rem(grp, 4)
    core = lax.rem(leaf, 2)
    base = leaf - core

    loads = [
        pltpu.make_async_copy(sample_any.at[pl.ds(512 * r, 512)], sample_ref.at[pl.ds(512 * r, 512)], load_sem.at[r])
        for r in range(3)
    ]
    for quarter in range(4):
        rows = pl.ds(512 * (quarter % 2) + 256 * (quarter // 2), 256)
        loads.append(pltpu.make_async_copy(front_any.at[rows], front_ref.at[rows], load_sem.at[3 + quarter]))
    for load in loads:
        load.start()
    barrier = pltpu.get_barrier_semaphore()
    for other in range(1, 16):
        pl.semaphore_signal(barrier, inc=1, device_id=(leaf, lax.rem(grp + other, 16)), device_id_type=MESH)
        pl.semaphore_signal(barrier, inc=1, device_id=(lax.rem(leaf + other, 16), grp), device_id_type=MESH)

    started = []

    def begin(copy):
        copy.start()
        started.append(copy)
        return copy

    def neighbour(along_x, offset):
        if along_x:
            return (leaf, y * 4 + lax.rem(x + offset, 4))
        return (leaf, lax.rem(y + offset, 4) * 4 + x)

    def source(phase, stream, chunk, sub):
        half = stream % 2
        if phase == 0:
            lanes = pl.ds(512 * half + 256 * (stream // 2), 256)
            if half == 0:
                return p_ref.at[pl.ds(2 * sub, 2), chunk, :, lanes]
            return p_ref.at[chunk, pl.ds(2 * sub, 2), :, lanes]
        return sum1.at[stream, chunk, pl.ds(32 * sub, 32), :]

    def landing(phase, stream, way, sub):
        if phase == 0:
            return near1.at[stream, way, pl.ds(2 * sub, 2), :, :]
        return near2.at[stream, way, pl.ds(32 * sub, 32), :]

    hops, combs = (hop1, hop2), (comb1, comb2)
    rings = {}

    def ring(phase, stream, way, kind, src, dst):
        along_x = (phase == 0) == (stream % 2 == 0)
        to = neighbour(along_x, 1 if way == 0 else 3)
        rings[phase, stream, way, kind] = begin(
            send(src, dst, rs_send.at[phase, stream, way, kind], rs_recv.at[phase, stream, way, kind], to)
        )

    def position(phase, stream):
        return x if (phase == 0) == (stream % 2 == 0) else y

    def ring_hop(phase, stream):
        at = position(phase, stream)
        for way in range(2):
            ring(phase, stream, way, 0, source(phase, stream, lax.rem(at + 2, 4), way), hops[phase].at[stream, way])

    def ring_own(phase, stream):
        at = position(phase, stream)
        for way in range(2):
            chunk = lax.rem(at + (1 if way == 0 else 3), 4)
            ring(phase, stream, way, 1, source(phase, stream, chunk, 1 - way), landing(phase, stream, way, 1 - way))

    def ring_join(phase, stream):
        at = position(phase, stream)
        for way in range(2):
            chunk = lax.rem(at + (1 if way == 0 else 3), 4)
            rings[phase, stream, way, 0].wait_recv()
            combs[phase][stream, way] = hops[phase][stream, way] + source(phase, stream, chunk, way)[...]
            ring(phase, stream, way, 2, combs[phase].at[stream, way], landing(phase, stream, way, way))

    def ring_last(phase, stream):
        for way in range(2):
            for kind in (1, 2):
                rings[phase, stream, way, kind].wait_recv()
        half = stream % 2
        if phase == 0:
            lanes = pl.ds(512 * half + 256 * (stream // 2), 256)
            own = p_ref[:, x, :, lanes] if half == 0 else p_ref[y, :, :, lanes]
            sum1[stream] = (near1[stream, 0] + own) + near1[stream, 1]
            return None
        own = sum1[stream, position(1, stream)]
        return (near2[stream, 0] + own) + near2[stream, 1]

    for r in range(3):
        loads[r].wait()
        for c in range(8):
            turned_ref[128 * c : 128 * c + 128, 512 * r : 512 * r + 512] = sample_ref[
                512 * r : 512 * r + 512, 128 * c : 128 * c + 128
            ].T
    for quarter in range(4):
        low = 512 * (quarter % 2) + 256 * (quarter // 2)
        loads[3 + quarter].wait()
        for c in range(4):
            product = lax.dot_general(
                turned_ref[256 * c : 256 * c + 256, :], front_ref[low : low + 256, :], (((1,), (1,)), ((), ())),
                preferred_element_type=jnp.float32,
            )
            for b in range(4):
                p_ref[c, b, :, low : low + 256] = product[64 * b : 64 * b + 64]
        if quarter == 0:
            pl.semaphore_wait(barrier, 30)
        for n in range(PARTS // 2):
            stream = quarter % 2 + 2 * (PARTS // 2 * (quarter // 2) + n)
            ring_hop(0, stream)
            if stream < 2:
                ring_own(0, stream)

    def orders(level, block):
        node = 32 - (32 >> level) + leaf // (1 << level)
        chosen, rest = one_hot_order(row_of(pivot_ref[:, 128 * block : 128 * block + 128], node), 256 * block)
        order_ref[4 * level + block, :, 0:128] = chosen
        order_ref[4 * level + block, :, 128:256] = rest

    def select(level, block, value):
        chosen = permuted(value, order_ref[4 * level + block])
        task = (level + 1) // 2
        y_ref[task, 2 + block] = chosen[:, :128]
        y_ref[task, block + 4 * (block // 2)] = chosen[:, 128:]

    done = {}
    for step in range(PARTS + 3):
        if step < PARTS:
            for half in range(2):
                ring_join(0, 2 * step + half)
            if step + 1 < PARTS:
                for half in range(2):
                    ring_own(0, 2 * step + 2 + half)
        if step == 0:
            for level in range(5):
                for block in range(4):
                    orders(level, block)
        if 1 <= step <= PARTS:
            for half in range(2):
                ring_last(0, 2 * step - 2 + half)
                ring_hop(1, 2 * step - 2 + half)
                ring_own(1, 2 * step - 2 + half)
        if 2 <= step <= PARTS + 1:
            for half in range(2):
                ring_join(1, 2 * step - 4 + half)
        if step >= 3:
            part = step - 3
            for half in range(2):
                done[half, part] = ring_last(1, 2 * part + half)
            each = PARTS // 2
            if (part + 1) % each == 0:
                for half in range(2):
                    value = jnp.concatenate([done[half, part + 1 - each + n] for n in range(each)], axis=1)
                    select(0, 2 * half + part // each, value)

    def own_slice(task, act, local=True):
        root = ROOTS[0][task] + core * (ROOTS[1][task] - ROOTS[0][task])
        first, slot = lookup(FIRST[task], core, grp), lookup(SLOT[task], core, grp)
        src = y_ref.at[task]

        @pl.when(jnp.logical_and(first == root, grp != root))
        def _():
            act(send(src, z_ref.at[grp], y_send.at[task], z_recv.at[grp], (leaf, root)))

        @pl.when(first != root)
        def _():
            act(send(src, relay_ref.at[task, slot], y_send.at[task], relay_recv.at[task, slot], (leaf, first)))

        if local:

            @pl.when(grp == root)
            def _():
                act(pltpu.make_async_copy(src, z_ref.at[grp], z_local))

    def to_root(task):
        own_slice(task, lambda copy: copy.start())

    def pass_on(task, act):
        root = ROOTS[0][task] + core * (ROOTS[1][task] - ROOTS[0][task])
        for slot in range(3):
            source_grp = lookup(PASS_ON[task][slot], core, grp)

            @pl.when(source_grp > 0)
            def _():
                held = relay_ref.at[task, slot]
                act(
                    send(held, held, y_send.at[task], relay_recv.at[task, slot], (leaf, root)),
                    send(held, z_ref.at[source_grp - 1], relay_send.at[task, slot], z_recv.at[source_grp - 1], (leaf, root)),
                )

    def relay(task):
        def act(landed, onward):
            landed.wait_recv()
            onward.start()

        pass_on(task, act)

    def both(first, second):
        return jnp.concatenate([first, second], axis=1)

    to_root(0)
    up = send(y_ref.at[0, pl.ds(2, 4)], r1_ref, leaf_send.at[0], leaf_recv.at[0], (base, grp))

    @pl.when(core == 1)
    def _():
        up.start()

    def chosen_only(level, block, value):
        return permuted(value, order_ref[4 * level + block][:, :128])

    kept = []

    def share(number, src, dst_ref, slot, recv, to_core, masks, value):
        for n, mask in enumerate(masks):
            copy = send(
                src, dst_ref.at[slot], leaf_send.at[number + n], leaf_recv.at[recv + slot], (flip(base, mask) + to_core, grp)
            )
            if mask == 0:

                @pl.when(core != to_core)
                def _():
                    copy.start()

                @pl.when(core == to_core)
                def _():
                    dst_ref[slot] = value

                kept.append((copy, to_core))
            else:
                begin(copy)

    for i in range(2):
        a1_ref[i] = chosen_only(1, 2 * core + i, both(y_ref[0, 2 + 2 * i], y_ref[0, 3 + 2 * i]))
    part1 = a1_ref[...]
    share(1, a1_ref, r2_ref, lax.rem(leaf, 4), 1, 1, (2, 0), part1)
    part2 = chosen_only(2, lax.rem(leaf, 4), both(part1[0], part1[1]))
    a2_ref[...] = part2
    share(3, a2_ref, r3_ref, lax.rem(leaf, 8), 5, 0, (4, 6, 2, 0), part2)
    zero = jnp.zeros_like(part2)
    spread_out = both(jnp.where(core == 0, part2, zero), jnp.where(core == 0, zero, part2))
    placed = chosen_only(3, lax.rem(leaf, 8) // 2, spread_out)
    part3 = placed[:32] + pltpu.roll(placed[32:], 64, 1)
    a3_ref[...] = part3
    share(7, a3_ref, r4_ref, leaf, 13, 1, (8, 10, 6, 12, 14, 4, 2, 0), part3)

    def arrived(ref, recv, slot):
        @pl.when(slot != lax.rem(leaf, ref.shape[0]))
        def _():
            send(ref.at[slot], ref.at[slot], leaf_send.at[0], leaf_recv.at[recv + slot], (base + 1 - core, grp)).wait_recv()

    @pl.when(core == 0)
    def _():
        for i in range(2):
            select(1, i, both(y_ref[0, 2 + 2 * i], y_ref[0, 3 + 2 * i]))
        send(r1_ref, r1_ref, leaf_send.at[0], leaf_recv.at[0], (base + 1, grp)).wait_recv()
        for i in range(2):
            select(1, 2 + i, both(r1_ref[2 * i], r1_ref[2 * i + 1]))

    @pl.when(core == 1)
    def _():
        for s in range(4):
            arrived(r2_ref, 1, s)
            select(2, s, both(r2_ref[s, 0], r2_ref[s, 1]))

    to_root(1)
    relay(0)

    @pl.when(core == 0)
    def _():
        for s in range(4):
            arrived(r3_ref, 5, 2 * s)
            arrived(r3_ref, 5, 2 * s + 1)
            select(3, s, both(r3_ref[2 * s], r3_ref[2 * s + 1]))

    @pl.when(core == 1)
    def _():
        low_lanes = lax.broadcasted_iota(jnp.int32, (32, 128), 1) < 64
        for s in range(16):
            arrived(r4_ref, 13, s)
        joined = []
        for i in range(8):
            even, odd = r4_ref[2 * i], r4_ref[2 * i + 1]
            upper = jnp.where(low_lanes, even, odd)
            lower = pltpu.roll(jnp.where(low_lanes, odd, even), 64, 1)
            joined.append(jnp.concatenate([upper, lower], axis=0))
        for s in range(4):
            select(4, s, both(joined[2 * s], joined[2 * s + 1]))

    to_root(2)
    relay(1)
    relay(2)

    top = send(y_ref.at[2, pl.ds(2, 4)], rt_ref, leaf_send.at[15], leaf_recv.at[29], (base, grp))

    @pl.when(core == 1)
    def _():
        top.start()

    earlier = jnp.where(
        lax.broadcasted_iota(jnp.int32, (64, 64), 1) < lax.broadcasted_iota(jnp.int32, (64, 64), 0), 1.0, 0.0
    ).astype(jnp.bfloat16)
    ones = jnp.full((512, 128), 1.0, jnp.bfloat16)
    for level in range(5):
        node = 32 - (32 >> level) + leaf // (1 << level)
        place = grp * 64 + lax.broadcasted_iota(jnp.int32, (64, 512), 0)
        is_pivot = jnp.where(place == row_of(pivot_ref[...], node), 1.0, 0.0)
        out_ref[level] = is_pivot
        free = 1.0 - jnp.dot(is_pivot.astype(jnp.bfloat16), ones, preferred_element_type=jnp.float32)
        rank = jnp.dot(earlier, free.astype(jnp.bfloat16), preferred_element_type=jnp.float32)
        lane = lax.broadcasted_iota(jnp.int32, (64, 128), 1).astype(jnp.float32)
        spot_ref[level] = jnp.where(jnp.logical_and(free > 0.5, rank == lane), 1.0, 0.0)

    is_main, is_twin = roles()
    twin_leaf = base + 1 - core
    coming = ((0, 0), (0, 1), (0, 3), (1, 0), (3, 0), (0, 2), (2, 0), (1, 1), (1, 3), (3, 1), (3, 3), (1, 2), (3, 2), (2, 1), (2, 3), (2, 2))

    def to_twin(at):
        part = z_ref.at[at, pl.ds(2, 6)]
        return send(part, part, twin_send.at[at], twin_recv.at[at], (twin_leaf, grp))

    for group in range(4):
        places = [lax.rem(y + dy, 4) * 4 + lax.rem(x + dx, 4) for dy, dx in coming[4 * group : 4 * group + 4]]

        @pl.when(is_main > 0)
        def _():
            for n, at in enumerate(places):
                if group == 0 and n == 0:
                    pltpu.make_async_copy(y_ref.at[0], z_ref.at[at], z_local).wait()
                else:
                    send(y_ref.at[0], z_ref.at[at], y_send.at[0], z_recv.at[at], (twin_leaf, grp)).wait_recv()
                to_twin(at).start()

        @pl.when(is_twin > 0)
        def _():
            for at in places:
                to_twin(at).wait_recv()

        @pl.when(is_main + is_twin > 0)
        def _():
            rows = []
            for at in places:
                blocks = [z_ref[at, 2 + b] for b in range(4)] + [z_ref[at, 6 * is_twin + b] for b in range(2)]
                rows.append(jnp.concatenate(blocks, axis=1))
            z = jnp.concatenate(rows, axis=0)
            gram = lax.dot_general(
                z, z[:, :512], (((0,), (0,)), ((), ())), precision=HI, preferred_element_type=jnp.float32
            )
            if group == 0:
                m_ref[...] = gram
            else:
                m_ref[...] += gram

    @pl.when(is_main + is_twin > 0)
    def _():
        solve_in_place(m_ref)

    def each(level, of_core, half, place, to_core, act):
        @pl.when(jnp.logical_and(core == of_core, grp == place))
        def _():
            for target in range(8 * half, 8 * half + 8):
                if (target, to_core) != (place, of_core):
                    act(
                        send(
                            m_ref.at[pl.ds(512 + 32 * (target - 8 * half), 32)], rows_ref.at[level],
                            u_send.at[target], u_recv.at[level], (base + to_core, target),
                        )
                    )

    for sender in senders():
        each(*sender, lambda copy: copy.start())

    block_half = grp // 8

    def onward(level):
        return send(rows_ref.at[level], rows_ref.at[level], u_onward.at[level], u_recv.at[level], (twin_leaf, grp))

    def served_here(of_core):
        return core == of_core + block_half * (1 - 2 * of_core)

    for of_core in range(2):
        for task in range(3):
            level, root = LEVELS[of_core][task], ROOTS[of_core][task]
            direct = core == of_core if task == 0 else served_here(of_core)
            is_root = grp == root
            if task == 0:
                is_root = jnp.logical_and(is_root, block_half == 0)

            @pl.when(jnp.logical_and(direct, is_root))
            def _():
                low = 512 + 32 * (root % 8)
                rows_ref[level] = m_ref[low : low + 32, :]

            @pl.when(jnp.logical_and(direct, jnp.logical_not(is_root)))
            def _():
                onward(level).wait_recv()

            if task > 0:

                @pl.when(direct)
                def _():
                    onward(level).start()

    for of_core in range(2):
        for task in (1, 2):
            level = LEVELS[of_core][task]

            @pl.when(jnp.logical_not(served_here(of_core)))
            def _():
                onward(level).wait_recv()

    for level in range(5):
        spot = spot_ref[level][:, :32].astype(jnp.bfloat16)
        out_ref[level] += jnp.dot(
            jnp.concatenate([spot, spot, spot], axis=1), split3(rows_ref[level]), preferred_element_type=jnp.float32
        )
    for sender in senders():
        each(*sender, lambda copy: copy.wait_send())
    for of_core in range(2):
        for task in (1, 2):
            level = LEVELS[of_core][task]

            @pl.when(served_here(of_core))
            def _():
                onward(level).wait_send()

    @pl.when(core == 1)
    def _():
        for b in range(4):
            top_ref[:, 128 * b : 128 * b + 128] = y_ref[2, 2 + b]
        up.wait_send()
        top.wait_send()

    @pl.when(core == 0)
    def _():
        top.wait_recv()
        for b in range(4):
            top_ref[:, 128 * b : 128 * b + 128] = rt_ref[b]

    @pl.when(is_main > 0)
    def _():
        for at in range(16):
            to_twin(at).wait_send()

    for copy, to_core in kept:

        @pl.when(core != to_core)
        def _():
            copy.wait_send()

    for copy in started:
        copy.wait_send()
    for task in range(3):
        own_slice(task, lambda copy: copy.wait_send(), local=False)
        pass_on(task, lambda landed, onward: onward.wait_send())


def gathered(front_rows, sample_matrix, pivots):
    dma = pltpu.SemaphoreType.DMA
    f32 = lambda *shape: pltpu.VMEM(shape, jnp.float32)
    bf16 = lambda *shape: pltpu.VMEM(shape, jnp.bfloat16)
    anywhere = pl.BlockSpec(memory_space=pl.ANY)
    vmem = pl.BlockSpec(memory_space=pltpu.VMEM)
    return pl.pallas_call(
        gather_kernel,
        out_shape=(jax.ShapeDtypeStruct((5, 64, 512), jnp.float32), jax.ShapeDtypeStruct((64, 512), jnp.float32)),
        in_specs=[anywhere, anywhere, vmem],
        out_specs=(vmem, vmem),
        scratch_shapes=[
            bf16(1024, 1536), bf16(1536, 1024), bf16(1024, 1536), f32(4, 4, 64, 1024),
            f32(4, 2, 2, 64, 256), f32(4, 2, 2, 64, 256), f32(4, 2, 4, 64, 256), f32(4, 4, 64, 256),
            f32(4, 2, 32, 256), f32(4, 2, 32, 256), f32(4, 2, 64, 256), bf16(20, 256, 256), f32(3, 8, 64, 128),
            f32(2, 64, 128), f32(64, 128), f32(32, 128), f32(4, 64, 128), f32(4, 2, 64, 128), f32(8, 64, 128), f32(16, 32, 128),
            f32(4, 64, 128), f32(3, 3, 8, 64, 128), f32(16, 8, 64, 128),
            f32(768, 512), f32(5, 64, 128), f32(5, 32, 512),
            dma((7,)), dma((2, 4, 2, 3)), dma((2, 4, 2, 3)), dma((16,)), dma((30,)),
            dma((3,)), dma((3, 3)), dma((3, 3)), dma((16,)), dma, dma((16,)), dma((16,)),
            dma((16,)), dma((5,)), dma((5,)),
        ],
        compiler_params=pltpu.CompilerParams(collective_id=1, has_side_effects=True, vmem_limit_bytes=52 * 1024 * 1024),
    )(front_rows, sample_matrix, pivots)


def senders():
    for core in range(2):
        for task in range(3):
            level, root = LEVELS[core][task], ROOTS[core][task]
            for half in range(2):
                sender = core if half == 0 else 1 - core
                yield level, sender, half, root, core if level == 0 else sender


def wide(value):
    return jnp.broadcast_to(value, (8, 128))


def small_inverse(columns, sub):
    columns = list(columns)
    for k in range(8):
        rows = [wide(column[k : k + 1, :]) for column in columns]
        scale = 1.0 / rows[k]
        here = sub == k
        lead = columns[k]
        for j in range(8):
            if j != k:
                row = rows[j] * scale
                columns[j] = jnp.where(here, row, columns[j] - lead * row)
        columns[k] = jnp.where(here, scale, -(lead * scale))
    return columns


def weighted(columns, rows):
    even, odd = columns[0] * rows[0], columns[1] * rows[1]
    for j in range(2, 8, 2):
        even = even + columns[j] * rows[j]
        odd = odd + columns[j + 1] * rows[j + 1]
    return even + odd


def eliminate(read):
    lane = lax.broadcasted_iota(jnp.int32, (8, 128), 1)
    sub = lax.broadcasted_iota(jnp.int32, (8, 128), 0)
    eye = jnp.where(lane == sub, 1.0, 0.0)

    def eight(_, blocks):
        corner = small_inverse([wide(blocks[0][:, 8 + j : 9 + j]) for j in range(8)], sub)
        columns = [[wide(block[:, 8 + j : 9 + j]) for j in range(8)] for block in blocks[1:]]
        rolled = [pltpu.roll(block, 120, 1) for block in blocks]
        top = jnp.where(lane < 8, eye, rolled[0])
        new = weighted(corner, [wide(top[j : j + 1]) for j in range(8)])
        rows = [wide(new[j : j + 1]) for j in range(8)]
        rest = [jnp.where(lane < 8, 0.0, block) - weighted(cols, rows) for cols, block in zip(columns, rolled[1:])]
        return tuple(rest + [new])

    blocks = lax.fori_loop(0, 8, eight, tuple(pltpu.roll(read(i), 8, 1) for i in range(8)))
    return jnp.concatenate([pltpu.roll(block, 56, 1) for block in blocks], axis=0)


def invert(block):
    upper, lower = block[:64], block[64:]
    lane = lax.broadcasted_iota(jnp.int32, (64, 128), 1)
    first = eliminate(lambda i: upper[8 * i : 8 * i + 8])
    reduced = pltpu.roll(jnp.where(lane < 64, 0.0, lower) - dot(lower[:, :64], first), 64, 1)
    second = eliminate(lambda i: reduced[8 * i : 8 * i + 8])
    bottom = pltpu.roll(second, 64, 1)
    across = pltpu.roll(first, 64, 1)[:, :64]
    top = jnp.where(lane < 64, first, 0.0) - dot(across, bottom)
    return jnp.concatenate([top, bottom], axis=0)


def dot(a, b):
    return lax.dot_general(a, b, (((1,), (0,)), ((), ())), precision=HI, preferred_element_type=jnp.float32)


def dot6(a, b):
    n = a.shape[0]
    ah, am, al = (split3(a)[k * n : k * n + n] for k in range(3))
    bh, bm, bl = (split3(b)[k * 128 : k * 128 + 128] for k in range(3))
    left1 = jnp.concatenate([ah, am], axis=1)
    d = lambda u, v: jnp.dot(u, v, preferred_element_type=jnp.float32)
    small = d(left1, jnp.concatenate([bl, bm], axis=0)) + d(jnp.concatenate([al, am], axis=1), jnp.concatenate([bh, bh], axis=0))
    return small + d(jnp.concatenate([ah, ah], axis=1), jnp.concatenate([bm, bh], axis=0))


def solve_in_place(m_ref):
    for p in range(4):
        at = 128 * p
        dinv = invert(m_ref[at : at + 128, at : at + 128])
        others = [q for q in range(4) if q != p]
        lead = jnp.concatenate([m_ref[at : at + 128, 128 * q : 128 * q + 128] for q in others], axis=1)
        both_sides = dot(dinv, lead)
        change = dot6(m_ref[at + 128 :, at : at + 128], jnp.concatenate([both_sides, dinv], axis=1))
        for n, q in enumerate(others):
            m_ref[at + 128 :, 128 * q : 128 * q + 128] -= change[:, 128 * n : 128 * n + 128]
        m_ref[at + 128 :, at : at + 128] = change[:, 384:]


def on_device(front_rows, sample_matrix, pivots):
    bases, top = gathered(front_rows, sample_matrix, pivots)
    return (bases[:, None], top)


def solution(mesh):
    return jax.shard_map(
        on_device,
        mesh=mesh,
        in_specs=(P("leaf", "grp"), P("grp", None), P()),
        out_specs=(P(None, "leaf", "grp", None), P("grp", None)),
        check_vma=False,
    )
```

```python
import jax
import jax.numpy as jnp
from jax import lax
from jax.experimental import pallas as pl
from jax.experimental.pallas import tpu as pltpu
from jax.sharding import PartitionSpec as P

HI = lax.Precision.HIGHEST
MESH = pl.DeviceIdType.MESH
PARTS = 2
ROOTS = ((8, 7, 5), (2, 10, 13))
LEVELS = ((0, 1, 3), (0, 2, 4))
FIRST = (
    ((4, 4, 12, 12, 8, 8, 11, 8, 8, 8, 9, 8, 8, 9, 11, 12), (1, 2, 2, 2, 3, 6, 2, 6, 1, 14, 6, 14, 3, 2, 2, 2)),
    ((7, 4, 6, 7, 7, 6, 7, 7, 11, 4, 7, 7, 3, 3, 7, 11), (6, 14, 6, 14, 11, 9, 10, 10, 9, 10, 10, 10, 9, 10, 10, 11)),
    ((5, 5, 5, 4, 5, 5, 5, 6, 9, 5, 9, 6, 1, 9, 1, 4), (13, 13, 13, 12, 1, 1, 9, 9, 13, 13, 14, 12, 13, 13, 13, 14)),
)
SLOT = (
    ((0, 1, 0, 1, 0, 0, 0, 0, 0, 0, 0, 0, 0, 1, 1, 2), (0, 0, 0, 0, 0, 0, 0, 1, 1, 0, 2, 1, 1, 0, 0, 0)),
    ((0, 0, 0, 0, 0, 1, 0, 0, 0, 1, 0, 0, 0, 1, 0, 1), (0, 0, 1, 1, 0, 0, 0, 0, 1, 0, 0, 0, 2, 0, 0, 1)),
    ((0, 0, 0, 0, 0, 0, 0, 0, 0, 0, 1, 1, 0, 2, 1, 1), (0, 0, 0, 0, 0, 1, 0, 1, 0, 0, 0, 1, 0, 0, 0, 1)),
)
PASS_ON = (
    (
        ((0, 0, 0, 0, 1, 0, 0, 0, 0, 11, 0, 7, 3, 0, 0, 0), (0, 1, 0, 5, 0, 0, 6, 0, 0, 0, 0, 0, 0, 0, 10, 0)),
        ((0, 0, 0, 0, 2, 0, 0, 0, 0, 14, 0, 15, 4, 0, 0, 0), (0, 9, 0, 13, 0, 0, 8, 0, 0, 0, 0, 0, 0, 0, 12, 0)),
        ((0, 0, 0, 0, 0, 0, 0, 0, 0, 0, 0, 0, 16, 0, 0, 0), (0, 0, 0, 0, 0, 0, 11, 0, 0, 0, 0, 0, 0, 0, 0, 0)),
    ),
    (
        ((0, 0, 0, 13, 2, 0, 3, 0, 0, 0, 0, 9, 0, 0, 0, 0), (0, 0, 0, 0, 0, 0, 1, 0, 0, 6, 0, 5, 0, 0, 2, 0)),
        ((0, 0, 0, 14, 10, 0, 6, 0, 0, 0, 0, 16, 0, 0, 0, 0), (0, 0, 0, 0, 0, 0, 3, 0, 0, 9, 0, 16, 0, 0, 4, 0)),
        ((0, 0, 0, 0, 0, 0, 0, 0, 0, 0, 0, 0, 0, 0, 0, 0), (0, 0, 0, 0, 0, 0, 0, 0, 0, 13, 0, 0, 0, 0, 0, 0)),
    ),
    (
        ((0, 13, 0, 0, 4, 0, 8, 0, 0, 9, 0, 0, 0, 0, 0, 0), (0, 5, 0, 0, 0, 0, 0, 0, 0, 7, 0, 0, 4, 0, 11, 0)),
        ((0, 15, 0, 0, 16, 0, 12, 0, 0, 11, 0, 0, 0, 0, 0, 0), (0, 6, 0, 0, 0, 0, 0, 0, 0, 8, 0, 0, 12, 0, 16, 0)),
        ((0, 0, 0, 0, 0, 0, 0, 0, 0, 14, 0, 0, 0, 0, 0, 0), (0, 0, 0, 0, 0, 0, 0, 0, 0, 0, 0, 0, 0, 0, 0, 0)),
    ),
)


def lookup(table, core, grp):
    at, value = 16 * core + grp, 0
    for position, entry in enumerate(table[0] + table[1]):
        if entry:
            value = value + jnp.where(at == position, entry, 0)
    return value


def roles():
    grp, core = lax.axis_index("grp"), lax.rem(lax.axis_index("leaf"), 2)
    main, twin = 0, 0
    for of_core in range(2):
        for root in ROOTS[of_core]:
            here = jnp.where(grp == root, 1, 0)
            main = main + here * jnp.where(core == of_core, 1, 0)
            twin = twin + here * jnp.where(core == of_core, 0, 1)
    return main, twin


def bit(value, place):
    return lax.rem(value // (1 << place), 2)


def flip(value, mask):
    for place in range(4):
        if mask >> place & 1:
            value = value + (1 << place) * (1 - 2 * bit(value, place))
    return value


def send(src, dst, send_sem, recv_sem, device):
    return pltpu.make_async_remote_copy(
        src_ref=src, dst_ref=dst, send_sem=send_sem, recv_sem=recv_sem, device_id=device, device_id_type=MESH
    )


def row_of(table, node):
    rows = lax.broadcasted_iota(jnp.int32, table.shape, 0)
    return jnp.sum(jnp.where(rows == node, table, 0), axis=0, keepdims=True)


def split3(value):
    high = value.astype(jnp.bfloat16)
    rest = value - high.astype(jnp.float32)
    middle = rest.astype(jnp.bfloat16)
    low = (rest - middle.astype(jnp.float32)).astype(jnp.bfloat16)
    return jnp.concatenate([high, middle, low], axis=0)


def permuted(src, order):
    rows = src.shape[0]
    out = jnp.dot(split3(src), order, preferred_element_type=jnp.float32)
    return (out[:rows] + out[rows : 2 * rows]) + out[2 * rows :]


def one_hot_order(pivots, start):
    src = lax.broadcasted_iota(jnp.int32, (256, 128), 0)
    lane = lax.broadcasted_iota(jnp.int32, (256, 128), 1)
    chosen = jnp.where(src == pivots - start, 1.0, 0.0)
    ones = jnp.full((128, 128), 1.0, jnp.bfloat16)
    free = 1.0 - jnp.dot(chosen.astype(jnp.bfloat16), ones, preferred_element_type=jnp.float32)
    row = lax.broadcasted_iota(jnp.int32, (256, 256), 0)
    column = lax.broadcasted_iota(jnp.int32, (256, 256), 1)
    before = jnp.where(jnp.logical_and(column < row, column // 64 == row // 64), 1.0, 0.0).astype(jnp.bfloat16)
    rank = jnp.dot(before, free.astype(jnp.bfloat16), preferred_element_type=jnp.float32)
    place = rank + (32 * (src // 64)).astype(jnp.float32)
    rest = jnp.where(jnp.logical_and(free > 0.5, place == lane.astype(jnp.float32)), 1.0, 0.0)
    return chosen.astype(jnp.bfloat16), rest.astype(jnp.bfloat16)


def gather_kernel(
    front_any, sample_any, pivot_ref, out_ref, top_ref,
    front_ref, sample_ref, turned_ref, p_ref,
    hop1, comb1, near1, sum1, hop2, comb2, near2, order_ref, y_ref,
    a1_ref, a2_ref, a3_ref, r1_ref, r2_ref, r3_ref, r4_ref, rt_ref, relay_ref, z_ref, m_ref, spot_ref, rows_ref,
    load_sem, rs_send, rs_recv, leaf_send, leaf_recv, y_send, relay_send, relay_recv, z_recv, z_local, twin_send, twin_recv,
    u_send, u_recv, u_onward,
):
    leaf, grp = lax.axis_index("leaf"), lax.axis_index("grp")
    y, x = grp // 4, lax.rem(grp, 4)
    core = lax.rem(leaf, 2)
    base = leaf - core

    loads = [
        pltpu.make_async_copy(sample_any.at[pl.ds(512 * r, 512)], sample_ref.at[pl.ds(512 * r, 512)], load_sem.at[r])
        for r in range(3)
    ]
    for quarter in range(4):
        rows = pl.ds(512 * (quarter % 2) + 256 * (quarter // 2), 256)
        loads.append(pltpu.make_async_copy(front_any.at[rows], front_ref.at[rows], load_sem.at[3 + quarter]))
    for load in loads:
        load.start()
    barrier = pltpu.get_barrier_semaphore()
    for other in range(1, 16):
        pl.semaphore_signal(barrier, inc=1, device_id=(leaf, lax.rem(grp + other, 16)), device_id_type=MESH)
        pl.semaphore_signal(barrier, inc=1, device_id=(lax.rem(leaf + other, 16), grp), device_id_type=MESH)

    started = []

    def begin(copy):
        copy.start()
        started.append(copy)
        return copy

    def neighbour(along_x, offset):
        if along_x:
            return (leaf, y * 4 + lax.rem(x + offset, 4))
        return (leaf, lax.rem(y + offset, 4) * 4 + x)

    def source(phase, stream, chunk, sub):
        half = stream % 2
        if phase == 0:
            lanes = pl.ds(512 * half + 256 * (stream // 2), 256)
            if half == 0:
                return p_ref.at[pl.ds(2 * sub, 2), chunk, :, lanes]
            return p_ref.at[chunk, pl.ds(2 * sub, 2), :, lanes]
        return sum1.at[stream, chunk, pl.ds(32 * sub, 32), :]

    def landing(phase, stream, way, sub):
        if phase == 0:
            return near1.at[stream, way, pl.ds(2 * sub, 2), :, :]
        return near2.at[stream, way, pl.ds(32 * sub, 32), :]

    hops, combs = (hop1, hop2), (comb1, comb2)
    rings = {}

    def ring(phase, stream, way, kind, src, dst):
        along_x = (phase == 0) == (stream % 2 == 0)
        to = neighbour(along_x, 1 if way == 0 else 3)
        rings[phase, stream, way, kind] = begin(
            send(src, dst, rs_send.at[phase, stream, way, kind], rs_recv.at[phase, stream, way, kind], to)
        )

    def position(phase, stream):
        return x if (phase == 0) == (stream % 2 == 0) else y

    def ring_hop(phase, stream):
        at = position(phase, stream)
        for way in range(2):
            ring(phase, stream, way, 0, source(phase, stream, lax.rem(at + 2, 4), way), hops[phase].at[stream, way])

    def ring_own(phase, stream):
        at = position(phase, stream)
        for way in range(2):
            chunk = lax.rem(at + (1 if way == 0 else 3), 4)
            ring(phase, stream, way, 1, source(phase, stream, chunk, 1 - way), landing(phase, stream, way, 1 - way))

    def ring_join(phase, stream):
        at = position(phase, stream)
        for way in range(2):
            chunk = lax.rem(at + (1 if way == 0 else 3), 4)
            rings[phase, stream, way, 0].wait_recv()
            combs[phase][stream, way] = hops[phase][stream, way] + source(phase, stream, chunk, way)[...]
            ring(phase, stream, way, 2, combs[phase].at[stream, way], landing(phase, stream, way, way))

    def ring_last(phase, stream):
        for way in range(2):
            for kind in (1, 2):
                rings[phase, stream, way, kind].wait_recv()
        half = stream % 2
        if phase == 0:
            lanes = pl.ds(512 * half + 256 * (stream // 2), 256)
            own = p_ref[:, x, :, lanes] if half == 0 else p_ref[y, :, :, lanes]
            sum1[stream] = (near1[stream, 0] + own) + near1[stream, 1]
            return None
        own = sum1[stream, position(1, stream)]
        return (near2[stream, 0] + own) + near2[stream, 1]

    for r in range(3):
        loads[r].wait()
        for c in range(8):
            turned_ref[128 * c : 128 * c + 128, 512 * r : 512 * r + 512] = sample_ref[
                512 * r : 512 * r + 512, 128 * c : 128 * c + 128
            ].T
    for quarter in range(4):
        low = 512 * (quarter % 2) + 256 * (quarter // 2)
        loads[3 + quarter].wait()
        for c in range(4):
            product = lax.dot_general(
                turned_ref[256 * c : 256 * c + 256, :], front_ref[low : low + 256, :], (((1,), (1,)), ((), ())),
                preferred_element_type=jnp.float32,
            )
            for b in range(4):
                p_ref[c, b, :, low : low + 256] = product[64 * b : 64 * b + 64]
        if quarter == 0:
            pl.semaphore_wait(barrier, 30)
        for n in range(PARTS // 2):
            stream = quarter % 2 + 2 * (PARTS // 2 * (quarter // 2) + n)
            ring_hop(0, stream)
            if stream < 2:
                ring_own(0, stream)

    def orders(level, block):
        node = 32 - (32 >> level) + leaf // (1 << level)
        chosen, rest = one_hot_order(row_of(pivot_ref[:, 128 * block : 128 * block + 128], node), 256 * block)
        order_ref[4 * level + block, :, 0:128] = chosen
        order_ref[4 * level + block, :, 128:256] = rest

    def select(level, block, value):
        chosen = permuted(value, order_ref[4 * level + block])
        task = (level + 1) // 2
        y_ref[task, 2 + block] = chosen[:, :128]
        y_ref[task, block + 4 * (block // 2)] = chosen[:, 128:]

    done = {}
    for step in range(PARTS + 3):
        if step < PARTS:
            for half in range(2):
                ring_join(0, 2 * step + half)
            if step + 1 < PARTS:
                for half in range(2):
                    ring_own(0, 2 * step + 2 + half)
        if step == 0:
            for level in range(5):
                for block in range(4):
                    orders(level, block)
        if 1 <= step <= PARTS:
            for half in range(2):
                ring_last(0, 2 * step - 2 + half)
                ring_hop(1, 2 * step - 2 + half)
                ring_own(1, 2 * step - 2 + half)
        if 2 <= step <= PARTS + 1:
            for half in range(2):
                ring_join(1, 2 * step - 4 + half)
        if step >= 3:
            part = step - 3
            for half in range(2):
                done[half, part] = ring_last(1, 2 * part + half)
            each = PARTS // 2
            if (part + 1) % each == 0:
                for half in range(2):
                    value = jnp.concatenate([done[half, part + 1 - each + n] for n in range(each)], axis=1)
                    select(0, 2 * half + part // each, value)

    def own_slice(task, act, local=True):
        root = ROOTS[0][task] + core * (ROOTS[1][task] - ROOTS[0][task])
        first, slot = lookup(FIRST[task], core, grp), lookup(SLOT[task], core, grp)
        pieces = [(part, y_ref.at[task, pl.ds(4 * part, 4)], pl.ds(4 * part, 4)) for part in range(2)]

        @pl.when(jnp.logical_and(first == root, grp != root))
        def _():
            for part, src, blocks in pieces:
                act(send(src, z_ref.at[grp, blocks], y_send.at[task, part], z_recv.at[grp, part], (leaf, root)))

        @pl.when(first != root)
        def _():
            for part, src, blocks in pieces:
                act(
                    send(
                        src, relay_ref.at[task, slot, blocks],
                        y_send.at[task, part], relay_recv.at[task, slot, part], (leaf, first),
                    )
                )

        if local:

            @pl.when(grp == root)
            def _():
                act(pltpu.make_async_copy(y_ref.at[task], z_ref.at[grp], z_local))

    def to_root(task):
        own_slice(task, lambda copy: copy.start())

    def pass_on(task, act):
        root = ROOTS[0][task] + core * (ROOTS[1][task] - ROOTS[0][task])
        for slot in range(3):
            source_grp = lookup(PASS_ON[task][slot], core, grp)

            @pl.when(source_grp > 0)
            def _():
                for part in range(2):
                    blocks = pl.ds(4 * part, 4)
                    held = relay_ref.at[task, slot, blocks]
                    act(
                        send(held, held, y_send.at[task, part], relay_recv.at[task, slot, part], (leaf, root)),
                        send(
                            held, z_ref.at[source_grp - 1, blocks],
                            relay_send.at[task, slot, part], z_recv.at[source_grp - 1, part], (leaf, root),
                        ),
                    )

    def relay(task):
        def act(landed, onward):
            landed.wait_recv()
            onward.start()

        pass_on(task, act)

    def both(first, second):
        return jnp.concatenate([first, second], axis=1)

    to_root(0)
    up = send(y_ref.at[0, pl.ds(2, 4)], r1_ref, leaf_send.at[0], leaf_recv.at[0], (base, grp))

    @pl.when(core == 1)
    def _():
        up.start()

    def chosen_only(level, block, value):
        return permuted(value, order_ref[4 * level + block][:, :128])

    kept = []

    def share(number, src, dst_ref, slot, recv, to_core, masks, value):
        for n, mask in enumerate(masks):
            copy = send(
                src, dst_ref.at[slot], leaf_send.at[number + n], leaf_recv.at[recv + slot], (flip(base, mask) + to_core, grp)
            )
            if mask == 0:

                @pl.when(core != to_core)
                def _():
                    copy.start()

                @pl.when(core == to_core)
                def _():
                    dst_ref[slot] = value

                kept.append((copy, to_core))
            else:
                begin(copy)

    for i in range(2):
        a1_ref[i] = chosen_only(1, 2 * core + i, both(y_ref[0, 2 + 2 * i], y_ref[0, 3 + 2 * i]))
    part1 = a1_ref[...]
    share(1, a1_ref, r2_ref, lax.rem(leaf, 4), 1, 1, (2, 0), part1)
    part2 = chosen_only(2, lax.rem(leaf, 4), both(part1[0], part1[1]))
    a2_ref[...] = part2
    share(3, a2_ref, r3_ref, lax.rem(leaf, 8), 5, 0, (4, 6, 2, 0), part2)
    zero = jnp.zeros_like(part2)
    spread_out = both(jnp.where(core == 0, part2, zero), jnp.where(core == 0, zero, part2))
    placed = chosen_only(3, lax.rem(leaf, 8) // 2, spread_out)
    part3 = placed[:32] + pltpu.roll(placed[32:], 64, 1)
    a3_ref[...] = part3
    share(7, a3_ref, r4_ref, leaf, 13, 1, (8, 10, 6, 12, 14, 4, 2, 0), part3)

    def arrived(ref, recv, slot):
        @pl.when(slot != lax.rem(leaf, ref.shape[0]))
        def _():
            send(ref.at[slot], ref.at[slot], leaf_send.at[0], leaf_recv.at[recv + slot], (base + 1 - core, grp)).wait_recv()

    @pl.when(core == 0)
    def _():
        for i in range(2):
            select(1, i, both(y_ref[0, 2 + 2 * i], y_ref[0, 3 + 2 * i]))
        send(r1_ref, r1_ref, leaf_send.at[0], leaf_recv.at[0], (base + 1, grp)).wait_recv()
        for i in range(2):
            select(1, 2 + i, both(r1_ref[2 * i], r1_ref[2 * i + 1]))

    @pl.when(core == 1)
    def _():
        for s in range(4):
            arrived(r2_ref, 1, s)
            select(2, s, both(r2_ref[s, 0], r2_ref[s, 1]))

    to_root(1)
    relay(0)

    @pl.when(core == 0)
    def _():
        for s in range(4):
            arrived(r3_ref, 5, 2 * s)
            arrived(r3_ref, 5, 2 * s + 1)
            select(3, s, both(r3_ref[2 * s], r3_ref[2 * s + 1]))

    @pl.when(core == 1)
    def _():
        low_lanes = lax.broadcasted_iota(jnp.int32, (32, 128), 1) < 64
        for s in range(16):
            arrived(r4_ref, 13, s)
        joined = []
        for i in range(8):
            even, odd = r4_ref[2 * i], r4_ref[2 * i + 1]
            upper = jnp.where(low_lanes, even, odd)
            lower = pltpu.roll(jnp.where(low_lanes, odd, even), 64, 1)
            joined.append(jnp.concatenate([upper, lower], axis=0))
        for s in range(4):
            select(4, s, both(joined[2 * s], joined[2 * s + 1]))

    to_root(2)
    relay(1)
    relay(2)

    top = send(y_ref.at[2, pl.ds(2, 4)], rt_ref, leaf_send.at[15], leaf_recv.at[29], (base, grp))

    @pl.when(core == 1)
    def _():
        top.start()

    earlier = jnp.where(
        lax.broadcasted_iota(jnp.int32, (64, 64), 1) < lax.broadcasted_iota(jnp.int32, (64, 64), 0), 1.0, 0.0
    ).astype(jnp.bfloat16)
    ones = jnp.full((512, 128), 1.0, jnp.bfloat16)
    for level in range(5):
        node = 32 - (32 >> level) + leaf // (1 << level)
        place = grp * 64 + lax.broadcasted_iota(jnp.int32, (64, 512), 0)
        is_pivot = jnp.where(place == row_of(pivot_ref[...], node), 1.0, 0.0)
        out_ref[level] = is_pivot
        free = 1.0 - jnp.dot(is_pivot.astype(jnp.bfloat16), ones, preferred_element_type=jnp.float32)
        rank = jnp.dot(earlier, free.astype(jnp.bfloat16), preferred_element_type=jnp.float32)
        lane = lax.broadcasted_iota(jnp.int32, (64, 128), 1).astype(jnp.float32)
        spot_ref[level] = jnp.where(jnp.logical_and(free > 0.5, rank == lane), 1.0, 0.0)

    is_main, is_twin = roles()
    twin_leaf = base + 1 - core
    coming = ((0, 0), (0, 1), (0, 3), (1, 0), (3, 0), (0, 2), (2, 0), (1, 1), (1, 3), (3, 1), (3, 3), (1, 2), (3, 2), (2, 1), (2, 3), (2, 2))

    def to_twin(at):
        part = z_ref.at[at, pl.ds(2, 6)]
        return send(part, part, twin_send.at[at], twin_recv.at[at], (twin_leaf, grp))

    for group in range(4):
        places = [lax.rem(y + dy, 4) * 4 + lax.rem(x + dx, 4) for dy, dx in coming[4 * group : 4 * group + 4]]

        @pl.when(is_main > 0)
        def _():
            for n, at in enumerate(places):
                if group == 0 and n == 0:
                    pltpu.make_async_copy(y_ref.at[0], z_ref.at[at], z_local).wait()
                else:
                    for part in range(2):
                        piece = z_ref.at[at, pl.ds(4 * part, 4)]
                        send(piece, piece, y_send.at[0, part], z_recv.at[at, part], (twin_leaf, grp)).wait_recv()
                to_twin(at).start()

        @pl.when(is_twin > 0)
        def _():
            for at in places:
                to_twin(at).wait_recv()

        @pl.when(is_main + is_twin > 0)
        def _():
            rows = []
            for at in places:
                blocks = [z_ref[at, 2 + b] for b in range(4)] + [z_ref[at, 6 * is_twin + b] for b in range(2)]
                rows.append(jnp.concatenate(blocks, axis=1))
            z = jnp.concatenate(rows, axis=0)
            gram = lax.dot_general(
                z, z[:, :512], (((0,), (0,)), ((), ())), precision=HI, preferred_element_type=jnp.float32
            )
            if group == 0:
                m_ref[...] = gram
            else:
                m_ref[...] += gram

    @pl.when(is_main + is_twin > 0)
    def _():
        solve_in_place(m_ref)

    def each(level, of_core, half, place, to_core, act):
        @pl.when(jnp.logical_and(core == of_core, grp == place))
        def _():
            for target in range(8 * half, 8 * half + 8):
                if (target, to_core) != (place, of_core):
                    act(
                        send(
                            m_ref.at[pl.ds(512 + 32 * (target - 8 * half), 32)], rows_ref.at[level],
                            u_send.at[target], u_recv.at[level], (base + to_core, target),
                        )
                    )

    for sender in senders():
        each(*sender, lambda copy: copy.start())

    block_half = grp // 8

    def onward(level):
        return send(rows_ref.at[level], rows_ref.at[level], u_onward.at[level], u_recv.at[level], (twin_leaf, grp))

    def served_here(of_core):
        return core == of_core + block_half * (1 - 2 * of_core)

    for of_core in range(2):
        for task in range(3):
            level, root = LEVELS[of_core][task], ROOTS[of_core][task]
            direct = core == of_core if task == 0 else served_here(of_core)
            is_root = grp == root
            if task == 0:
                is_root = jnp.logical_and(is_root, block_half == 0)

            @pl.when(jnp.logical_and(direct, is_root))
            def _():
                low = 512 + 32 * (root % 8)
                rows_ref[level] = m_ref[low : low + 32, :]

            @pl.when(jnp.logical_and(direct, jnp.logical_not(is_root)))
            def _():
                onward(level).wait_recv()

            if task > 0:

                @pl.when(direct)
                def _():
                    onward(level).start()

    for of_core in range(2):
        for task in (1, 2):
            level = LEVELS[of_core][task]

            @pl.when(jnp.logical_not(served_here(of_core)))
            def _():
                onward(level).wait_recv()

    for level in range(5):
        spot = spot_ref[level][:, :32].astype(jnp.bfloat16)
        out_ref[level] += jnp.dot(
            jnp.concatenate([spot, spot, spot], axis=1), split3(rows_ref[level]), preferred_element_type=jnp.float32
        )
    for sender in senders():
        each(*sender, lambda copy: copy.wait_send())
    for of_core in range(2):
        for task in (1, 2):
            level = LEVELS[of_core][task]

            @pl.when(served_here(of_core))
            def _():
                onward(level).wait_send()

    @pl.when(core == 1)
    def _():
        for b in range(4):
            top_ref[:, 128 * b : 128 * b + 128] = y_ref[2, 2 + b]
        up.wait_send()
        top.wait_send()

    @pl.when(core == 0)
    def _():
        top.wait_recv()
        for b in range(4):
            top_ref[:, 128 * b : 128 * b + 128] = rt_ref[b]

    @pl.when(is_main > 0)
    def _():
        for at in range(16):
            to_twin(at).wait_send()

    for copy, to_core in kept:

        @pl.when(core != to_core)
        def _():
            copy.wait_send()

    for copy in started:
        copy.wait_send()
    for task in range(3):
        own_slice(task, lambda copy: copy.wait_send(), local=False)
        pass_on(task, lambda landed, onward: onward.wait_send())


def gathered(front_rows, sample_matrix, pivots):
    dma = pltpu.SemaphoreType.DMA
    f32 = lambda *shape: pltpu.VMEM(shape, jnp.float32)
    bf16 = lambda *shape: pltpu.VMEM(shape, jnp.bfloat16)
    anywhere = pl.BlockSpec(memory_space=pl.ANY)
    vmem = pl.BlockSpec(memory_space=pltpu.VMEM)
    return pl.pallas_call(
        gather_kernel,
        out_shape=(jax.ShapeDtypeStruct((5, 64, 512), jnp.float32), jax.ShapeDtypeStruct((64, 512), jnp.float32)),
        in_specs=[anywhere, anywhere, vmem],
        out_specs=(vmem, vmem),
        scratch_shapes=[
            bf16(1024, 1536), bf16(1536, 1024), bf16(1024, 1536), f32(4, 4, 64, 1024),
            f32(4, 2, 2, 64, 256), f32(4, 2, 2, 64, 256), f32(4, 2, 4, 64, 256), f32(4, 4, 64, 256),
            f32(4, 2, 32, 256), f32(4, 2, 32, 256), f32(4, 2, 64, 256), bf16(20, 256, 256), f32(3, 8, 64, 128),
            f32(2, 64, 128), f32(64, 128), f32(32, 128), f32(4, 64, 128), f32(4, 2, 64, 128), f32(8, 64, 128), f32(16, 32, 128),
            f32(4, 64, 128), f32(3, 3, 8, 64, 128), f32(16, 8, 64, 128),
            f32(768, 512), f32(5, 64, 128), f32(5, 32, 512),
            dma((7,)), dma((2, 4, 2, 3)), dma((2, 4, 2, 3)), dma((16,)), dma((30,)),
            dma((3, 2)), dma((3, 3, 2)), dma((3, 3, 2)), dma((16, 2)), dma, dma((16,)), dma((16,)),
            dma((16,)), dma((5,)), dma((5,)),
        ],
        compiler_params=pltpu.CompilerParams(collective_id=1, has_side_effects=True, vmem_limit_bytes=52 * 1024 * 1024),
    )(front_rows, sample_matrix, pivots)


def senders():
    for core in range(2):
        for task in range(3):
            level, root = LEVELS[core][task], ROOTS[core][task]
            for half in range(2):
                sender = core if half == 0 else 1 - core
                yield level, sender, half, root, core if level == 0 else sender


def wide(value):
    return jnp.broadcast_to(value, (8, 128))


def small_inverse(columns, sub):
    columns = list(columns)
    for k in range(8):
        rows = [wide(column[k : k + 1, :]) for column in columns]
        scale = 1.0 / rows[k]
        here = sub == k
        lead = columns[k]
        for j in range(8):
            if j != k:
                row = rows[j] * scale
                columns[j] = jnp.where(here, row, columns[j] - lead * row)
        columns[k] = jnp.where(here, scale, -(lead * scale))
    return columns


def weighted(columns, rows):
    even, odd = columns[0] * rows[0], columns[1] * rows[1]
    for j in range(2, 8, 2):
        even = even + columns[j] * rows[j]
        odd = odd + columns[j + 1] * rows[j + 1]
    return even + odd


def eliminate(read):
    lane = lax.broadcasted_iota(jnp.int32, (8, 128), 1)
    sub = lax.broadcasted_iota(jnp.int32, (8, 128), 0)
    eye = jnp.where(lane == sub, 1.0, 0.0)

    def eight(_, blocks):
        corner = small_inverse([wide(blocks[0][:, 8 + j : 9 + j]) for j in range(8)], sub)
        columns = [[wide(block[:, 8 + j : 9 + j]) for j in range(8)] for block in blocks[1:]]
        rolled = [pltpu.roll(block, 120, 1) for block in blocks]
        top = jnp.where(lane < 8, eye, rolled[0])
        new = weighted(corner, [wide(top[j : j + 1]) for j in range(8)])
        rows = [wide(new[j : j + 1]) for j in range(8)]
        rest = [jnp.where(lane < 8, 0.0, block) - weighted(cols, rows) for cols, block in zip(columns, rolled[1:])]
        return tuple(rest + [new])

    blocks = lax.fori_loop(0, 8, eight, tuple(pltpu.roll(read(i), 8, 1) for i in range(8)))
    return jnp.concatenate([pltpu.roll(block, 56, 1) for block in blocks], axis=0)


def invert(block):
    upper, lower = block[:64], block[64:]
    lane = lax.broadcasted_iota(jnp.int32, (64, 128), 1)
    first = eliminate(lambda i: upper[8 * i : 8 * i + 8])
    reduced = pltpu.roll(jnp.where(lane < 64, 0.0, lower) - product(lower[:, :64], first), 64, 1)
    second = eliminate(lambda i: reduced[8 * i : 8 * i + 8])
    bottom = pltpu.roll(second, 64, 1)
    across = pltpu.roll(first, 64, 1)[:, :64]
    top = jnp.where(lane < 64, first, 0.0) - product(across, bottom)
    return jnp.concatenate([top, bottom], axis=0)


def dot(a, b):
    return lax.dot_general(a, b, (((1,), (0,)), ((), ())), precision=HI, preferred_element_type=jnp.float32)


def product(a, b):
    n, depth = a.shape
    ah, am, al = (split3(a)[k * n : k * n + n] for k in range(3))
    bh, bm, bl = (split3(b)[k * depth : k * depth + depth] for k in range(3))
    left = jnp.concatenate([al, am, ah, am, ah, ah], axis=1)
    right = jnp.concatenate([bh, bm, bl, bh, bm, bh], axis=0)
    return jnp.dot(left, right, preferred_element_type=jnp.float32)


def solve_in_place(m_ref):
    for p in range(4):
        at = 128 * p
        dinv = invert(m_ref[at : at + 128, at : at + 128])
        others = [q for q in range(4) if q != p]
        lead = jnp.concatenate([m_ref[at : at + 128, 128 * q : 128 * q + 128] for q in others], axis=1)
        both_sides = product(dinv, lead)
        change = product(m_ref[at + 128 :, at : at + 128], jnp.concatenate([both_sides, dinv], axis=1))
        for n, q in enumerate(others):
            m_ref[at + 128 :, 128 * q : 128 * q + 128] -= change[:, 128 * n : 128 * n + 128]
        m_ref[at + 128 :, at : at + 128] = change[:, 384:]


def on_device(front_rows, sample_matrix, pivots):
    bases, top = gathered(front_rows, sample_matrix, pivots)
    return (bases[:, None], top)


def solution(mesh):
    return jax.shard_map(
        on_device,
        mesh=mesh,
        in_specs=(P("leaf", "grp"), P("grp", None), P()),
        out_specs=(P(None, "leaf", "grp", None), P("grp", None)),
        check_vma=False,
    )
```

```python
import jax
import jax.numpy as jnp
from jax import lax
from jax.experimental import pallas as pl
from jax.experimental.pallas import tpu as pltpu
from jax.sharding import PartitionSpec as P

HI = lax.Precision.HIGHEST
MESH = pl.DeviceIdType.MESH
PARTS = 2
ROOTS = ((8, 7, 5), (2, 10, 13))
LEVELS = ((0, 1, 3), (0, 2, 4))
FIRST = (
    ((4, 4, 12, 12, 8, 8, 11, 8, 8, 8, 9, 8, 8, 9, 11, 12), (1, 2, 2, 2, 3, 6, 2, 6, 1, 14, 6, 14, 3, 2, 2, 2)),
    ((7, 4, 6, 7, 7, 6, 7, 7, 11, 4, 7, 7, 3, 3, 7, 11), (6, 14, 6, 14, 11, 9, 10, 10, 9, 10, 10, 10, 9, 10, 10, 11)),
    ((5, 5, 5, 4, 5, 5, 5, 6, 9, 5, 9, 6, 1, 9, 1, 4), (13, 13, 13, 12, 1, 1, 9, 9, 13, 13, 14, 12, 13, 13, 13, 14)),
)
SLOT = (
    ((0, 1, 0, 1, 0, 0, 0, 0, 0, 0, 0, 0, 0, 1, 1, 2), (0, 0, 0, 0, 0, 0, 0, 1, 1, 0, 2, 1, 1, 0, 0, 0)),
    ((0, 0, 0, 0, 0, 1, 0, 0, 0, 1, 0, 0, 0, 1, 0, 1), (0, 0, 1, 1, 0, 0, 0, 0, 1, 0, 0, 0, 2, 0, 0, 1)),
    ((0, 0, 0, 0, 0, 0, 0, 0, 0, 0, 1, 1, 0, 2, 1, 1), (0, 0, 0, 0, 0, 1, 0, 1, 0, 0, 0, 1, 0, 0, 0, 1)),
)
PASS_ON = (
    (
        ((0, 0, 0, 0, 1, 0, 0, 0, 0, 11, 0, 7, 3, 0, 0, 0), (0, 1, 0, 5, 0, 0, 6, 0, 0, 0, 0, 0, 0, 0, 10, 0)),
        ((0, 0, 0, 0, 2, 0, 0, 0, 0, 14, 0, 15, 4, 0, 0, 0), (0, 9, 0, 13, 0, 0, 8, 0, 0, 0, 0, 0, 0, 0, 12, 0)),
        ((0, 0, 0, 0, 0, 0, 0, 0, 0, 0, 0, 0, 16, 0, 0, 0), (0, 0, 0, 0, 0, 0, 11, 0, 0, 0, 0, 0, 0, 0, 0, 0)),
    ),
    (
        ((0, 0, 0, 13, 2, 0, 3, 0, 0, 0, 0, 9, 0, 0, 0, 0), (0, 0, 0, 0, 0, 0, 1, 0, 0, 6, 0, 5, 0, 0, 2, 0)),
        ((0, 0, 0, 14, 10, 0, 6, 0, 0, 0, 0, 16, 0, 0, 0, 0), (0, 0, 0, 0, 0, 0, 3, 0, 0, 9, 0, 16, 0, 0, 4, 0)),
        ((0, 0, 0, 0, 0, 0, 0, 0, 0, 0, 0, 0, 0, 0, 0, 0), (0, 0, 0, 0, 0, 0, 0, 0, 0, 13, 0, 0, 0, 0, 0, 0)),
    ),
    (
        ((0, 13, 0, 0, 4, 0, 8, 0, 0, 9, 0, 0, 0, 0, 0, 0), (0, 5, 0, 0, 0, 0, 0, 0, 0, 7, 0, 0, 4, 0, 11, 0)),
        ((0, 15, 0, 0, 16, 0, 12, 0, 0, 11, 0, 0, 0, 0, 0, 0), (0, 6, 0, 0, 0, 0, 0, 0, 0, 8, 0, 0, 12, 0, 16, 0)),
        ((0, 0, 0, 0, 0, 0, 0, 0, 0, 14, 0, 0, 0, 0, 0, 0), (0, 0, 0, 0, 0, 0, 0, 0, 0, 0, 0, 0, 0, 0, 0, 0)),
    ),
)


def lookup(table, core, grp):
    at, value = 16 * core + grp, 0
    for position, entry in enumerate(table[0] + table[1]):
        if entry:
            value = value + jnp.where(at == position, entry, 0)
    return value


def roles():
    grp, core = lax.axis_index("grp"), lax.rem(lax.axis_index("leaf"), 2)
    main, twin = 0, 0
    for of_core in range(2):
        for root in ROOTS[of_core]:
            here = jnp.where(grp == root, 1, 0)
            main = main + here * jnp.where(core == of_core, 1, 0)
            twin = twin + here * jnp.where(core == of_core, 0, 1)
    return main, twin


def bit(value, place):
    return lax.rem(value // (1 << place), 2)


def flip(value, mask):
    for place in range(4):
        if mask >> place & 1:
            value = value + (1 << place) * (1 - 2 * bit(value, place))
    return value


def send(src, dst, send_sem, recv_sem, device):
    return pltpu.make_async_remote_copy(
        src_ref=src, dst_ref=dst, send_sem=send_sem, recv_sem=recv_sem, device_id=device, device_id_type=MESH
    )


def row_of(table, node):
    rows = lax.broadcasted_iota(jnp.int32, table.shape, 0)
    return jnp.sum(jnp.where(rows == node, table, 0), axis=0, keepdims=True)


def split3(value):
    high = value.astype(jnp.bfloat16)
    rest = value - high.astype(jnp.float32)
    middle = rest.astype(jnp.bfloat16)
    low = (rest - middle.astype(jnp.float32)).astype(jnp.bfloat16)
    return jnp.concatenate([high, middle, low], axis=0)


def permuted(src, order):
    rows = src.shape[0]
    out = jnp.dot(split3(src), order, preferred_element_type=jnp.float32)
    return (out[:rows] + out[rows : 2 * rows]) + out[2 * rows :]


def one_hot_order(pivots, start):
    src = lax.broadcasted_iota(jnp.int32, (256, 128), 0)
    lane = lax.broadcasted_iota(jnp.int32, (256, 128), 1)
    chosen = jnp.where(src == pivots - start, 1.0, 0.0)
    ones = jnp.full((128, 128), 1.0, jnp.bfloat16)
    free = 1.0 - jnp.dot(chosen.astype(jnp.bfloat16), ones, preferred_element_type=jnp.float32)
    row = lax.broadcasted_iota(jnp.int32, (256, 256), 0)
    column = lax.broadcasted_iota(jnp.int32, (256, 256), 1)
    before = jnp.where(jnp.logical_and(column < row, column // 64 == row // 64), 1.0, 0.0).astype(jnp.bfloat16)
    rank = jnp.dot(before, free.astype(jnp.bfloat16), preferred_element_type=jnp.float32)
    place = rank + (32 * (src // 64)).astype(jnp.float32)
    rest = jnp.where(jnp.logical_and(free > 0.5, place == lane.astype(jnp.float32)), 1.0, 0.0)
    return chosen.astype(jnp.bfloat16), rest.astype(jnp.bfloat16)


def gather_kernel(
    front_any, sample_any, pivot_ref, out_ref, top_ref,
    front_ref, sample_ref, turned_ref, p_ref,
    hop1, comb1, near1, sum1, hop2, comb2, near2, order_ref, y_ref,
    a1_ref, a2_ref, a3_ref, r1_ref, r2_ref, r3_ref, r4_ref, rt_ref, relay_ref, z_ref, m_ref, spot_ref, rows_ref,
    load_sem, rs_send, rs_recv, leaf_send, leaf_recv, y_send, relay_send, relay_recv, z_recv, z_local, twin_send, twin_recv,
    u_send, u_recv, u_onward,
):
    leaf, grp = lax.axis_index("leaf"), lax.axis_index("grp")
    y, x = grp // 4, lax.rem(grp, 4)
    core = lax.rem(leaf, 2)
    base = leaf - core

    loads = [
        pltpu.make_async_copy(sample_any.at[pl.ds(512 * r, 512)], sample_ref.at[pl.ds(512 * r, 512)], load_sem.at[r])
        for r in range(3)
    ]
    for quarter in range(4):
        rows = pl.ds(512 * (quarter % 2) + 256 * (quarter // 2), 256)
        loads.append(pltpu.make_async_copy(front_any.at[rows], front_ref.at[rows], load_sem.at[3 + quarter]))
    for load in loads:
        load.start()
    barrier = pltpu.get_barrier_semaphore()
    for other in range(1, 16):
        pl.semaphore_signal(barrier, inc=1, device_id=(leaf, lax.rem(grp + other, 16)), device_id_type=MESH)
        pl.semaphore_signal(barrier, inc=1, device_id=(lax.rem(leaf + other, 16), grp), device_id_type=MESH)

    started = []

    def begin(copy):
        copy.start()
        started.append(copy)
        return copy

    def neighbour(along_x, offset):
        if along_x:
            return (leaf, y * 4 + lax.rem(x + offset, 4))
        return (leaf, lax.rem(y + offset, 4) * 4 + x)

    def source(phase, stream, chunk, sub):
        half = stream % 2
        if phase == 0:
            lanes = pl.ds(512 * half + 256 * (stream // 2), 256)
            if half == 0:
                return p_ref.at[pl.ds(2 * sub, 2), chunk, :, lanes]
            return p_ref.at[chunk, pl.ds(2 * sub, 2), :, lanes]
        return sum1.at[stream, chunk, pl.ds(32 * sub, 32), :]

    def landing(phase, stream, way, sub):
        if phase == 0:
            return near1.at[stream, way, pl.ds(2 * sub, 2), :, :]
        return near2.at[stream, way, pl.ds(32 * sub, 32), :]

    hops, combs = (hop1, hop2), (comb1, comb2)
    rings = {}

    def ring(phase, stream, way, kind, src, dst):
        along_x = (phase == 0) == (stream % 2 == 0)
        to = neighbour(along_x, 1 if way == 0 else 3)
        rings[phase, stream, way, kind] = begin(
            send(src, dst, rs_send.at[phase, stream, way, kind], rs_recv.at[phase, stream, way, kind], to)
        )

    def position(phase, stream):
        return x if (phase == 0) == (stream % 2 == 0) else y

    def ring_hop(phase, stream):
        at = position(phase, stream)
        for way in range(2):
            ring(phase, stream, way, 0, source(phase, stream, lax.rem(at + 2, 4), way), hops[phase].at[stream, way])

    def ring_own(phase, stream):
        at = position(phase, stream)
        for way in range(2):
            chunk = lax.rem(at + (1 if way == 0 else 3), 4)
            ring(phase, stream, way, 1, source(phase, stream, chunk, 1 - way), landing(phase, stream, way, 1 - way))

    def ring_join(phase, stream):
        at = position(phase, stream)
        for way in range(2):
            chunk = lax.rem(at + (1 if way == 0 else 3), 4)
            rings[phase, stream, way, 0].wait_recv()
            combs[phase][stream, way] = hops[phase][stream, way] + source(phase, stream, chunk, way)[...]
            ring(phase, stream, way, 2, combs[phase].at[stream, way], landing(phase, stream, way, way))

    def ring_last(phase, stream):
        for way in range(2):
            for kind in (1, 2):
                rings[phase, stream, way, kind].wait_recv()
        half = stream % 2
        if phase == 0:
            lanes = pl.ds(512 * half + 256 * (stream // 2), 256)
            own = p_ref[:, x, :, lanes] if half == 0 else p_ref[y, :, :, lanes]
            sum1[stream] = (near1[stream, 0] + own) + near1[stream, 1]
            return None
        own = sum1[stream, position(1, stream)]
        return (near2[stream, 0] + own) + near2[stream, 1]

    for r in range(3):
        loads[r].wait()
        for c in range(8):
            turned_ref[128 * c : 128 * c + 128, 512 * r : 512 * r + 512] = sample_ref[
                512 * r : 512 * r + 512, 128 * c : 128 * c + 128
            ].T
    for quarter in range(4):
        low = 512 * (quarter % 2) + 256 * (quarter // 2)
        loads[3 + quarter].wait()
        for c in range(4):
            product = lax.dot_general(
                turned_ref[256 * c : 256 * c + 256, :], front_ref[low : low + 256, :], (((1,), (1,)), ((), ())),
                preferred_element_type=jnp.float32,
            )
            for b in range(4):
                p_ref[c, b, :, low : low + 256] = product[64 * b : 64 * b + 64]
        if quarter == 0:
            pl.semaphore_wait(barrier, 30)
        for n in range(PARTS // 2):
            stream = quarter % 2 + 2 * (PARTS // 2 * (quarter // 2) + n)
            ring_hop(0, stream)
            if stream < 2:
                ring_own(0, stream)

    def orders(level, block):
        node = 32 - (32 >> level) + leaf // (1 << level)
        chosen, rest = one_hot_order(row_of(pivot_ref[:, 128 * block : 128 * block + 128], node), 256 * block)
        order_ref[4 * level + block, :, 0:128] = chosen
        order_ref[4 * level + block, :, 128:256] = rest

    def select(level, block, value):
        chosen = permuted(value, order_ref[4 * level + block])
        task = (level + 1) // 2
        y_ref[task, 2 + block] = chosen[:, :128]
        y_ref[task, block + 4 * (block // 2)] = chosen[:, 128:]

    done = {}
    for step in range(PARTS + 3):
        if step < PARTS:
            for half in range(2):
                ring_join(0, 2 * step + half)
            if step + 1 < PARTS:
                for half in range(2):
                    ring_own(0, 2 * step + 2 + half)
        if step == 0:
            for level in range(5):
                for block in range(4):
                    orders(level, block)
        if 1 <= step <= PARTS:
            for half in range(2):
                ring_last(0, 2 * step - 2 + half)
                ring_hop(1, 2 * step - 2 + half)
                ring_own(1, 2 * step - 2 + half)
        if 2 <= step <= PARTS + 1:
            for half in range(2):
                ring_join(1, 2 * step - 4 + half)
        if step >= 3:
            part = step - 3
            for half in range(2):
                done[half, part] = ring_last(1, 2 * part + half)
            each = PARTS // 2
            if (part + 1) % each == 0:
                for half in range(2):
                    value = jnp.concatenate([done[half, part + 1 - each + n] for n in range(each)], axis=1)
                    select(0, 2 * half + part // each, value)

    def own_slice(task, act, local=True):
        root = ROOTS[0][task] + core * (ROOTS[1][task] - ROOTS[0][task])
        first, slot = lookup(FIRST[task], core, grp), lookup(SLOT[task], core, grp)
        pieces = [(part, y_ref.at[task, pl.ds(4 * part, 4)], pl.ds(4 * part, 4)) for part in range(2)]

        @pl.when(jnp.logical_and(first == root, grp != root))
        def _():
            for part, src, blocks in pieces:
                act(send(src, z_ref.at[grp, blocks], y_send.at[task, part], z_recv.at[grp, part], (leaf, root)))

        @pl.when(first != root)
        def _():
            for part, src, blocks in pieces:
                act(
                    send(
                        src, relay_ref.at[task, slot, blocks],
                        y_send.at[task, part], relay_recv.at[task, slot, part], (leaf, first),
                    )
                )

        if local:

            @pl.when(grp == root)
            def _():
                act(pltpu.make_async_copy(y_ref.at[task], z_ref.at[grp], z_local))

    def to_root(task):
        own_slice(task, lambda copy: copy.start())

    def pass_on(task, act):
        root = ROOTS[0][task] + core * (ROOTS[1][task] - ROOTS[0][task])
        for slot in range(3):
            source_grp = lookup(PASS_ON[task][slot], core, grp)

            @pl.when(source_grp > 0)
            def _():
                for part in range(2):
                    blocks = pl.ds(4 * part, 4)
                    held = relay_ref.at[task, slot, blocks]
                    act(
                        send(held, held, y_send.at[task, part], relay_recv.at[task, slot, part], (leaf, root)),
                        send(
                            held, z_ref.at[source_grp - 1, blocks],
                            relay_send.at[task, slot, part], z_recv.at[source_grp - 1, part], (leaf, root),
                        ),
                    )

    def relay(task):
        def act(landed, onward):
            landed.wait_recv()
            onward.start()

        pass_on(task, act)

    def both(first, second):
        return jnp.concatenate([first, second], axis=1)

    to_root(0)
    up = send(y_ref.at[0, pl.ds(2, 4)], r1_ref, leaf_send.at[0], leaf_recv.at[0], (base, grp))

    @pl.when(core == 1)
    def _():
        up.start()

    def chosen_only(level, block, value):
        return permuted(value, order_ref[4 * level + block][:, :128])

    kept = []

    def share(number, src, dst_ref, slot, recv, to_core, masks, value):
        for n, mask in enumerate(masks):
            copy = send(
                src, dst_ref.at[slot], leaf_send.at[number + n], leaf_recv.at[recv + slot], (flip(base, mask) + to_core, grp)
            )
            if mask == 0:

                @pl.when(core != to_core)
                def _():
                    copy.start()

                @pl.when(core == to_core)
                def _():
                    dst_ref[slot] = value

                kept.append((copy, to_core))
            else:
                begin(copy)

    for i in range(2):
        a1_ref[i] = chosen_only(1, 2 * core + i, both(y_ref[0, 2 + 2 * i], y_ref[0, 3 + 2 * i]))
    part1 = a1_ref[...]
    share(1, a1_ref, r2_ref, lax.rem(leaf, 4), 1, 1, (2, 0), part1)
    part2 = chosen_only(2, lax.rem(leaf, 4), both(part1[0], part1[1]))
    a2_ref[...] = part2
    share(3, a2_ref, r3_ref, lax.rem(leaf, 8), 5, 0, (4, 6, 2, 0), part2)
    zero = jnp.zeros_like(part2)
    spread_out = both(jnp.where(core == 0, part2, zero), jnp.where(core == 0, zero, part2))
    placed = chosen_only(3, lax.rem(leaf, 8) // 2, spread_out)
    part3 = placed[:32] + pltpu.roll(placed[32:], 64, 1)
    a3_ref[...] = part3
    share(7, a3_ref, r4_ref, leaf, 13, 1, (8, 10, 6, 12, 14, 4, 2, 0), part3)

    def arrived(ref, recv, slot):
        @pl.when(slot != lax.rem(leaf, ref.shape[0]))
        def _():
            send(ref.at[slot], ref.at[slot], leaf_send.at[0], leaf_recv.at[recv + slot], (base + 1 - core, grp)).wait_recv()

    @pl.when(core == 0)
    def _():
        for i in range(2):
            select(1, i, both(y_ref[0, 2 + 2 * i], y_ref[0, 3 + 2 * i]))
        send(r1_ref, r1_ref, leaf_send.at[0], leaf_recv.at[0], (base + 1, grp)).wait_recv()
        for i in range(2):
            select(1, 2 + i, both(r1_ref[2 * i], r1_ref[2 * i + 1]))

    @pl.when(core == 1)
    def _():
        for s in range(4):
            arrived(r2_ref, 1, s)
            select(2, s, both(r2_ref[s, 0], r2_ref[s, 1]))

    to_root(1)
    relay(0)

    @pl.when(core == 0)
    def _():
        for s in range(4):
            arrived(r3_ref, 5, 2 * s)
            arrived(r3_ref, 5, 2 * s + 1)
            select(3, s, both(r3_ref[2 * s], r3_ref[2 * s + 1]))

    @pl.when(core == 1)
    def _():
        low_lanes = lax.broadcasted_iota(jnp.int32, (32, 128), 1) < 64
        for s in range(16):
            arrived(r4_ref, 13, s)
        joined = []
        for i in range(8):
            even, odd = r4_ref[2 * i], r4_ref[2 * i + 1]
            upper = jnp.where(low_lanes, even, odd)
            lower = pltpu.roll(jnp.where(low_lanes, odd, even), 64, 1)
            joined.append(jnp.concatenate([upper, lower], axis=0))
        for s in range(4):
            select(4, s, both(joined[2 * s], joined[2 * s + 1]))

    to_root(2)
    relay(1)
    relay(2)

    top = send(y_ref.at[2, pl.ds(2, 4)], rt_ref, leaf_send.at[15], leaf_recv.at[29], (base, grp))

    @pl.when(core == 1)
    def _():
        top.start()

    earlier = jnp.where(
        lax.broadcasted_iota(jnp.int32, (64, 64), 1) < lax.broadcasted_iota(jnp.int32, (64, 64), 0), 1.0, 0.0
    ).astype(jnp.bfloat16)
    ones = jnp.full((512, 128), 1.0, jnp.bfloat16)
    for level in range(5):
        node = 32 - (32 >> level) + leaf // (1 << level)
        place = grp * 64 + lax.broadcasted_iota(jnp.int32, (64, 512), 0)
        is_pivot = jnp.where(place == row_of(pivot_ref[...], node), 1.0, 0.0)
        out_ref[level] = is_pivot
        free = 1.0 - jnp.dot(is_pivot.astype(jnp.bfloat16), ones, preferred_element_type=jnp.float32)
        rank = jnp.dot(earlier, free.astype(jnp.bfloat16), preferred_element_type=jnp.float32)
        lane = lax.broadcasted_iota(jnp.int32, (64, 128), 1).astype(jnp.float32)
        spot_ref[level] = jnp.where(jnp.logical_and(free > 0.5, rank == lane), 1.0, 0.0)

    is_main, is_twin = roles()
    twin_leaf = base + 1 - core
    coming = ((0, 0), (0, 1), (0, 3), (1, 0), (3, 0), (0, 2), (2, 0), (1, 1), (1, 3), (3, 1), (3, 3), (1, 2), (3, 2), (2, 1), (2, 3), (2, 2))

    def to_twin(at):
        part = z_ref.at[at, pl.ds(2, 6)]
        return send(part, part, twin_send.at[at], twin_recv.at[at], (twin_leaf, grp))

    for group in range(4):
        places = [lax.rem(y + dy, 4) * 4 + lax.rem(x + dx, 4) for dy, dx in coming[4 * group : 4 * group + 4]]

        @pl.when(is_main > 0)
        def _():
            for n, at in enumerate(places):
                if group == 0 and n == 0:
                    pltpu.make_async_copy(y_ref.at[0], z_ref.at[at], z_local).wait()
                else:
                    for part in range(2):
                        piece = z_ref.at[at, pl.ds(4 * part, 4)]
                        send(piece, piece, y_send.at[0, part], z_recv.at[at, part], (twin_leaf, grp)).wait_recv()
                to_twin(at).start()

        @pl.when(is_twin > 0)
        def _():
            for at in places:
                to_twin(at).wait_recv()

        @pl.when(is_main + is_twin > 0)
        def _():
            rows = []
            for at in places:
                blocks = [z_ref[at, 2 + b] for b in range(4)] + [z_ref[at, 6 * is_twin + b] for b in range(2)]
                rows.append(jnp.concatenate(blocks, axis=1))
            z = jnp.concatenate(rows, axis=0)
            gram = lax.dot_general(
                z, z[:, :512], (((0,), (0,)), ((), ())), precision=HI, preferred_element_type=jnp.float32
            )
            if group == 0:
                m_ref[...] = gram
            else:
                m_ref[...] += gram

    def each(level, of_core, half, place, to_core, act, parts=(0, 1)):
        @pl.when(jnp.logical_and(core == of_core, grp == place))
        def _():
            for target in [8 * half + 4 * part + n for part in parts for n in range(4)]:
                if (target, to_core) != (place, of_core):
                    act(
                        send(
                            m_ref.at[pl.ds(512 + 32 * (target - 8 * half), 32)], rows_ref.at[level],
                            u_send.at[target], u_recv.at[level], (base + to_core, target),
                        )
                    )

    def rows_ready(part):
        for sender in senders():
            each(*sender, lambda copy: copy.start(), (part,))

    @pl.when(is_main + is_twin > 0)
    def _():
        solve_in_place(m_ref, rows_ready)

    block_half = grp // 8

    def onward(level):
        return send(rows_ref.at[level], rows_ref.at[level], u_onward.at[level], u_recv.at[level], (twin_leaf, grp))

    def served_here(of_core):
        return core == of_core + block_half * (1 - 2 * of_core)

    for of_core in range(2):
        for task in range(3):
            level, root = LEVELS[of_core][task], ROOTS[of_core][task]
            direct = core == of_core if task == 0 else served_here(of_core)
            is_root = grp == root
            if task == 0:
                is_root = jnp.logical_and(is_root, block_half == 0)

            @pl.when(jnp.logical_and(direct, is_root))
            def _():
                low = 512 + 32 * (root % 8)
                rows_ref[level] = m_ref[low : low + 32, :]

            @pl.when(jnp.logical_and(direct, jnp.logical_not(is_root)))
            def _():
                onward(level).wait_recv()

            if task > 0:

                @pl.when(direct)
                def _():
                    onward(level).start()

    for of_core in range(2):
        for task in (1, 2):
            level = LEVELS[of_core][task]

            @pl.when(jnp.logical_not(served_here(of_core)))
            def _():
                onward(level).wait_recv()

    for level in range(5):
        spot = spot_ref[level][:, :32].astype(jnp.bfloat16)
        out_ref[level] += jnp.dot(
            jnp.concatenate([spot, spot, spot], axis=1), split3(rows_ref[level]), preferred_element_type=jnp.float32
        )
    for sender in senders():
        each(*sender, lambda copy: copy.wait_send())
    for of_core in range(2):
        for task in (1, 2):
            level = LEVELS[of_core][task]

            @pl.when(served_here(of_core))
            def _():
                onward(level).wait_send()

    @pl.when(core == 1)
    def _():
        for b in range(4):
            top_ref[:, 128 * b : 128 * b + 128] = y_ref[2, 2 + b]
        up.wait_send()
        top.wait_send()

    @pl.when(core == 0)
    def _():
        top.wait_recv()
        for b in range(4):
            top_ref[:, 128 * b : 128 * b + 128] = rt_ref[b]

    @pl.when(is_main > 0)
    def _():
        for at in range(16):
            to_twin(at).wait_send()

    for copy, to_core in kept:

        @pl.when(core != to_core)
        def _():
            copy.wait_send()

    for copy in started:
        copy.wait_send()
    for task in range(3):
        own_slice(task, lambda copy: copy.wait_send(), local=False)
        pass_on(task, lambda landed, onward: onward.wait_send())


def gathered(front_rows, sample_matrix, pivots):
    dma = pltpu.SemaphoreType.DMA
    f32 = lambda *shape: pltpu.VMEM(shape, jnp.float32)
    bf16 = lambda *shape: pltpu.VMEM(shape, jnp.bfloat16)
    anywhere = pl.BlockSpec(memory_space=pl.ANY)
    vmem = pl.BlockSpec(memory_space=pltpu.VMEM)
    return pl.pallas_call(
        gather_kernel,
        out_shape=(jax.ShapeDtypeStruct((5, 64, 512), jnp.float32), jax.ShapeDtypeStruct((64, 512), jnp.float32)),
        in_specs=[anywhere, anywhere, vmem],
        out_specs=(vmem, vmem),
        scratch_shapes=[
            bf16(1024, 1536), bf16(1536, 1024), bf16(1024, 1536), f32(4, 4, 64, 1024),
            f32(4, 2, 2, 64, 256), f32(4, 2, 2, 64, 256), f32(4, 2, 4, 64, 256), f32(4, 4, 64, 256),
            f32(4, 2, 32, 256), f32(4, 2, 32, 256), f32(4, 2, 64, 256), bf16(20, 256, 256), f32(3, 8, 64, 128),
            f32(2, 64, 128), f32(64, 128), f32(32, 128), f32(4, 64, 128), f32(4, 2, 64, 128), f32(8, 64, 128), f32(16, 32, 128),
            f32(4, 64, 128), f32(3, 3, 8, 64, 128), f32(16, 8, 64, 128),
            f32(768, 512), f32(5, 64, 128), f32(5, 32, 512),
            dma((7,)), dma((2, 4, 2, 3)), dma((2, 4, 2, 3)), dma((16,)), dma((30,)),
            dma((3, 2)), dma((3, 3, 2)), dma((3, 3, 2)), dma((16, 2)), dma, dma((16,)), dma((16,)),
            dma((16,)), dma((5,)), dma((5,)),
        ],
        compiler_params=pltpu.CompilerParams(collective_id=1, has_side_effects=True, vmem_limit_bytes=52 * 1024 * 1024),
    )(front_rows, sample_matrix, pivots)


def senders():
    for core in range(2):
        for task in range(3):
            level, root = LEVELS[core][task], ROOTS[core][task]
            for half in range(2):
                sender = core if half == 0 else 1 - core
                yield level, sender, half, root, core if level == 0 else sender


def wide(value):
    return jnp.broadcast_to(value, (8, 128))


def small_inverse(columns, sub):
    columns = list(columns)
    for k in range(8):
        rows = [wide(column[k : k + 1, :]) for column in columns]
        scale = 1.0 / rows[k]
        here = sub == k
        lead = columns[k]
        for j in range(8):
            if j != k:
                row = rows[j] * scale
                columns[j] = jnp.where(here, row, columns[j] - lead * row)
        columns[k] = jnp.where(here, scale, -(lead * scale))
    return columns


def weighted(columns, rows):
    even, odd = columns[0] * rows[0], columns[1] * rows[1]
    for j in range(2, 8, 2):
        even = even + columns[j] * rows[j]
        odd = odd + columns[j + 1] * rows[j + 1]
    return even + odd


def eliminate(read):
    lane = lax.broadcasted_iota(jnp.int32, (8, 128), 1)
    sub = lax.broadcasted_iota(jnp.int32, (8, 128), 0)
    eye = jnp.where(lane == sub, 1.0, 0.0)

    def eight(_, blocks):
        corner = small_inverse([wide(blocks[0][:, 8 + j : 9 + j]) for j in range(8)], sub)
        columns = [[wide(block[:, 8 + j : 9 + j]) for j in range(8)] for block in blocks[1:]]
        rolled = [pltpu.roll(block, 120, 1) for block in blocks]
        top = jnp.where(lane < 8, eye, rolled[0])
        new = weighted(corner, [wide(top[j : j + 1]) for j in range(8)])
        rows = [wide(new[j : j + 1]) for j in range(8)]
        rest = [jnp.where(lane < 8, 0.0, block) - weighted(cols, rows) for cols, block in zip(columns, rolled[1:])]
        return tuple(rest + [new])

    blocks = lax.fori_loop(0, 8, eight, tuple(pltpu.roll(read(i), 8, 1) for i in range(8)))
    return jnp.concatenate([pltpu.roll(block, 56, 1) for block in blocks], axis=0)


def invert(block):
    upper, lower = block[:64], block[64:]
    lane = lax.broadcasted_iota(jnp.int32, (64, 128), 1)
    first = eliminate(lambda i: upper[8 * i : 8 * i + 8])
    reduced = pltpu.roll(jnp.where(lane < 64, 0.0, lower) - product(lower[:, :64], first), 64, 1)
    second = eliminate(lambda i: reduced[8 * i : 8 * i + 8])
    bottom = pltpu.roll(second, 64, 1)
    across = pltpu.roll(first, 64, 1)[:, :64]
    top = jnp.where(lane < 64, first, 0.0) - product(across, bottom)
    return jnp.concatenate([top, bottom], axis=0)


def dot(a, b):
    return lax.dot_general(a, b, (((1,), (0,)), ((), ())), precision=HI, preferred_element_type=jnp.float32)


def product(a, b):
    n, depth = a.shape
    ah, am, al = (split3(a)[k * n : k * n + n] for k in range(3))
    bh, bm, bl = (split3(b)[k * depth : k * depth + depth] for k in range(3))
    left = jnp.concatenate([al, am, ah, am, ah, ah], axis=1)
    right = jnp.concatenate([bh, bm, bl, bh, bm, bh], axis=0)
    return jnp.dot(left, right, preferred_element_type=jnp.float32)


def solve_in_place(m_ref, rows_ready):
    for p in range(4):
        at = 128 * p
        dinv = invert(m_ref[at : at + 128, at : at + 128])
        others = [q for q in range(4) if q != p]
        lead = jnp.concatenate([m_ref[at : at + 128, 128 * q : 128 * q + 128] for q in others], axis=1)
        both_sides = product(dinv, lead)
        right = jnp.concatenate([both_sides, dinv], axis=1)
        bounds = (at + 128, 768) if p < 3 else (512, 640, 768)
        for part, (low, high) in enumerate(zip(bounds, bounds[1:])):
            change = product(m_ref[low:high, at : at + 128], right)
            for n, q in enumerate(others):
                m_ref[low:high, 128 * q : 128 * q + 128] -= change[:, 128 * n : 128 * n + 128]
            m_ref[low:high, at : at + 128] = change[:, 384:]
            if p == 3:
                rows_ready(part)


def on_device(front_rows, sample_matrix, pivots):
    bases, top = gathered(front_rows, sample_matrix, pivots)
    return (bases[:, None], top)


def solution(mesh):
    return jax.shard_map(
        on_device,
        mesh=mesh,
        in_specs=(P("leaf", "grp"), P("grp", None), P()),
        out_specs=(P(None, "leaf", "grp", None), P("grp", None)),
        check_vma=False,
    )
```
